32 devices in a mesh: dp: 1 (over z), cz: 4 (over y), cy: 4 (over x), cx: 2 (over core).
Axes of the slice: x: 4, y: 4, z: 1, core: 2. Of those that a mesh axis runs over, the one named last changes fastest.
The devices are a block of a 4x4x8 slice.
Arguments:
- x_act: bfloat16 [4096, 4096], P(('dp', 'cx', 'cz'), 'cy')
- w_up: bfloat16 [4096, 16384], P('cy', ('cz', 'cx'))
- w_down: bfloat16 [16384, 4096], P('cz', ('cy', 'cx'))
- z_grad: bfloat16 [4096, 4096], P(('dp', 'cx', 'cz'), 'cy')
Outputs:
- output 1: bfloat16 [4096, 4096], P(('dp', 'cx', 'cz'), 'cy')
- output 2: bfloat16 [4096, 16384], P(('dp', 'cy'), ('cz', 'cx'))
- output 3: bfloat16 [16384, 4096], P(('dp', 'cz'), ('cy', 'cx'))
All inputs are finite; a program needn't handle non-finite values.
Results may differ from the reference program's by a relative error of at most 0.0115233.
Values are sent between devices in bfloat16 or wider.
A program may use at most 768 MiB of HBM per device.

```python
import math
import jax
import jax.numpy as jnp

TOKENS = 4096
MODEL_DIM = 4096
HIDDEN_DIM = 16384
GELU_COEF = 0.044715
SQRT_TWO_PI = math.sqrt(2.0 / math.pi)


def gelu_parts(pre_act):
    inner_arg = SQRT_TWO_PI * (pre_act + GELU_COEF * pre_act * pre_act * pre_act)
    tanh_val = jnp.tanh(inner_arg)
    gelu_val = 0.5 * pre_act * (1.0 + tanh_val)
    gelu_slope = 0.5 * (1.0 + tanh_val) + 0.5 * pre_act * (1.0 - tanh_val * tanh_val) * SQRT_TWO_PI * (1.0 + 3.0 * GELU_COEF * pre_act * pre_act)
    return gelu_val, gelu_slope


def setup_inputs(seed: int = 0, part: int = 0) -> dict:
    base_key = jax.random.key(seed)
    key_up, key_down, key_acts = jax.random.split(base_key, 3)
    part_key = jax.random.fold_in(key_acts, part)
    key_x, key_z = jax.random.split(part_key)
    x_act = jax.random.normal(key_x, (TOKENS, MODEL_DIM), jnp.float32)
    w_up = jax.random.normal(key_up, (MODEL_DIM, HIDDEN_DIM), jnp.float32) * MODEL_DIM ** -0.5
    w_down = jax.random.normal(key_down, (HIDDEN_DIM, MODEL_DIM), jnp.float32) * HIDDEN_DIM ** -0.5
    z_grad = jax.random.normal(key_z, (TOKENS, MODEL_DIM), jnp.float32)
    return {"x_act": x_act.astype(jnp.bfloat16), "w_up": w_up.astype(jnp.bfloat16), "w_down": w_down.astype(jnp.bfloat16), "z_grad": z_grad.astype(jnp.bfloat16)}


def reference(x_act, w_up, w_down, z_grad):
    pre_act = jnp.dot(x_act, w_up, preferred_element_type=jnp.float32).astype(jnp.bfloat16).astype(jnp.float32)
    gelu_val, gelu_slope = gelu_parts(pre_act)
    hidden = gelu_val.astype(jnp.bfloat16)
    h_grad = jnp.dot(z_grad, w_down.T, preferred_element_type=jnp.float32)
    pre_grad = (h_grad * gelu_slope).astype(jnp.bfloat16)
    x_grad = jnp.dot(pre_grad, w_up.T, preferred_element_type=jnp.float32).astype(jnp.bfloat16)
    up_grad = jnp.dot(x_act.T, pre_grad, preferred_element_type=jnp.float32).astype(jnp.bfloat16)
    down_grad = jnp.dot(hidden.T, z_grad, preferred_element_type=jnp.float32).astype(jnp.bfloat16)
    return (x_grad, up_grad, down_grad)
```

```python
import math
import jax
import jax.numpy as jnp
from jax import lax
from jax.sharding import PartitionSpec as P

GELU_COEF = 0.044715
SQRT_TWO_PI = math.sqrt(2.0 / math.pi)
CONTRACT_LAST = (((1,), (1,)), ((), ()))
CONTRACT_FIRST = (((0,), (0,)), ((), ()))


def gelu_parts(pre_act):
    inner_arg = SQRT_TWO_PI * (pre_act + GELU_COEF * pre_act * pre_act * pre_act)
    tanh_val = jnp.tanh(inner_arg)
    gelu_val = 0.5 * pre_act * (1.0 + tanh_val)
    gelu_slope = 0.5 * (1.0 + tanh_val) + 0.5 * pre_act * (1.0 - tanh_val * tanh_val) * SQRT_TWO_PI * (1.0 + 3.0 * GELU_COEF * pre_act * pre_act)
    return gelu_val, gelu_slope


def solution(mesh):
    ncx, ncy = mesh.shape["cx"], mesh.shape["cy"]
    row_spec = P(("dp", "cx", "cz"), "cy")
    up_spec = P("cy", ("cz", "cx"))
    down_spec = P("cz", ("cy", "cx"))
    up_out = P(("dp", "cy"), ("cz", "cx"))
    down_out = P(("dp", "cz"), ("cy", "cx"))

    def local_step(x_act, w_up, w_down, z_grad):
        dloc, floc = w_up.shape
        sub = floc // ncy
        x_row = lax.all_gather(x_act, "cy", axis=1, tiled=True)
        x_full = lax.all_gather(x_row, "cz", axis=0, tiled=True)
        g_row = lax.all_gather(z_grad, "cy", axis=1, tiled=True)
        g_full = lax.all_gather(g_row, "cz", axis=0, tiled=True)
        up_slice = lax.all_to_all(w_up, "cy", split_axis=1, concat_axis=0, tiled=True)
        up_slice = lax.all_gather(up_slice, "cx", axis=1, tiled=True)
        wd = w_down.reshape(ncx, ncy, sub, -1).transpose(1, 0, 2, 3).reshape(ncy, ncx * sub, -1)
        wd = lax.all_to_all(wd, "cy", split_axis=0, concat_axis=0)
        wd = lax.all_gather(wd, "cx", axis=1)
        down_slice = wd.transpose(2, 0, 1, 3).reshape(ncx * sub, -1)
        pre_act = jnp.dot(x_full, up_slice, preferred_element_type=jnp.float32).astype(jnp.bfloat16).astype(jnp.float32)
        gelu_val, gelu_slope = gelu_parts(pre_act)
        hidden = gelu_val.astype(jnp.bfloat16)
        h_grad = lax.dot_general(g_full, down_slice, CONTRACT_LAST, preferred_element_type=jnp.float32)
        pre_grad = (h_grad * gelu_slope).astype(jnp.bfloat16)
        grad_all = lax.all_gather(pre_grad, "cy", axis=0)
        rows = grad_all.shape[1]
        grad_full = grad_all.reshape(ncy, rows, ncx, sub).transpose(1, 2, 0, 3).reshape(rows, -1)
        up_full = lax.all_gather(w_up, "cx", axis=1, tiled=True)
        x_part = lax.dot_general(grad_full, up_full, CONTRACT_LAST, preferred_element_type=jnp.float32)
        x_grad = lax.psum_scatter(x_part, "cz", scatter_dimension=0, tiled=True).astype(jnp.bfloat16)
        down_part = lax.dot_general(hidden, g_full, CONTRACT_FIRST, preferred_element_type=jnp.float32)
        down_part = down_part.reshape(ncx * sub, ncy, ncx, -1).transpose(2, 0, 1, 3).reshape(ncx * ncx * sub, -1)
        down_sum = lax.psum_scatter(down_part, "cx", scatter_dimension=0, tiled=True).astype(jnp.bfloat16)
        down_sum = down_sum.reshape(ncx * sub, ncy, -1)
        down_all = lax.all_to_all(down_sum, "cy", split_axis=1, concat_axis=0)
        down_grad = down_all.reshape(ncy, ncx, sub, -1).transpose(1, 0, 2, 3).reshape(ncy * ncx * sub, -1)
        x_col = lax.all_gather(x_act, "cz", axis=0, tiled=True)
        up_part = lax.dot_general(x_col, grad_full, CONTRACT_FIRST, preferred_element_type=jnp.float32)
        up_grad = lax.psum_scatter(up_part, "cx", scatter_dimension=1, tiled=True).astype(jnp.bfloat16)
        return (x_grad, up_grad, down_grad)

    return jax.shard_map(local_step, mesh=mesh, in_specs=(row_spec, up_spec, down_spec, row_spec), out_specs=(row_spec, up_out, down_out), check_vma=False)
```

```python
import functools
import math

import jax
import jax.numpy as jnp
from jax import lax
from jax.experimental import pallas as pl
from jax.experimental.pallas import tpu as pltpu
from jax.sharding import PartitionSpec as P

GELU_COEF = 0.044715
SQRT_TWO_PI = math.sqrt(2.0 / math.pi)
NN = (((1,), (0,)), ((), ()))
NT = (((1,), (1,)), ((), ()))
TN = (((0,), (0,)), ((), ()))
MESH = pl.DeviceIdType.MESH
RING = 4
CORES = 2
NR = 4
PAN = 3


def gelu_parts(pre_act):
    inner_arg = SQRT_TWO_PI * (pre_act + GELU_COEF * pre_act * pre_act * pre_act)
    tanh_val = jnp.tanh(inner_arg)
    gelu_val = 0.5 * pre_act * (1.0 + tanh_val)
    gelu_slope = 0.5 * (1.0 + tanh_val) + 0.5 * pre_act * (1.0 - tanh_val * tanh_val) * SQRT_TWO_PI * (1.0 + 3.0 * GELU_COEF * pre_act * pre_act)
    return gelu_val, gelu_slope


def full(a, r):
    row = [f"x{a}{r}", f"rx{a}{r}", f"ry{a}{r}", "own"]
    return row + ([f"y{a}{r}a", f"y{a}{r}b"] if r < 2 else [f"y{a}{r}"])


def make_plan():
    it = {}
    groups = range(NR)
    q = 1.0 / NR
    for r in groups:
        for a in "XG":
            it[f"x{a}{r}"] = ("X", q, [])
            it[f"rx{a}{r}"] = ("X", q / 2, [f"x{a}{r}"])
            row = [f"x{a}{r}", f"rx{a}{r}"]
            if r < 2:
                it[f"y{a}{r}a"] = ("Y", q, [])
                it[f"y{a}{r}b"] = ("Y", 3 * q, row)
                it[f"ry{a}{r}"] = ("Y", 2 * q, [f"y{a}{r}a", f"y{a}{r}b"])
            else:
                it[f"y{a}{r}"] = ("Y", 4 * q, row + ["own"])
                it[f"ry{a}{r}"] = ("Y", 2 * q, [f"y{a}{r}"])
        it[f"GP{r}"] = ("D", 8 * q, full("G", r))
        it[f"XP{r}"] = ("D", 4 * q, full("X", r))
        it[f"HP{r}"] = ("D", 4 * q, [f"m2_{r}"])
        it[f"dC{r}"] = ("X", 4 * q, [f"m2_{r}"])
        it[f"rdC{r}"] = ("X", 2 * q, [f"dC{r}"])
        it[f"dCP{r}"] = ("D", 8 * q, [f"dC{r}", f"rdC{r}"])
        it[f"q2_{r}"] = ("Y", q, [f"m3_{r}"])
        it[f"qd_{r}"] = ("Y", q, [f"m3_{r}"])
        it[f"qs_{r}"] = ("Y", q, [f"qa_{r}"])
        it[f"l1_{r}"] = ("L", 4, full("X", r))
        it[f"l2_{r}"] = ("L", 4, full("G", r))
        it[f"l3_{r}"] = ("L", 4, [f"dC{r}", f"rdC{r}"])
    for w in "ud":
        it[f"W{w}2"] = ("X", 0.5, [])
        it[f"W{w}1"] = ("X", 1.0, [])
        it[f"rW{w}"] = ("X", 0.5, [f"W{w}2"])
        it[f"W{w}P0"] = ("D", 1, [])
        it[f"W{w}P1"] = ("D", 2, [f"W{w}1"])
        it[f"W{w}P2"] = ("D", 1, [f"rW{w}"])
    it["WN"] = ("D", 4, [])
    it["own"] = ("L", 2, [])
    it["w2"] = ("X", 0.5, ["m5_2"])
    it["w1"] = ("X", 1.0, ["m5_1", "m5_3"])
    it["rw"] = ("X", 0.5, ["w2"])
    for j in range(RING):
        it[f"l5_{j}"] = ("L", 4, [f"GP{r}" for r in groups] + sum([full("G", r) for r in groups], []))
        it[f"l4_{j}"] = ("L", 4, [f"dCP{r}" for r in groups] + [f"rdC{r}" for r in groups])
    it["lh"] = ("L", 4, [f"HP{r}" for r in groups] + [f"m2_{r}" for r in groups])
    it["lx"] = ("L", 8, [f"XP{r}" for r in groups] + [f"m1_{r}" for r in groups])
    lists = {
        "X": (
            ["xX0", "xG0", "rxX0", "rxG0", "xX1", "xG1", "rxX1", "rxG1", "Wu2", "Wu1", "rWu", "xX2", "xG2", "rxX2", "rxG2"]
            + ["Wd2", "Wd1", "rWd", "xX3", "xG3", "rxX3", "rxG3", "dC0", "dC1", "rdC0", "rdC1", "dC2", "rdC2", "dC3", "rdC3"]
            + ["w2", "w1", "rw"]
        ),
        "Y": (
            ["yX0a", "yG0a", "yX1a", "yG1a", "yX0b", "yG0b", "ryX0", "ryG0", "yX1b", "yG1b", "ryX1", "ryG1"]
            + ["yX2", "yG2", "ryX2", "ryG2", "yX3", "yG3", "ryX3", "ryG3"]
            + [f"{k}_{r}" for r in groups for k in ("q2", "qd", "qs")]
        ),
        "D": (
            ["WN", "WuP0", "WdP0", "WuP1", "WuP2", "XP0", "GP0", "WdP1", "WdP2", "XP1", "GP1", "HP0", "HP1"]
            + ["XP2", "GP2", "HP2", "dCP0", "dCP1", "XP3", "GP3", "HP3", "dCP2", "dCP3"]
        ),
        "L": (
            ["own", "l1_0", "l2_0", "l1_1", "l2_1", "l1_2", "l2_2", "l3_0", "l3_1", "l1_3", "l2_3", "l3_2", "lx", "lh"]
            + ["l5_2", "l5_1", "l5_3", "l5_0", "l3_3", "l4_0", "l4_1", "l4_2", "l4_3"]
        ),
    }
    wu, wd = ["WuP0", "WuP1", "WuP2"], ["WdP0", "WdP1", "WdP2"]
    m1 = lambda r: (f"m1_{r}", 5.5, [f"l1_{r}"] + wu)
    m2 = lambda r: (f"m2_{r}", 8.5, [f"l2_{r}", f"m1_{r}"] + wd)
    m3 = lambda r: (f"m3_{r}", 5.5, [f"l3_{r}", "WN"] + ([f"qf_{r - 2}"] if r >= 2 else []))
    m5 = lambda j: (f"m5_{j}", 6.0, [f"l5_{j}", "lh"])
    m4 = lambda j: (f"m4_{j}", 6.0, [f"l4_{j}", "lx"] + [f"m5_{i}" for i in range(RING)])
    units = [m2(0), m1(0), m2(1), m1(1), m2(2), m1(2), m2(3), m1(3)]
    units += [(f"qa_{r}", 1.0, [f"q2_{r}"]) for r in groups] + [(f"qf_{r}", 1.0, [f"qs_{r}", f"qd_{r}"]) for r in groups]
    units += [m5(2), m5(1), m5(3), m3(0), m3(1), m3(2), m3(3), m5(0)] + [m4(j) for j in range(RING)]
    return it, lists, units


RATE = {"X": 22.5, "Y": 22.5, "D": 1.7, "L": 0.4}
DELAY = {"X": 3.0, "Y": 3.0, "D": 1.5, "L": 1.5}


def make_order(it, lists, units):
    done, free, pos = {}, {k: 0.0 for k in lists}, {k: 0 for k in lists}
    pend, now, order = list(units), 0.0, []
    panels = []
    finished = set()
    while True:
        moved = True
        while moved:
            moved = False
            for k in lists:
                while pos[k] < len(lists[k]):
                    n = lists[k][pos[k]]
                    ready = all(done.get(d, 1e9) <= now for d in it[n][2])
                    if n[0] == "l" and n not in ("lh", "lx"):
                        ready = ready and (len(panels) < PAN or ("m" + panels[-PAN][1:]) in finished)
                    if not ready:
                        break
                    if n[0] == "l" and n not in ("lh", "lx"):
                        panels.append(n)
                    free[k] = max(now + 0.3, free[k]) + it[n][1] * RATE[k]
                    done[n] = free[k] + DELAY[k]
                    order.append((n, now))
                    pos[k] += 1
                    moved = True
        can = [u for u in pend if all(done.get(d, 1e9) <= now for d in u[2])]
        if can:
            u = can[0]
            pend.remove(u)
            order.append((u[0], now))
            now += u[1]
            done[u[0]] = now
            finished.add(u[0])
            continue
        later = [v for v in done.values() if v > now]
        if not later:
            break
        now = min(later)
    assert not pend and all(pos[k] == len(lists[k]) for k in lists), (pend, pos)
    return order, panels, max(done.values())


class Copies:
    def __init__(self, send, recv, local, peers):
        self.send, self.recv, self.local, self.peers = send, recv, local, peers
        self.n_remote = self.n_local = 0
        self.by_name = {}

    def add(self, name, pairs):
        made = []
        for src, dst, to in pairs:
            if to is None:
                c = pltpu.make_async_copy(src, dst, self.local.at[self.n_local])
                self.n_local += 1
            else:
                axis, idx = self.peers[to]
                c = pltpu.make_async_remote_copy(
                    src, dst, self.send.at[self.n_remote], self.recv.at[self.n_remote],
                    device_id={axis: idx}, device_id_type=MESH)
                self.n_remote += 1
            made.append([c, to, False, False])
            c.start()
        self.by_name.setdefault(name, []).extend(made)

    def arrived(self, name):
        for m in self.by_name.get(name, ()):
            if not m[2]:
                m[2] = True
                m[0].wait() if m[1] is None else m[0].wait_recv()

    def left(self, name):
        for m in self.by_name.get(name, ()):
            if m[1] is None:
                if not m[2]:
                    m[2] = True
                    m[0].wait()
            elif not m[3]:
                m[3] = True
                m[0].wait_send()

    def finish(self):
        for name in list(self.by_name):
            self.arrived(name)
            self.left(name)


N_REMOTE = 190
N_LOCAL = 80


def kernel(plan, order, panels, xa, wu, wd, za, dx, dwu, dwd, XF, GF, DF, GP, DP, XP, HP, su, sd, sw,
           wus, wds, wun, hbuf, pan, ft, dct, rst, rrc, obuf, xo, acc, send, recv, local):
    it, lists, units = plan
    x, y, c = lax.axis_index("cy"), lax.axis_index("cz"), lax.axis_index("cx")
    peers = {
        "R": ("cy", lax.rem(x + 1, RING)), "L": ("cy", lax.rem(x + RING - 1, RING)),
        "U": ("cz", lax.rem(y + 1, RING)), "N": ("cz", lax.rem(y + RING - 1, RING)),
        "P": ("cx", 1 - c),
    }
    barrier = pltpu.get_barrier_semaphore()
    for axis, idx in peers.values():
        pl.semaphore_signal(barrier, inc=1, device_id={axis: idx}, device_id_type=MESH)
    pl.semaphore_wait(barrier, len(peers))

    cp = Copies(send, recv, local, peers)
    rows = xa.shape[1]
    half = rows // 2
    grp = RING * rows
    sub = wd.shape[2]
    dh = wu.shape[1]
    mine = pl.ds(pl.multiple_of(c * sub, sub), sub)
    theirs = pl.ds(pl.multiple_of((1 - c) * sub, sub), sub)
    lo, hi = pl.ds(0, sub), pl.ds(sub, sub)
    at = lambda j: lax.rem(x + j, RING)
    cols = lambda j: pl.ds(pl.multiple_of(at(j) * sub, sub), sub)
    K = lambda k: pl.ds(k * rows, rows)
    slot_of = {n: i % PAN for i, n in enumerate(panels)}
    inp = {"X": xa, "G": za}
    buf = {"X": XF, "G": GF}

    def copies_of(n):
        if n == "WN":
            return sum([[(wu.at[:, :, cols(j)], wun.at[2 * j:2 * j + 2, :, mine], to) for to in (None, "P")] for j in range(RING)], [])
        if n[0] == "x":
            a, r = n[1], int(n[2])
            return [(inp[a].at[r], buf[a].at[3, r, K(0)], "R"), (inp[a].at[r], buf[a].at[1, r, K(0)], "L")]
        if n[:2] == "rx":
            a, r = n[2], int(n[3])
            first, second = pl.ds(0, half), pl.ds(half, half)
            return [(buf[a].at[3, r, first], buf[a].at[2, r, first], "R"), (buf[a].at[1, r, second], buf[a].at[2, r, second], "L")]
        if n[0] == "y":
            a, r = n[1], int(n[2])
            b = buf[a]
            if n.endswith("a"):
                return [(inp[a].at[r], b.at[0, r, K(3)], "U"), (inp[a].at[r], b.at[0, r, K(1)], "N")]
            js = pl.ds(1, RING - 1) if n.endswith("b") else pl.ds(0, RING)
            return [(b.at[js, r, K(0)], b.at[js, r, K(3)], "U"), (b.at[js, r, K(0)], b.at[js, r, K(1)], "N")]
        if n[:2] == "ry":
            a, r = n[2], int(n[3])
            b = buf[a]
            return [(b.at[0:2, r, K(3)], b.at[0:2, r, K(2)], "U"), (b.at[2:4, r, K(1)], b.at[2:4, r, K(2)], "N")]
        if n in ("Wu2", "Wd2"):
            src, st = (lambda h: wu.at[h, :, cols(2)], su) if n == "Wu2" else (lambda h: wd.at[h, at(2)], sd)
            return [(src(0), st.at[0], "R"), (src(1), st.at[1], "L")]
        if n in ("Wu1", "Wd1"):
            src, dst = (lambda j: wu.at[:, :, cols(j)], wus) if n == "Wu1" else (lambda j: wd.at[:, at(j)], wds)
            return [(src(1), dst.at[6:8, :, mine], "R"), (src(3), dst.at[2:4, :, mine], "L")]
        if n in ("rWu", "rWd"):
            st, dst = (su, wus) if n == "rWu" else (sd, wds)
            return [(st.at[0], dst.at[4, :, mine], "R"), (st.at[1], dst.at[5, :, mine], "L")]
        if n in ("WuP0", "WdP0"):
            src, dst = (wu.at[:, :, cols(0)], wus) if n == "WuP0" else (wd.at[:, at(0)], wds)
            return [(src, dst.at[0:2, :, mine], None), (src, dst.at[0:2, :, mine], "P")]
        if n in ("WuP1", "WdP1"):
            b = wus if n == "WuP1" else wds
            return [(b.at[2:4, :, mine], b.at[2:4, :, mine], "P"), (b.at[6:8, :, mine], b.at[6:8, :, mine], "P")]
        if n in ("WuP2", "WdP2"):
            b = wus if n == "WuP2" else wds
            return [(b.at[4:6, :, mine], b.at[4:6, :, mine], "P")]
        if n[:2] == "GP":
            r = int(n[2])
            return [(GF.at[:, r, :, theirs], GP.at[:, r], "P")]
        if n[:2] == "XP":
            r = int(n[2])
            return [(XF.at[0, r], XP.at[r], "P")]
        if n[:2] == "HP":
            r = int(n[2])
            return [(hbuf.at[r], HP.at[r], "P")]
        if n[:3] == "dCP":
            r = int(n[3])
            return [(DF.at[:, r, :, theirs], DP.at[:, r], "P")]
        if n[:2] == "dC":
            r = int(n[2])
            s = dct.at[r % 2]
            return [(s, DF.at[3, r], "R"), (s, DF.at[1, r], "L"), (s, DF.at[0, r], None)]
        if n[:3] == "rdC":
            r = int(n[3])
            first, second = pl.ds(0, grp // 2), pl.ds(grp // 2, grp // 2)
            return [(DF.at[3, r, first], DF.at[2, r, first], "R"), (DF.at[1, r, second], DF.at[2, r, second], "L")]
        if n[:2] == "q2":
            r = int(n[3])
            f = ft.at[r % 2]
            return [(f.at[0, K(2)], rst.at[r, 0], "U"), (f.at[1, K(2)], rst.at[r, 1], "N")]
        if n[:2] == "qd":
            r = int(n[3])
            f = ft.at[r % 2]
            return [(f.at[1, K(1)], rrc.at[r, 0, 1], "U"), (f.at[0, K(3)], rrc.at[r, 1, 0], "N")]
        if n[:2] == "qs":
            r = int(n[3])
            f = ft.at[r % 2]
            return [(f.at[0, K(1)], rrc.at[r, 0, 0], "U"), (f.at[1, K(3)], rrc.at[r, 1, 1], "N")]
        if n[:3] == "l1_" or n[:3] == "l2_" or n[:3] == "l3_":
            r = int(n[3])
            b = {"1": XF, "2": GF, "3": DF}[n[1]]
            return [(b.at[:, r], pan.at[slot_of[n]], None)]
        if n[:3] == "l5_" or n[:3] == "l4_":
            j = int(n[3])
            b, p = (GF, GP) if n[1] == "5" else (DF, DP)
            s = pan.at[slot_of[n]]
            return [(b.at[j, :, :, mine], s.at[:, :, lo], None), (p.at[j], s.at[:, :, hi], None)]
        if n == "lh":
            return [(HP, wds.at[0:4], None)]
        if n == "lx":
            return [(XF.at[0], wus.at[0:4], None), (XP, wus.at[4:8], None)]
        if n == "w2":
            return [(obuf.at[2, 0], sw.at[0], "R"), (obuf.at[2, 1], sw.at[1], "L")]
        if n == "w1":
            return [(obuf.at[1], dwd.at[:, x], "R"), (obuf.at[3], dwd.at[:, x], "L")]
        if n == "rw":
            return [(sw.at[0], dwd.at[0, at(3)], "R"), (sw.at[1], dwd.at[1, at(1)], "L")]
        raise ValueError(n)

    def total(terms):
        out = None
        for a, b, dims in terms:
            d = lax.dot_general(a, b, dims, preferred_element_type=jnp.float32)
            out = d if out is None else out + d
        return out

    def tiles(body):
        def step(i, carry):
            body(i)
            return carry
        lax.fori_loop(0, 2, step, 0)

    def unit(n):
        kind, i = n[:2], int(n[3])
        if kind == "m1":
            p = pan.at[slot_of[f"l1_{i}"]]

            def body(t):
                ns = pl.ds(pl.multiple_of(t * sub, sub), sub)
                s = total([(p[j, :, h * dh:(h + 1) * dh], wus[2 * j + h, :, ns], NN) for j in range(RING) for h in range(2)])
                hbuf[i, :, ns] = s.astype(jnp.bfloat16)
            tiles(body)
        if kind == "m2":
            p = pan.at[slot_of[f"l2_{i}"]]
            if i >= 2:
                cp.left(f"dC{i - 2}")
            d = dct.at[i % 2]

            def body(t):
                ns = pl.ds(pl.multiple_of(t * sub, sub), sub)
                acc[...] = total([(p[j], wds[2 * j + t], NT) for j in range(RING)])
                step = min(32, grp)

                def elem(e, carry):
                    rs = pl.ds(pl.multiple_of(e * step, step), step)
                    g, s = gelu_parts(hbuf[i, rs, ns].astype(jnp.float32))
                    hbuf[i, rs, ns] = g.astype(jnp.bfloat16)
                    d[rs, ns] = (acc[rs, :] * s).astype(jnp.bfloat16)
                    return carry
                lax.fori_loop(0, grp // step, elem, 0)
            tiles(body)
        if kind == "m3":
            p = pan.at[slot_of[f"l3_{i}"]]
            if i >= 2:
                for q in ("q2", "qd", "qs"):
                    cp.left(f"{q}_{i - 2}")
            f = ft.at[i % 2]

            def body(t):
                f[t] = total([(p[j], wun[2 * j + t], NT) for j in range(RING)])
            tiles(body)
        if kind == "m5" or kind == "m4":
            p = pan.at[slot_of[f"l{kind[1]}_{i}"]]
            own, par = (hbuf, wds) if kind == "m5" else (wus, wus.at[4:8])
            if kind == "m4" and i == 0:
                for r in range(NR):
                    cp.left(f"HP{r}")

            def body(t):
                ms = pl.ds(pl.multiple_of(t * dh, dh), dh)
                s = total([(own[r, :, ms], p[r, :, lo], TN) for r in range(NR)] + [(par[r, :, ms], p[r, :, hi], TN) for r in range(NR)])
                if kind == "m5":
                    obuf[i, t] = s.astype(jnp.bfloat16)
                else:
                    hbuf[i, :, ms] = s.astype(jnp.bfloat16)
            tiles(body)
            if kind == "m5" and i == 0:
                cp.add("out5", [(obuf.at[0], dwd.at[:, x], None)])
            if kind == "m4":
                cp.add(f"out4_{i}", [(hbuf.at[i, :, h * dh:(h + 1) * dh], dwu.at[h, :, cols(i)], None) for h in range(2)])
        if kind == "qa":
            f = ft.at[i % 2]
            f[0, K(1), :] = f[0, K(1), :] + rst[i, 0]
            f[1, K(3), :] = f[1, K(3), :] + rst[i, 1]
        if kind == "qf":
            f = ft.at[i % 2]
            for h in range(2):
                xo[i, :, h * dh:(h + 1) * dh] = (f[h, K(0), :] + rrc[i, 0, h] + rrc[i, 1, h]).astype(jnp.bfloat16)
            cp.add(f"outx_{i}", [(xo.at[i], dx.at[i], None)])

    deps = {n: d for n, (_, _, d) in it.items()}
    deps.update({u[0]: u[2] for u in units})
    for n, _ in order:
        for d in deps[n]:
            cp.arrived(d)
        if n == "own":
            b0, b1 = pan.at[0, :, K(0)], pan.at[1, :, K(0)]
            cp.add("own0", [(xa, b0, None), (za, b1, None)])
            cp.arrived("own0")
            cp.add("own", [(b0, XF.at[0, :, K(0)], None), (b1, GF.at[0, :, K(0)], None)])
        elif n in it:
            if n == "lx":
                for w in ("WuP0", "WuP1", "WuP2"):
                    cp.left(w)
            if n == "lh":
                for w in ("WdP0", "WdP1", "WdP2"):
                    cp.left(w)
            cp.add(n, copies_of(n))
        else:
            unit(n)
    cp.finish()
    assert cp.n_remote <= N_REMOTE and cp.n_local <= N_LOCAL, (cp.n_remote, cp.n_local)


def solution(mesh):
    assert mesh.shape["cy"] == RING and mesh.shape["cz"] == RING and mesh.shape["cx"] == CORES
    row_spec = P(("dp", "cx", "cz"), "cy")
    up_spec = P("cy", ("cz", "cx"))
    down_spec = P("cz", ("cy", "cx"))
    up_out = P(("dp", "cy"), ("cz", "cx"))
    down_out = P(("dp", "cz"), ("cy", "cx"))
    plan = make_plan()
    order, panels, _ = make_order(*plan)

    def local_step(x_act, w_up, w_down, z_grad):
        t_loc, d_loc = x_act.shape
        f_loc = w_up.shape[1]
        rows, sub, dh = t_loc // NR, f_loc // RING, d_loc // 2
        grp = RING * rows
        bf, f32 = jnp.bfloat16, jnp.float32
        xa, za = x_act.reshape(NR, rows, d_loc), z_grad.reshape(NR, rows, d_loc)
        wu = w_up.reshape(2, dh, f_loc)
        wd = w_down.reshape(CORES, RING, sub, dh)
        hbm = lambda *s: jax.ShapeDtypeStruct(s, bf)
        outs = (
            hbm(NR, rows, d_loc), hbm(2, dh, f_loc), hbm(CORES, RING, sub, dh),
            hbm(RING, NR, grp, d_loc), hbm(RING, NR, grp, d_loc), hbm(RING, NR, grp, 2 * sub),
            hbm(RING, NR, grp, sub), hbm(RING, NR, grp, sub), hbm(NR, grp, d_loc), hbm(NR, grp, 2 * sub),
            hbm(2, dh, sub), hbm(2, sub, dh), hbm(2, sub, dh),
        )
        scratch = [
            pltpu.VMEM((2 * RING, dh, 2 * sub), bf), pltpu.VMEM((2 * RING, sub, d_loc), bf), pltpu.VMEM((2 * RING, dh, 2 * sub), bf),
            pltpu.VMEM((NR, grp, 2 * sub), bf), pltpu.VMEM((PAN, RING, grp, d_loc), bf),
            pltpu.VMEM((2, 2, grp, dh), f32), pltpu.VMEM((2, grp, 2 * sub), bf),
            pltpu.VMEM((NR, 2, rows, dh), f32), pltpu.VMEM((NR, 2, 2, rows, dh), f32),
            pltpu.VMEM((RING, CORES, sub, dh), bf), pltpu.VMEM((NR, rows, d_loc), bf),
            pltpu.VMEM((grp, sub), f32),
            pltpu.SemaphoreType.DMA((N_REMOTE,)), pltpu.SemaphoreType.DMA((N_REMOTE,)), pltpu.SemaphoreType.DMA((N_LOCAL,)),
        ]
        any_spec = pl.BlockSpec(memory_space=pl.ANY)
        res = pl.pallas_call(
            functools.partial(kernel, plan, order, panels),
            out_shape=outs,
            in_specs=[any_spec] * 4,
            out_specs=[any_spec] * len(outs),
            scratch_shapes=scratch,
            compiler_params=pltpu.CompilerParams(collective_id=0, has_side_effects=True, vmem_limit_bytes=67043328),
            name="mlp_bwd",
        )(xa, wu, wd, za)
        return (res[0].reshape(t_loc, d_loc), res[1].reshape(w_up.shape), res[2].reshape(w_down.shape))

    return jax.shard_map(local_step, mesh=mesh, in_specs=(row_spec, up_spec, down_spec, row_spec), out_specs=(row_spec, up_out, down_out), check_vma=False)
```

```python
import functools
import math

import jax
import jax.numpy as jnp
from jax import lax
from jax.experimental import pallas as pl
from jax.experimental.pallas import tpu as pltpu
from jax.sharding import PartitionSpec as P

GELU_COEF = 0.044715
SQRT_TWO_PI = math.sqrt(2.0 / math.pi)
NN = (((1,), (0,)), ((), ()))
NT = (((1,), (1,)), ((), ()))
TN = (((0,), (0,)), ((), ()))
MESH = pl.DeviceIdType.MESH
RING = 4
CORES = 2
PAN = 3
GROUPS = ((0, 0, 8), (1, 0, 8), (2, 0, 8), (3, 0, 4), (3, 4, 4))
NB = 4
NG = len(GROUPS)
EARLY = 2
X, G = 0, 1


def gelu_parts(pre_act):
    inner_arg = SQRT_TWO_PI * (pre_act + GELU_COEF * pre_act * pre_act * pre_act)
    tanh_val = jnp.tanh(inner_arg)
    gelu_val = 0.5 * pre_act * (1.0 + tanh_val)
    gelu_slope = 0.5 * (1.0 + tanh_val) + 0.5 * pre_act * (1.0 - tanh_val * tanh_val) * SQRT_TWO_PI * (1.0 + 3.0 * GELU_COEF * pre_act * pre_act)
    return gelu_val, gelu_slope


(XS, XR, W2, W1, WR, CS, CR, O2, O1, OR, YA, YB, YF, YR, Q2, QD, QS, WN, WP, GP, XP, HP, CP,
 OWN, L1, L2, L3, L4, L5, LX, LH, M1, M2, M3, M4, M5, QA, QF, OUT) = range(39)
PANEL_OF = {L1: M1, L2: M2, L3: M3, L4: M4, L5: M5}
O5 = (2, 0, 1, 3)
O4 = (0, 1, 2, 3)


def full(a, r):
    return [(XS, a, r), (XR, a, r), (YR, a, r), (OWN, 0, 0)] + ([(YA, a, r), (YB, a, r)] if r < EARLY else [(YF, a, r)])


def make_plan():
    it, un = {}, {}
    groups = range(NG)
    for r in groups:
        q = GROUPS[r][2] / 8 / NB
        f = 4 * q
        for a in (X, G):
            it[XS, a, r] = (0, q, [])
            it[XR, a, r] = (0, q / 2, [(XS, a, r)])
            row = [(XS, a, r), (XR, a, r)]
            if r < EARLY:
                it[YA, a, r] = (1, q, [])
                it[YB, a, r] = (1, 3 * q, row)
                it[YR, a, r] = (1, 2 * q, [(YA, a, r), (YB, a, r)])
            else:
                it[YF, a, r] = (1, 4 * q, row + [(OWN, 0, 0)])
                it[YR, a, r] = (1, 2 * q, [(YF, a, r)])
        it[GP, 0, r] = (2, 8 * q, full(G, r))
        it[XP, 0, r] = (2, 4 * q, full(X, r))
        it[HP, 0, r] = (2, 4 * q, [(M2, 0, r)])
        it[CS, 0, r] = (0, 4 * q, [(M2, 0, r)])
        it[CR, 0, r] = (0, 2 * q, [(CS, 0, r)])
        dc = [(CS, 0, r), (CR, 0, r)]
        it[CP, 0, r] = (2, 8 * q, dc)
        it[Q2, 0, r] = (1, q, [(M3, 0, r)])
        it[QD, 0, r] = (1, q, [(M3, 0, r)])
        it[QS, 0, r] = (1, q, [(QA, 0, r)])
        it[L1, 0, r] = (3, 16 * q, full(X, r))
        it[L2, 0, r] = (3, 16 * q, full(G, r))
        it[L3, 0, r] = (3, 16 * q, dc)
        wu = [(WP, 0, p) for p in range(3)]
        wd = [(WP, 1, p) for p in range(3)]
        un[M1, 0, r] = (0.4 + 4.4 * f, [(L1, 0, r)] + wu)
        un[M2, 0, r] = (0.4 + 6.2 * f, [(L2, 0, r), (M1, 0, r)] + wd)
        un[M3, 0, r] = (0.4 + 4.4 * f, [(L3, 0, r), (WN, 0, 0)] + ([(QF, 0, r - 2)] if r >= 2 else []))
        un[QA, 0, r] = (0.1 + 0.4 * f, [(Q2, 0, r)])
        un[QF, 0, r] = (0.1 + 0.4 * f, [(QS, 0, r), (QD, 0, r)])
    for w in range(2):
        it[W2, 0, w] = (0, 0.5, [])
        it[W1, 0, w] = (0, 1.0, [])
        it[WR, 0, w] = (0, 0.5, [(W2, 0, w)])
        it[WP, w, 0] = (2, 1, [])
        it[WP, w, 1] = (2, 2, [(W1, 0, w)])
        it[WP, w, 2] = (2, 1, [(WR, 0, w)])
    it[WN, 0, 0] = (2, 4, [])
    it[OWN, 0, 0] = (3, 2, [])
    it[O2, 0, 0] = (0, 0.5, [(M5, 0, 0)])
    it[O1, 0, 0] = (0, 1.0, [(M5, 0, 1)])
    it[OR, 0, 0] = (0, 0.5, [(O2, 0, 0)])
    for p in range(RING):
        it[L5, 0, p] = (3, 4, [(GP, 0, r) for r in groups] + sum([full(G, r) for r in groups], []))
        it[L4, 0, p] = (3, 4, [(CP, 0, r) for r in groups] + [(CR, 0, r) for r in groups])
    it[LH, 0, 0] = (3, 4, [(HP, 0, r) for r in groups] + [(M2, 0, r) for r in groups])
    it[LX, 0, 0] = (3, 8, [(XP, 0, r) for r in groups] + [(M1, 0, r) for r in groups])
    for p in range(2):
        un[M5, 0, p] = (9.6, [(L5, 0, 2 * p), (L5, 0, 2 * p + 1), (LH, 0, 0)])
        un[M4, 0, p] = (9.6, [(L4, 0, 2 * p), (L4, 0, 2 * p + 1), (LX, 0, 0), (M5, 0, 0), (M5, 0, 1)])
    return it, un


def make_lists():
    over_cy = [
        (XS, 0, 0), (XS, 1, 1), (XR, 0, 0), (XS, 0, 1), (XR, 1, 1), (XS, 1, 2), (XS, 0, 3), (XS, 1, 0), (XS, 0, 2),
        (XR, 0, 1), (XR, 1, 2), (XR, 1, 0), (W2, 0, 0), (W1, 0, 1), (W2, 0, 1), (W1, 0, 0), (XR, 0, 2), (WR, 0, 0),
        (WR, 0, 1), (XS, 1, 4), (XS, 1, 3), (XS, 0, 4), (XR, 1, 4), (XR, 0, 3), (XR, 1, 3), (CS, 0, 0), (CS, 0, 1),
        (XR, 0, 4), (CR, 0, 0), (CS, 0, 2), (CR, 0, 1), (CS, 0, 3), (CR, 0, 2), (CR, 0, 3), (CS, 0, 4), (O2, 0, 0),
        (CR, 0, 4), (OR, 0, 0), (O1, 0, 0),
    ]
    over_cz = [
        (YA, 1, 0), (YA, 1, 1), (YA, 0, 0), (YA, 0, 1), (YB, 0, 0), (YB, 1, 1), (YR, 0, 0), (YB, 0, 1), (YB, 1, 0),
        (YR, 0, 1), (YR, 1, 0), (YF, 1, 2), (YR, 1, 1), (YF, 0, 2), (YR, 1, 2), (YR, 0, 2), (YF, 1, 3), (YF, 0, 3),
        (YR, 1, 3), (YR, 0, 3), (YF, 0, 4), (YF, 1, 4), (YR, 0, 4), (YR, 1, 4), (Q2, 0, 1), (Q2, 0, 0), (QD, 0, 0),
        (QS, 0, 0), (QS, 0, 1), (QD, 0, 1), (Q2, 0, 2), (QD, 0, 2), (QS, 0, 2), (Q2, 0, 4), (Q2, 0, 3), (QD, 0, 3),
        (QS, 0, 3), (QS, 0, 4), (QD, 0, 4),
    ]
    units = [
        (QF, 0, 3), (QA, 0, 0), (M3, 0, 1), (M4, 0, 0), (M5, 0, 0), (M1, 0, 0), (M2, 0, 0), (QA, 0, 2), (QF, 0, 0),
        (QF, 0, 4), (M3, 0, 2), (M3, 0, 0), (M4, 0, 1), (QF, 0, 2), (M2, 0, 2), (M1, 0, 2), (M1, 0, 1), (M2, 0, 3),
        (M2, 0, 1), (M5, 0, 1), (M1, 0, 4), (M3, 0, 3), (M3, 0, 4), (M2, 0, 4), (QA, 0, 1), (QF, 0, 1), (M1, 0, 3),
        (QA, 0, 4), (QA, 0, 3),
    ]
    return [over_cy, over_cz], units


RATE = (22.5, 22.5, 1.7, 0.4)
DELAY = (3.0, 3.0, 1.5, 1.5)


def make_order(plan, lists, units):
    it, un = plan
    done, free, pos = {}, [0.0] * 4, [0] * 4
    pend, now, order, panels, waits = list(units), 0.0, [], [], []
    late = [n for n in it if it[n][0] >= 2]
    rank = {u: i for i, u in enumerate(units)}
    panel_rank = lambda n: rank[PANEL_OF[n[0]], 0, n[2] // 2 if n[0] in (L4, L5) else n[2]] if n[0] in PANEL_OF else -1
    through = lambda n: (PANEL_OF[n[0]], 0, n[2] // 2 if n[0] in (L4, L5) else n[2]) in gone
    gone = set()
    big = 1e9

    def ready(n):
        return all(done.get(d, big) <= now for d in it[n][2])

    def send(n):
        k = it[n][0]
        start = max(now + 0.3, free[k])
        waits.append((k, start - free[k], n))
        free[k] = start + it[n][1] * RATE[k]
        done[n] = free[k] + DELAY[k]
        order.append(n)

    while True:
        for k in (0, 1):
            while pos[k] < len(lists[k]) and ready(lists[k][pos[k]]):
                send(lists[k][pos[k]])
                pos[k] += 1
        for n in sorted((n for n in late if ready(n)), key=lambda n: (panel_rank(n), n)):
            if n[0] in PANEL_OF:
                if len(panels) >= PAN and not through(panels[-PAN]):
                    continue
                panels.append(n)
            late.remove(n)
            send(n)
        can = [u for u in pend if all(done.get(d, big) <= now for d in un[u][1])]
        if can:
            pend.remove(can[0])
            order.append(can[0])
            now += un[can[0]][0]
            done[can[0]] = now
            gone.add(can[0])
            continue
        later = [v for v in done.values() if v > now]
        if not later:
            break
        now = min(later)
    assert not pend and not late and all(pos[k] == len(lists[k]) for k in (0, 1)), (pend, late, pos)
    return order, panels, max(done.values()), waits


class Copies:
    def __init__(self, send, recv, local, peers):
        self.send, self.recv, self.local, self.peers = send, recv, local, peers
        self.n_remote = self.n_local = 0
        self.by_name = {}

    def add(self, name, pairs):
        made = []
        for src, dst, to in pairs:
            if to is None:
                c = pltpu.make_async_copy(src, dst, self.local.at[self.n_local])
                self.n_local += 1
            else:
                axis, idx = self.peers[to]
                c = pltpu.make_async_remote_copy(
                    src, dst, self.send.at[self.n_remote], self.recv.at[self.n_remote],
                    device_id={axis: idx}, device_id_type=MESH)
                self.n_remote += 1
            made.append([c, to, False, False])
            c.start()
        self.by_name.setdefault(name, []).extend(made)

    def arrived(self, name):
        for m in self.by_name.get(name, ()):
            if not m[2]:
                m[2] = True
                m[0].wait() if m[1] is None else m[0].wait_recv()

    def left(self, name):
        for m in self.by_name.get(name, ()):
            if m[1] is None:
                if not m[2]:
                    m[2] = True
                    m[0].wait()
            elif not m[3]:
                m[3] = True
                m[0].wait_send()

    def finish(self):
        for name in list(self.by_name):
            self.arrived(name)
            self.left(name)


N_REMOTE = 196
N_LOCAL = 80


def kernel(plan, order, panels, xa, wu, wd, za, dx, dwu, dwd, XF, GF, DF, GPB, DPB, XPB, HPB, su, sd, sw,
           wus, wds, wun, hbuf, pan, ft, dct, rst, rrc, obuf, xo, acc, send, recv, local):
    it, un = plan
    x, y, c = lax.axis_index("cy"), lax.axis_index("cz"), lax.axis_index("cx")
    peers = {
        "R": ("cy", lax.rem(x + 1, RING)), "L": ("cy", lax.rem(x + RING - 1, RING)),
        "U": ("cz", lax.rem(y + 1, RING)), "N": ("cz", lax.rem(y + RING - 1, RING)),
        "P": ("cx", 1 - c),
    }
    barrier = pltpu.get_barrier_semaphore()
    for axis, idx in peers.values():
        pl.semaphore_signal(barrier, inc=1, device_id={axis: idx}, device_id_type=MESH)
    pl.semaphore_wait(barrier, len(peers))

    cp = Copies(send, recv, local, peers)
    blk_rows = xa.shape[1]
    sub = wd.shape[2]
    dh = wu.shape[1]
    mine = pl.ds(pl.multiple_of(c * sub, sub), sub)
    theirs = pl.ds(pl.multiple_of((1 - c) * sub, sub), sub)
    lo, hi = pl.ds(0, sub), pl.ds(sub, sub)
    at = lambda j: lax.rem(x + j, RING)
    cols = lambda j: pl.ds(pl.multiple_of(at(j) * sub, sub), sub)
    slot_of = {n: i % PAN for i, n in enumerate(panels)}
    inp, buf = (xa, za), (XF, GF)

    def group(r):
        b, first, n = GROUPS[r]
        unit_rows = blk_rows // 8
        return b, first * unit_rows, n * unit_rows

    def rel(r, k, part=None):
        _, first, n = group(r)
        start = RING * first + k * n
        return pl.ds(start, n) if part is None else pl.ds(start + part * (n // 2), n // 2)

    def span(r):
        _, first, n = group(r)
        return pl.ds(RING * first, RING * n)

    def copies_of(name):
        kind, a, r = name
        both = lambda right, left: [right + ("R",), left + ("L",)]
        updn = lambda up, down: [up + ("U",), down + ("N",)]
        if kind == WN:
            return sum([[(wu.at[:, :, cols(j)], wun.at[2 * j:2 * j + 2, :, mine], to) for to in (None, "P")] for j in range(RING)], [])
        if kind == XS or kind == YA:
            b, first, n = group(r)
            src = inp[a].at[b, pl.ds(first, n)]
            if kind == XS:
                return both((src, buf[a].at[3, b, rel(r, 0)]), (src, buf[a].at[1, b, rel(r, 0)]))
            return updn((src, buf[a].at[0, b, rel(r, 3)]), (src, buf[a].at[0, b, rel(r, 1)]))
        if kind == XR:
            b, f, s = group(r)[0], rel(r, 0, 0), rel(r, 0, 1)
            return both((buf[a].at[3, b, f], buf[a].at[2, b, f]), (buf[a].at[1, b, s], buf[a].at[2, b, s]))
        if kind in (YB, YF):
            b, m = group(r)[0], buf[a]
            js = pl.ds(1, RING - 1) if kind == YB else pl.ds(0, RING)
            return updn((m.at[js, b, rel(r, 0)], m.at[js, b, rel(r, 3)]), (m.at[js, b, rel(r, 0)], m.at[js, b, rel(r, 1)]))
        if kind == YR:
            b, m = group(r)[0], buf[a]
            return updn((m.at[0:2, b, rel(r, 3)], m.at[0:2, b, rel(r, 2)]), (m.at[2:4, b, rel(r, 1)], m.at[2:4, b, rel(r, 2)]))
        if kind in (W2, W1, WR):
            half = (lambda h, j: wu.at[h, :, cols(j)]) if r == 0 else (lambda h, j: wd.at[h, at(j)])
            piece = (lambda j: wu.at[:, :, cols(j)]) if r == 0 else (lambda j: wd.at[:, at(j)])
            st, dst = (su, sd)[r], (wus, wds)[r]
            if kind == W2:
                return both((half(0, 2), st.at[0]), (half(1, 2), st.at[1]))
            if kind == W1:
                return both((piece(1), dst.at[6:8, :, mine]), (piece(3), dst.at[2:4, :, mine]))
            return both((st.at[0], dst.at[4, :, mine]), (st.at[1], dst.at[5, :, mine]))
        if kind == WP:
            m = (wus, wds)[a]
            if r == 0:
                src = wu.at[:, :, cols(0)] if a == 0 else wd.at[:, at(0)]
                return [(src, m.at[0:2, :, mine], to) for to in (None, "P")]
            return [(m.at[2 * j:2 * j + 2, :, mine], m.at[2 * j:2 * j + 2, :, mine], "P") for j in ((1, 3) if r == 1 else (2,))]
        if kind == GP:
            return [(GF.at[:, group(r)[0], span(r), theirs], GPB.at[:, group(r)[0], span(r)], "P")]
        if kind == XP:
            return [(XF.at[0, group(r)[0], span(r)], XPB.at[group(r)[0], span(r)], "P")]
        if kind == HP:
            return [(hbuf.at[group(r)[0], span(r)], HPB.at[group(r)[0], span(r)], "P")]
        if kind == CP:
            return [(DF.at[:, group(r)[0], span(r), theirs], DPB.at[:, group(r)[0], span(r)], "P")]
        if kind == CS:
            b, _, n = group(r)
            s = dct.at[r % 2, pl.ds(0, RING * n)]
            return both((s, DF.at[3, b, span(r)]), (s, DF.at[1, b, span(r)])) + [(s, DF.at[0, b, span(r)], None)]
        if kind == CR:
            b, first, n = group(r)
            f, s = (pl.ds(RING * first + h * 2 * n, 2 * n) for h in range(2))
            return both((DF.at[3, b, f], DF.at[2, b, f]), (DF.at[1, b, s], DF.at[2, b, s]))
        if kind in (Q2, QD, QS):
            b, first, n = group(r)
            f = ft.at[r % 2]
            own = lambda k: pl.ds(k * n, n)
            rs = pl.ds(first, n)
            if kind == Q2:
                return updn((f.at[0, own(2)], rst.at[b, 0, rs]), (f.at[1, own(2)], rst.at[b, 1, rs]))
            if kind == QD:
                return updn((f.at[1, own(1)], rrc.at[b, 0, 1, rs]), (f.at[0, own(3)], rrc.at[b, 1, 0, rs]))
            return updn((f.at[0, own(1)], rrc.at[b, 0, 0, rs]), (f.at[1, own(3)], rrc.at[b, 1, 1, rs]))
        if kind in (L1, L2, L3):
            b, _, n = group(r)
            m = {L1: XF, L2: GF, L3: DF}[kind]
            return [(m.at[:, b, span(r)], pan.at[slot_of[name], :, pl.ds(0, RING * n)], None)]
        if kind in (L5, L4):
            m, p, j = (GF, GPB, O5[r]) if kind == L5 else (DF, DPB, O4[r])
            s = pan.at[slot_of[name]]
            return [(m.at[j, :, :, mine], s.at[:, :, lo], None), (p.at[j], s.at[:, :, hi], None)]
        if kind == LH:
            return [(HPB, wds.at[0:4], None)]
        if kind == LX:
            return [(XF.at[0], wus.at[0:4], None), (XPB, wus.at[4:8], None)]
        place = {j: i for i, j in enumerate(O5)}
        if kind == O2:
            return both((obuf.at[place[2], 0], sw.at[0]), (obuf.at[place[2], 1], sw.at[1]))
        if kind == O1:
            return both((obuf.at[place[1]], dwd.at[:, x]), (obuf.at[place[3]], dwd.at[:, x]))
        assert kind == OR
        return both((sw.at[0], dwd.at[0, at(3)]), (sw.at[1], dwd.at[1, at(1)]))

    def total(terms):
        out = None
        for a, b, dims in terms:
            d = lax.dot_general(a, b, dims, preferred_element_type=jnp.float32)
            out = d if out is None else out + d
        return out

    def loop(n, body):
        def step(i, carry):
            body(i)
            return carry
        lax.fori_loop(0, n, step, 0)

    def unit(name):
        kind, _, r = name
        if kind in (M1, M2, M3):
            b, first, n = group(r)
            rows = pl.ds(0, RING * n)
        if kind == M1:
            p = pan.at[slot_of[L1, 0, r]]

            def body(t):
                ns = pl.ds(pl.multiple_of(t * sub, sub), sub)
                s = total([(p[j, rows, h * dh:(h + 1) * dh], wus[2 * j + h, :, ns], NN) for j in range(RING) for h in range(2)])
                hbuf[b, span(r), ns] = s.astype(jnp.bfloat16)
            loop(2, body)
        elif kind == M2:
            p = pan.at[slot_of[L2, 0, r]]
            if r >= 2:
                cp.left((CS, 0, r - 2))
            d = dct.at[r % 2]
            step = min(32, RING * n)

            def body(t):
                ns = pl.ds(pl.multiple_of(t * sub, sub), sub)
                acc[rows, :] = total([(p[j, rows, :], wds[2 * j + t], NT) for j in range(RING)])

                def elem(e):
                    rs = pl.ds(pl.multiple_of(e * step, step), step)
                    hs = pl.ds(pl.multiple_of(RING * first + e * step, step), step)
                    g, s = gelu_parts(hbuf[b, hs, ns].astype(jnp.float32))
                    hbuf[b, hs, ns] = g.astype(jnp.bfloat16)
                    d[rs, ns] = (acc[rs, :] * s).astype(jnp.bfloat16)
                loop(RING * n // step, elem)
            loop(2, body)
        elif kind == M3:
            p = pan.at[slot_of[L3, 0, r]]
            if r >= 2:
                for q in (Q2, QD, QS):
                    cp.left((q, 0, r - 2))
            f = ft.at[r % 2]

            def body(t):
                f[t, rows, :] = total([(p[j, rows, :], wun[2 * j + t], NT) for j in range(RING)])
            loop(2, body)
        elif kind in (M5, M4):
            ld = L5 if kind == M5 else L4
            s0, s1 = slot_of[ld, 0, 2 * r], slot_of[ld, 0, 2 * r + 1]
            own, par = (hbuf, wds) if kind == M5 else (wus, wus.at[4:8])
            if kind == M4 and r == 0:
                for g in range(NG):
                    cp.left((HP, 0, g))

            def body(i):
                e, t = i // 2, lax.rem(i, 2)
                p = pan.at[s0 + e * (s1 - s0)]
                ms = pl.ds(pl.multiple_of(t * dh, dh), dh)
                s = total([(own[g, :, ms], p[g, :, lo], TN) for g in range(NB)] + [(par[g, :, ms], p[g, :, hi], TN) for g in range(NB)])
                if kind == M5:
                    obuf[2 * r + e, t] = s.astype(jnp.bfloat16)
                else:
                    hbuf[2 * r + e, :, ms] = s.astype(jnp.bfloat16)
            loop(4, body)
            for e in range(2):
                i = 2 * r + e
                if kind == M5 and O5[i] == 0:
                    cp.add((OUT, kind, i), [(obuf.at[i], dwd.at[:, x], None)])
                if kind == M4:
                    cp.add((OUT, kind, i), [(hbuf.at[i, :, h * dh:(h + 1) * dh], dwu.at[h, :, cols(O4[i])], None) for h in range(2)])
        else:
            b, first, n = group(r)
            f = ft.at[r % 2]
            rs = pl.ds(first, n)
            own = lambda k: pl.ds(k * n, n)
            if kind == QA:
                f[0, own(1), :] = f[0, own(1), :] + rst[b, 0, rs, :]
                f[1, own(3), :] = f[1, own(3), :] + rst[b, 1, rs, :]
            else:
                for h in range(2):
                    xo[b, rs, h * dh:(h + 1) * dh] = (f[h, own(0), :] + rrc[b, 0, h, rs, :] + rrc[b, 1, h, rs, :]).astype(jnp.bfloat16)
                cp.add((OUT, kind, r), [(xo.at[b, rs], dx.at[b, rs], None)])

    for name in order:
        for d in (it[name][2] if name in it else un[name][1]):
            cp.arrived(d)
        if name[0] == OWN:
            own = pl.ds(0, blk_rows)
            b0, b1 = pan.at[0, :, own], pan.at[1, :, own]
            cp.add((OUT, OWN, 0), [(xa, b0, None), (za, b1, None)])
            cp.arrived((OUT, OWN, 0))
            pairs = []
            for r in range(NG):
                b, first, n = group(r)
                pairs += [(pan.at[a, b, pl.ds(first, n)], buf[a].at[0, b, rel(r, 0)], None) for a in (X, G)]
            cp.add(name, pairs)
        elif name in it:
            for w in {LX: (0,), LH: (1,)}.get(name[0], ()):
                for p in range(3):
                    cp.left((WP, w, p))
            cp.add(name, copies_of(name))
        else:
            unit(name)
    cp.finish()
    assert cp.n_remote <= N_REMOTE and cp.n_local <= N_LOCAL, (cp.n_remote, cp.n_local)


def solution(mesh):
    assert mesh.shape["cy"] == RING and mesh.shape["cz"] == RING and mesh.shape["cx"] == CORES
    row_spec = P(("dp", "cx", "cz"), "cy")
    up_spec = P("cy", ("cz", "cx"))
    down_spec = P("cz", ("cy", "cx"))
    up_out = P(("dp", "cy"), ("cz", "cx"))
    down_out = P(("dp", "cz"), ("cy", "cx"))
    plan = make_plan()
    order, panels, _, _ = make_order(plan, *make_lists())

    def local_step(x_act, w_up, w_down, z_grad):
        t_loc, d_loc = x_act.shape
        f_loc = w_up.shape[1]
        rows, sub, dh = t_loc // NB, f_loc // RING, d_loc // 2
        grp = RING * rows
        bf, f32 = jnp.bfloat16, jnp.float32
        xa, za = x_act.reshape(NB, rows, d_loc), z_grad.reshape(NB, rows, d_loc)
        wu = w_up.reshape(2, dh, f_loc)
        wd = w_down.reshape(CORES, RING, sub, dh)
        hbm = lambda *s: jax.ShapeDtypeStruct(s, bf)
        outs = (
            hbm(NB, rows, d_loc), hbm(2, dh, f_loc), hbm(CORES, RING, sub, dh),
            hbm(RING, NB, grp, d_loc), hbm(RING, NB, grp, d_loc), hbm(RING, NB, grp, 2 * sub),
            hbm(RING, NB, grp, sub), hbm(RING, NB, grp, sub), hbm(NB, grp, d_loc), hbm(NB, grp, 2 * sub),
            hbm(2, dh, sub), hbm(2, sub, dh), hbm(2, sub, dh),
        )
        scratch = [
            pltpu.VMEM((2 * RING, dh, 2 * sub), bf), pltpu.VMEM((2 * RING, sub, d_loc), bf), pltpu.VMEM((2 * RING, dh, 2 * sub), bf),
            pltpu.VMEM((NB, grp, 2 * sub), bf), pltpu.VMEM((PAN, RING, grp, d_loc), bf),
            pltpu.VMEM((2, 2, grp, dh), f32), pltpu.VMEM((2, grp, 2 * sub), bf),
            pltpu.VMEM((NB, 2, rows, dh), f32), pltpu.VMEM((NB, 2, 2, rows, dh), f32),
            pltpu.VMEM((RING, CORES, sub, dh), bf), pltpu.VMEM((NB, rows, d_loc), bf),
            pltpu.VMEM((grp, sub), f32),
            pltpu.SemaphoreType.DMA((N_REMOTE,)), pltpu.SemaphoreType.DMA((N_REMOTE,)), pltpu.SemaphoreType.DMA((N_LOCAL,)),
        ]
        any_spec = pl.BlockSpec(memory_space=pl.ANY)
        res = pl.pallas_call(
            functools.partial(kernel, plan, order, panels),
            out_shape=outs,
            in_specs=[any_spec] * 4,
            out_specs=[any_spec] * len(outs),
            scratch_shapes=scratch,
            compiler_params=pltpu.CompilerParams(collective_id=0, has_side_effects=True, vmem_limit_bytes=67043328),
            name="mlp_bwd",
        )(xa, wu, wd, za)
        return (res[0].reshape(t_loc, d_loc), res[1].reshape(w_up.shape), res[2].reshape(w_down.shape))

    return jax.shard_map(local_step, mesh=mesh, in_specs=(row_spec, up_spec, down_spec, row_spec), out_specs=(row_spec, up_out, down_out), check_vma=False)
```

```python
import functools
import math
import string

import jax
import jax.numpy as jnp
from jax import lax
from jax.experimental import pallas as pl
from jax.experimental.pallas import tpu as pltpu
from jax.sharding import PartitionSpec as P

GELU_COEF = 0.044715
SQRT_TWO_PI = math.sqrt(2.0 / math.pi)
NN = (((1,), (0,)), ((), ()))
NT = (((1,), (1,)), ((), ()))
TN = (((0,), (0,)), ((), ()))
MESH = pl.DeviceIdType.MESH
RING = 4
CORES = 2
PAN = 3
GROUPS = ((0, 0, 8), (1, 0, 8), (2, 0, 8), (3, 0, 4), (3, 4, 4))
NB = 4
NG = len(GROUPS)
EARLY = 2
X, G = 0, 1


def gelu_parts(pre_act):
    inner_arg = SQRT_TWO_PI * (pre_act + GELU_COEF * pre_act * pre_act * pre_act)
    tanh_val = jnp.tanh(inner_arg)
    gelu_val = 0.5 * pre_act * (1.0 + tanh_val)
    gelu_slope = 0.5 * (1.0 + tanh_val) + 0.5 * pre_act * (1.0 - tanh_val * tanh_val) * SQRT_TWO_PI * (1.0 + 3.0 * GELU_COEF * pre_act * pre_act)
    return gelu_val, gelu_slope


(XS, XR, W2, W1, WR, CS, CR, O2, O1, OR, YA, YB, YF, YR, Q2, QD, QS, WN, WP, GP, XP, HP, CP,
 OWN, L1, L2, L3, L4, L5, LX, LH, M1, M2, M3, M4, M5, QA, QF, OUT) = range(39)
PANEL_OF = {L1: M1, L2: M2, L3: M3, L4: M4, L5: M5}
O5 = (2, 1, 3, 0)


def full(a, r):
    return [(XS, a, r), (XR, a, r), (YR, a, r), (OWN,)] + ([(YA, a, r), (YB, a, r)] if r < EARLY else [(YF, a, r)])


def make_plan():
    it, un = {}, {}
    groups = range(NG)
    for r in groups:
        q = GROUPS[r][2] / 8 / NB
        f = 4 * q
        for a in (X, G):
            it[XS, a, r] = (0, q, [])
            it[XR, a, r] = (0, q / 2, [(XS, a, r)])
            row = [(XS, a, r), (XR, a, r)]
            if r < EARLY:
                it[YA, a, r] = (1, q, [])
                it[YB, a, r] = (1, 3 * q, row)
                it[YR, a, r] = (1, 2 * q, [(YA, a, r), (YB, a, r)])
            else:
                it[YF, a, r] = (1, 4 * q, row + [(OWN,)])
                it[YR, a, r] = (1, 2 * q, [(YF, a, r)])
        it[GP, r] = (2, 8 * q, full(G, r))
        it[XP, r] = (2, 4 * q, full(X, r))
        it[HP, r] = (2, 4 * q, [(M2, r)])
        it[CS, r] = (0, 4 * q, [(M2, r)])
        it[CR, r] = (0, 2 * q, [(CS, r)])
        dc = [(CS, r), (CR, r)]
        it[CP, r] = (2, 8 * q, dc)
        it[Q2, r] = (1, q, [(M3, r)])
        it[QD, r] = (1, q, [(M3, r)])
        it[QS, r] = (1, q, [(QA, r)])
        it[L1, r] = (3, 16 * q, full(X, r))
        it[L2, r] = (3, 16 * q, full(G, r))
        it[L3, r] = (3, 16 * q, dc)
        wu = [(WP, 0, p) for p in range(3)]
        wd = [(WP, 1, p) for p in range(3)]
        un[M1, r] = (0.4 + 4.4 * f, [(L1, r)] + wu)
        un[M2, r] = (0.4 + 6.2 * f, [(L2, r), (M1, r)] + wd)
        un[M3, r] = (0.4 + 4.4 * f, [(L3, r), (WN,)] + ([(QF, r - 2)] if r >= 2 else []))
        un[QA, r] = (0.1 + 0.4 * f, [(Q2, r)])
        un[QF, r] = (0.1 + 0.4 * f, [(QS, r), (QD, r)])
    for w in range(2):
        it[W2, w] = (0, 0.5, [])
        it[W1, w] = (0, 1.0, [])
        it[WR, w] = (0, 0.5, [(W2, w)])
        it[WP, w, 0] = (2, 1, [])
        it[WP, w, 1] = (2, 2, [(W1, w)])
        it[WP, w, 2] = (2, 1, [(WR, w)])
    it[(WN,)] = (2, 4, [])
    it[(OWN,)] = (3, 2, [])
    it[(O2,)] = (0, 0.5, [(M5, 0)])
    it[(O1,)] = (0, 1.0, [(M5, 1), (M5, 2)])
    it[(OR,)] = (0, 0.5, [(O2,)])
    for p in range(RING):
        it[L5, p] = (3, 4, [(GP, r) for r in groups] + sum([full(G, r) for r in groups], []))
        it[L4, p] = (3, 4, [(CP, r) for r in groups] + [(CR, r) for r in groups])
    it[(LH,)] = (3, 4, [(HP, r) for r in groups] + [(M2, r) for r in groups])
    it[(LX,)] = (3, 8, [(XP, r) for r in groups] + [(M1, r) for r in groups])
    for p in range(RING):
        un[M5, p] = (4.9, [(L5, p), (LH,)])
    for p in range(2):
        un[M4, p] = (9.6, [(L4, 2 * p), (L4, 2 * p + 1), (LX,)])
    return it, un


def make_lists(keys=None):
    xs = lambda r: [(XS, X, r), (XS, G, r), (XR, X, r), (XR, G, r)]
    w = lambda i: [(W2, i), (W1, i), (WR, i)]
    y = lambda r: [(YF, X, r), (YF, G, r), (YR, X, r), (YR, G, r)]
    cs, cr = lambda r: [(CS, r)], lambda r: [(CR, r)]
    q = lambda r: [(Q2, r), (QD, r), (QS, r)]
    rest = range(4, NG)
    lists = [
        xs(0) + xs(1) + w(0) + xs(2) + w(1) + sum([xs(r) for r in range(3, NG)], []) + cs(0) + cs(1) + cr(0) + cr(1) + cs(2) + cr(2)
        + sum([cs(r) for r in range(3, NG)], []) + sum([cr(r) for r in range(3, NG)], []) + [(O2,), (O1,), (OR,)],
        [(YA, X, 0), (YA, G, 0), (YA, X, 1), (YA, G, 1), (YB, X, 0), (YB, G, 0), (YR, X, 0), (YR, G, 0), (YB, X, 1), (YB, G, 1), (YR, X, 1), (YR, G, 1)]
        + sum([y(r) for r in range(2, NG)], []) + sum([q(r) for r in range(NG)], []),
    ]
    units = []
    for r in range(NG):
        units += [(M2, r), (M1, r)]
    units += [(QA, r) for r in range(NG)] + [(QF, r) for r in range(NG)]
    units += [(M3, 0), (M3, 1)] + [(M5, p) for p in range(RING)] + [(M3, r) for r in range(2, NG)] + [(M4, 0), (M4, 1)]
    if keys is not None:
        lists[0], lists[1], units = ([base[string.ascii_letters.index(ch)] for ch in key] for base, key in zip(lists[:2] + [units], keys))
    return lists, units


ORDER = (
    "tafcewhbgpdlvixnjyrkqmsozAuBCDEGIFHKJLM",
    "abdcejfrhglimknopqtsuvwxyBzACDEFGHKJIML",
    "BmhownAsbpEjrlayvqDkcxdtgfCziue",
)

RATE = (22.5, 22.5, 1.7, 0.4)
DELAY = (3.0, 3.0, 1.5, 1.5)


def make_order(plan, lists, units):
    it, un = plan
    done, free, pos = {}, [0.0] * 4, [0] * 4
    pend, now, order, panels, waits = list(units), 0.0, [], [], []
    late = [n for n in it if it[n][0] >= 2]
    rank = {u: i for i, u in enumerate(units)}
    user = lambda n: (PANEL_OF[n[0]], n[1] // 2 if n[0] == L4 else n[1])
    panel_rank = lambda n: rank[user(n)] if n[0] in PANEL_OF else -1
    gone = set()
    big = 1e9

    def ready(n):
        return all(done.get(d, big) <= now for d in it[n][2])

    def send(n):
        k = it[n][0]
        start = max(now + 0.3, free[k])
        waits.append((k, start - free[k], n))
        free[k] = start + it[n][1] * RATE[k]
        done[n] = free[k] + DELAY[k]
        order.append(n)

    while True:
        for k in (0, 1):
            while pos[k] < len(lists[k]) and ready(lists[k][pos[k]]):
                send(lists[k][pos[k]])
                pos[k] += 1
        for n in sorted((n for n in late if ready(n)), key=lambda n: (panel_rank(n), n)):
            if n[0] in PANEL_OF:
                if len(panels) >= PAN and user(panels[-PAN]) not in gone:
                    continue
                panels.append(n)
            late.remove(n)
            send(n)
        can = [u for u in pend if all(done.get(d, big) <= now for d in un[u][1])]
        if can:
            pend.remove(can[0])
            order.append(can[0])
            now += un[can[0]][0]
            done[can[0]] = now
            gone.add(can[0])
            continue
        later = [v for v in done.values() if v > now]
        if not later:
            break
        now = min(later)
    assert not pend and not late and all(pos[k] == len(lists[k]) for k in (0, 1)), (pend, late, pos)
    return order, panels, max(done.values()), waits


class Copies:
    def __init__(self, send, recv, local, peers):
        self.send, self.recv, self.local, self.peers = send, recv, local, peers
        self.n_remote = self.n_local = 0
        self.by_name = {}

    def add(self, name, pairs):
        made = []
        for src, dst, to in pairs:
            if to is None:
                c = pltpu.make_async_copy(src, dst, self.local.at[self.n_local])
                self.n_local += 1
            else:
                axis, idx = self.peers[to]
                c = pltpu.make_async_remote_copy(
                    src, dst, self.send.at[self.n_remote], self.recv.at[self.n_remote],
                    device_id={axis: idx}, device_id_type=MESH)
                self.n_remote += 1
            made.append([c, to, False, False])
            c.start()
        self.by_name.setdefault(name, []).extend(made)

    def arrived(self, name):
        for m in self.by_name.get(name, ()):
            if not m[2]:
                m[2] = True
                m[0].wait() if m[1] is None else m[0].wait_recv()

    def left(self, name):
        for m in self.by_name.get(name, ()):
            if m[1] is None:
                if not m[2]:
                    m[2] = True
                    m[0].wait()
            elif not m[3]:
                m[3] = True
                m[0].wait_send()

    def finish(self):
        for name in list(self.by_name):
            self.arrived(name)
            self.left(name)


N_REMOTE = 196
N_LOCAL = 80


def kernel(plan, order, panels, xa, wu, wd, za, dx, dwu, dwd, XF, GF, DF, GPB, DPB, XPB, HPB, su, sd, sw,
           wus, wds, wun, hbuf, pan, ft, dct, rst, rrc, obuf, acc, send, recv, local):
    it, un = plan
    x, y, c = lax.axis_index("cy"), lax.axis_index("cz"), lax.axis_index("cx")
    peers = {
        "R": ("cy", lax.rem(x + 1, RING)), "L": ("cy", lax.rem(x + RING - 1, RING)),
        "U": ("cz", lax.rem(y + 1, RING)), "N": ("cz", lax.rem(y + RING - 1, RING)),
        "P": ("cx", 1 - c),
    }
    barrier = pltpu.get_barrier_semaphore()
    for axis, idx in peers.values():
        pl.semaphore_signal(barrier, inc=1, device_id={axis: idx}, device_id_type=MESH)
    pl.semaphore_wait(barrier, len(peers))

    cp = Copies(send, recv, local, peers)
    blk_rows = xa.shape[1]
    sub = wd.shape[2]
    dh = wu.shape[1]
    mine = pl.ds(pl.multiple_of(c * sub, sub), sub)
    theirs = pl.ds(pl.multiple_of((1 - c) * sub, sub), sub)
    lo, hi = pl.ds(0, sub), pl.ds(sub, sub)
    at = lambda j: lax.rem(x + j, RING)
    cols = lambda j: pl.ds(pl.multiple_of(at(j) * sub, sub), sub)
    slot_of = {n: i % PAN for i, n in enumerate(panels)}
    inp, buf = (xa, za), (XF, GF)

    def group(r):
        b, first, n = GROUPS[r]
        unit_rows = blk_rows // 8
        return b, first * unit_rows, n * unit_rows

    def rel(r, k, part=None):
        _, first, n = group(r)
        start = RING * first + k * n
        return pl.ds(start, n) if part is None else pl.ds(start + part * (n // 2), n // 2)

    def span(r):
        _, first, n = group(r)
        return pl.ds(RING * first, RING * n)

    def copies_of(name):
        kind, a, r = name[0], name[-2:][0], name[-1]
        both = lambda right, left: [right + ("R",), left + ("L",)]
        updn = lambda up, down: [up + ("U",), down + ("N",)]
        if kind == WN:
            return sum([[(wu.at[:, :, cols(j)], wun.at[2 * j:2 * j + 2, :, mine], to) for to in (None, "P")] for j in range(RING)], [])
        if kind == XS or kind == YA:
            b, first, n = group(r)
            src = inp[a].at[b, pl.ds(first, n)]
            if kind == XS:
                return both((src, buf[a].at[3, b, rel(r, 0)]), (src, buf[a].at[1, b, rel(r, 0)]))
            return updn((src, buf[a].at[0, b, rel(r, 3)]), (src, buf[a].at[0, b, rel(r, 1)]))
        if kind == XR:
            b, f, s = group(r)[0], rel(r, 0, 0), rel(r, 0, 1)
            return both((buf[a].at[3, b, f], buf[a].at[2, b, f]), (buf[a].at[1, b, s], buf[a].at[2, b, s]))
        if kind in (YB, YF):
            b, m = group(r)[0], buf[a]
            js = pl.ds(1, RING - 1) if kind == YB else pl.ds(0, RING)
            return updn((m.at[js, b, rel(r, 0)], m.at[js, b, rel(r, 3)]), (m.at[js, b, rel(r, 0)], m.at[js, b, rel(r, 1)]))
        if kind == YR:
            b, m = group(r)[0], buf[a]
            return updn((m.at[0:2, b, rel(r, 3)], m.at[0:2, b, rel(r, 2)]), (m.at[2:4, b, rel(r, 1)], m.at[2:4, b, rel(r, 2)]))
        if kind in (W2, W1, WR):
            half = (lambda h, j: wu.at[h, :, cols(j)]) if r == 0 else (lambda h, j: wd.at[h, at(j)])
            piece = (lambda j: wu.at[:, :, cols(j)]) if r == 0 else (lambda j: wd.at[:, at(j)])
            st, dst = (su, sd)[r], (wus, wds)[r]
            if kind == W2:
                return both((half(0, 2), st.at[0]), (half(1, 2), st.at[1]))
            if kind == W1:
                return both((piece(1), dst.at[6:8, :, mine]), (piece(3), dst.at[2:4, :, mine]))
            return both((st.at[0], dst.at[4, :, mine]), (st.at[1], dst.at[5, :, mine]))
        if kind == WP:
            m = (wus, wds)[a]
            if r == 0:
                src = wu.at[:, :, cols(0)] if a == 0 else wd.at[:, at(0)]
                return [(src, m.at[0:2, :, mine], to) for to in (None, "P")]
            return [(m.at[2 * j:2 * j + 2, :, mine], m.at[2 * j:2 * j + 2, :, mine], "P") for j in ((1, 3) if r == 1 else (2,))]
        if kind == GP:
            return [(GF.at[:, group(r)[0], span(r), theirs], GPB.at[:, group(r)[0], span(r)], "P")]
        if kind == XP:
            return [(XF.at[0, group(r)[0], span(r)], XPB.at[group(r)[0], span(r)], "P")]
        if kind == HP:
            return [(hbuf.at[group(r)[0], span(r)], HPB.at[group(r)[0], span(r)], "P")]
        if kind == CP:
            return [(DF.at[:, group(r)[0], span(r), theirs], DPB.at[:, group(r)[0], span(r)], "P")]
        if kind == CS:
            b, _, n = group(r)
            s = dct.at[r % 2, pl.ds(0, RING * n)]
            return both((s, DF.at[3, b, span(r)]), (s, DF.at[1, b, span(r)])) + [(s, DF.at[0, b, span(r)], None)]
        if kind == CR:
            b, first, n = group(r)
            f, s = (pl.ds(RING * first + h * 2 * n, 2 * n) for h in range(2))
            return both((DF.at[3, b, f], DF.at[2, b, f]), (DF.at[1, b, s], DF.at[2, b, s]))
        if kind in (Q2, QD, QS):
            b, first, n = group(r)
            f = ft.at[r % 2]
            own = lambda k: pl.ds(k * n, n)
            rs = pl.ds(first, n)
            if kind == Q2:
                return updn((f.at[0, own(2)], rst.at[b, 0, rs]), (f.at[1, own(2)], rst.at[b, 1, rs]))
            if kind == QD:
                return updn((f.at[1, own(1)], rrc.at[b, 0, 1, rs]), (f.at[0, own(3)], rrc.at[b, 1, 0, rs]))
            return updn((f.at[0, own(1)], rrc.at[b, 0, 0, rs]), (f.at[1, own(3)], rrc.at[b, 1, 1, rs]))
        if kind in (L1, L2, L3):
            b, _, n = group(r)
            m = {L1: XF, L2: GF, L3: DF}[kind]
            return [(m.at[:, b, span(r)], pan.at[slot_of[name], :, pl.ds(0, RING * n)], None)]
        if kind in (L5, L4):
            m, p, j = (GF, GPB, O5[r]) if kind == L5 else (DF, DPB, r)
            s = pan.at[slot_of[name]]
            return [(m.at[j, :, :, mine], s.at[:, :, lo], None), (p.at[j], s.at[:, :, hi], None)]
        if kind == LH:
            return [(HPB, wds.at[0:4], None)]
        if kind == LX:
            return [(XF.at[0], wus.at[0:4], None), (XPB, wus.at[4:8], None)]
        place = {j: i for i, j in enumerate(O5)}
        if kind == O2:
            return both((obuf.at[place[2], 0], sw.at[0]), (obuf.at[place[2], 1], sw.at[1]))
        if kind == O1:
            return both((obuf.at[place[1]], dwd.at[:, x]), (obuf.at[place[3]], dwd.at[:, x]))
        assert kind == OR
        return both((sw.at[0], dwd.at[0, at(3)]), (sw.at[1], dwd.at[1, at(1)]))

    def total(terms):
        out = None
        for a, b, dims in terms:
            d = lax.dot_general(a, b, dims, preferred_element_type=jnp.float32)
            out = d if out is None else out + d
        return out

    def loop(n, body):
        def step(i, carry):
            body(i)
            return carry
        lax.fori_loop(0, n, step, 0)

    def unit(name):
        kind, r = name[0], name[-1]
        if kind in (M1, M2, M3):
            b, first, n = group(r)
            rows = pl.ds(0, RING * n)
        if kind == M1:
            p = pan.at[slot_of[L1, r]]

            def body(t):
                ns = pl.ds(pl.multiple_of(t * sub, sub), sub)
                s = total([(p[j, rows, h * dh:(h + 1) * dh], wus[2 * j + h, :, ns], NN) for j in range(RING) for h in range(2)])
                hbuf[b, span(r), ns] = s.astype(jnp.bfloat16)
            loop(2, body)
        elif kind == M2:
            p = pan.at[slot_of[L2, r]]
            if r >= 2:
                cp.left((CS, r - 2))
            d = dct.at[r % 2]
            step = min(32, RING * n)

            def body(t):
                ns = pl.ds(pl.multiple_of(t * sub, sub), sub)
                acc[rows, :] = total([(p[j, rows, :], wds[2 * j + t], NT) for j in range(RING)])

                def elem(e):
                    rs = pl.ds(pl.multiple_of(e * step, step), step)
                    hs = pl.ds(pl.multiple_of(RING * first + e * step, step), step)
                    g, s = gelu_parts(hbuf[b, hs, ns].astype(jnp.float32))
                    hbuf[b, hs, ns] = g.astype(jnp.bfloat16)
                    d[rs, ns] = (acc[rs, :] * s).astype(jnp.bfloat16)
                loop(RING * n // step, elem)
            loop(2, body)
        elif kind == M3:
            p = pan.at[slot_of[L3, r]]
            if r >= 2:
                for q in (Q2, QD, QS):
                    cp.left((q, r - 2))
            f = ft.at[r % 2]

            def body(t):
                f[t, rows, :] = total([(p[j, rows, :], wun[2 * j + t], NT) for j in range(RING)])
            loop(2, body)
        elif kind == M5:
            p = pan.at[slot_of[L5, r]]

            def body(t):
                ms = pl.ds(pl.multiple_of(t * dh, dh), dh)
                s = total([(hbuf[g, :, ms], p[g, :, lo], TN) for g in range(NB)] + [(wds[g, :, ms], p[g, :, hi], TN) for g in range(NB)])
                obuf[r, t] = s.astype(jnp.bfloat16)
            loop(2, body)
            if O5[r] == 0:
                cp.add((OUT, kind, r), [(obuf.at[r], dwd.at[:, x], None)])
        elif kind == M4:
            s0, s1 = slot_of[L4, 2 * r], slot_of[L4, 2 * r + 1]

            def body(i):
                e, t = i // 2, lax.rem(i, 2)
                p = pan.at[s0 + e * (s1 - s0)]
                ms = pl.ds(pl.multiple_of(t * dh, dh), dh)
                s = total([(wus[g, :, ms], p[g, :, lo], TN) for g in range(NB)] + [(wus[NB + g, :, ms], p[g, :, hi], TN) for g in range(NB)])
                dwu[t, :, cols(2 * r + e)] = s.astype(jnp.bfloat16)
            loop(4, body)
        else:
            b, first, n = group(r)
            f = ft.at[r % 2]
            rs = pl.ds(first, n)
            own = lambda k: pl.ds(k * n, n)
            if kind == QA:
                f[0, own(1), :] = f[0, own(1), :] + rst[b, 0, rs, :]
                f[1, own(3), :] = f[1, own(3), :] + rst[b, 1, rs, :]
            else:
                for h in range(2):
                    dx[b, rs, h * dh:(h + 1) * dh] = (f[h, own(0), :] + rrc[b, 0, h, rs, :] + rrc[b, 1, h, rs, :]).astype(jnp.bfloat16)

    for name in order:
        for d in (it[name][2] if name in it else un[name][1]):
            cp.arrived(d)
        if name[0] == OWN:
            own = pl.ds(0, blk_rows)
            b0, b1 = pan.at[0, :, own], pan.at[1, :, own]
            cp.add((OUT, OWN), [(xa, b0, None), (za, b1, None)])
            cp.arrived((OUT, OWN))
            pairs = []
            for r in range(NG):
                b, first, n = group(r)
                pairs += [(pan.at[a, b, pl.ds(first, n)], buf[a].at[0, b, rel(r, 0)], None) for a in (X, G)]
            cp.add(name, pairs)
        elif name in it:
            for w in {LX: (0,), LH: (1,)}.get(name[0], ()):
                for p in range(3):
                    cp.left((WP, w, p))
            cp.add(name, copies_of(name))
        else:
            unit(name)
    cp.finish()
    assert cp.n_remote <= N_REMOTE and cp.n_local <= N_LOCAL, (cp.n_remote, cp.n_local)


def solution(mesh):
    assert mesh.shape["cy"] == RING and mesh.shape["cz"] == RING and mesh.shape["cx"] == CORES
    row_spec = P(("dp", "cx", "cz"), "cy")
    up_spec = P("cy", ("cz", "cx"))
    down_spec = P("cz", ("cy", "cx"))
    up_out = P(("dp", "cy"), ("cz", "cx"))
    down_out = P(("dp", "cz"), ("cy", "cx"))
    plan = make_plan()
    order, panels, _, _ = make_order(plan, *make_lists(ORDER))

    def local_step(x_act, w_up, w_down, z_grad):
        t_loc, d_loc = x_act.shape
        f_loc = w_up.shape[1]
        rows, sub, dh = t_loc // NB, f_loc // RING, d_loc // 2
        grp = RING * rows
        bf, f32 = jnp.bfloat16, jnp.float32
        xa, za = x_act.reshape(NB, rows, d_loc), z_grad.reshape(NB, rows, d_loc)
        wu = w_up.reshape(2, dh, f_loc)
        wd = w_down.reshape(CORES, RING, sub, dh)
        hbm = lambda *s: jax.ShapeDtypeStruct(s, bf)
        outs = (
            pltpu.VMEM((NB, rows, d_loc), bf), pltpu.VMEM((2, dh, f_loc), bf), hbm(CORES, RING, sub, dh),
            hbm(RING, NB, grp, d_loc), hbm(RING, NB, grp, d_loc), hbm(RING, NB, grp, 2 * sub),
            hbm(RING, NB, grp, sub), hbm(RING, NB, grp, sub), hbm(NB, grp, d_loc), hbm(NB, grp, 2 * sub),
            hbm(2, dh, sub), hbm(2, sub, dh), hbm(2, sub, dh),
        )
        scratch = [
            pltpu.VMEM((2 * RING, dh, 2 * sub), bf), pltpu.VMEM((2 * RING, sub, d_loc), bf), pltpu.VMEM((2 * RING, dh, 2 * sub), bf),
            pltpu.VMEM((NB, grp, 2 * sub), bf), pltpu.VMEM((PAN, RING, grp, d_loc), bf),
            pltpu.VMEM((2, 2, grp, dh), f32), pltpu.VMEM((2, grp, 2 * sub), bf),
            pltpu.VMEM((NB, 2, rows, dh), f32), pltpu.VMEM((NB, 2, 2, rows, dh), f32),
            pltpu.VMEM((RING, CORES, sub, dh), bf),
            pltpu.VMEM((grp, sub), f32),
            pltpu.SemaphoreType.DMA((N_REMOTE,)), pltpu.SemaphoreType.DMA((N_REMOTE,)), pltpu.SemaphoreType.DMA((N_LOCAL,)),
        ]
        any_spec = pl.BlockSpec(memory_space=pl.ANY)
        res = pl.pallas_call(
            functools.partial(kernel, plan, order, panels),
            out_shape=outs,
            in_specs=[any_spec] * 4,
            out_specs=[pl.BlockSpec(memory_space=pltpu.VMEM)] * 2 + [any_spec] * (len(outs) - 2),
            scratch_shapes=scratch,
            compiler_params=pltpu.CompilerParams(collective_id=0, has_side_effects=True, vmem_limit_bytes=61800000),
            name="mlp_bwd",
        )(xa, wu, wd, za)
        return (res[0].reshape(t_loc, d_loc), res[1].reshape(w_up.shape), res[2].reshape(w_down.shape))

    return jax.shard_map(local_step, mesh=mesh, in_specs=(row_spec, up_spec, down_spec, row_spec), out_specs=(row_spec, up_out, down_out), check_vma=False)
```

```python
import functools
import math
import string

import jax
import jax.numpy as jnp
from jax import lax
from jax.experimental import pallas as pl
from jax.experimental.pallas import tpu as pltpu
from jax.sharding import PartitionSpec as P

GELU_COEF = 0.044715
SQRT_TWO_PI = math.sqrt(2.0 / math.pi)
NN = (((1,), (0,)), ((), ()))
NT = (((1,), (1,)), ((), ()))
TN = (((0,), (0,)), ((), ()))
MESH = pl.DeviceIdType.MESH
RING = 4
CORES = 2
PAN = 3
GROUPS = ((0, 0, 8), (1, 0, 8), (2, 0, 8), (3, 0, 4), (3, 4, 4))
NB = 4
NG = len(GROUPS)
EARLY = 2
X, G = 0, 1


def gelu_parts(pre_act):
    inner_arg = SQRT_TWO_PI * (pre_act + GELU_COEF * pre_act * pre_act * pre_act)
    tanh_val = jnp.tanh(inner_arg)
    gelu_val = 0.5 * pre_act * (1.0 + tanh_val)
    gelu_slope = 0.5 * (1.0 + tanh_val) + 0.5 * pre_act * (1.0 - tanh_val * tanh_val) * SQRT_TWO_PI * (1.0 + 3.0 * GELU_COEF * pre_act * pre_act)
    return gelu_val, gelu_slope


(XS, XR, W2, W1, WR, CS, CR, O2, O1, OR, YA, YB, YF, YR, Q2, QD, QS, WN, WP, GP, XP, HP, CP, CF,
 OWN, L1, L2, L3, L4, L5, LX, LH, M1, M2, M3, M4, M5, QA, QF, OUT) = range(40)
PANEL_OF = {L1: M1, L2: M2, L3: M3, L4: M4, L5: M5}
O5 = (2, 1, 3, 0)
O4 = (0, 1, 3, 2)
PARTS = ((0, 1), (1, 2), (3, 1))
PART_OF = (0, 1, 1, 2)


def full(a, r):
    return [(XS, a, r), (XR, a, r), (YR, a, r), (OWN,)] + ([(YA, a, r), (YB, a, r)] if r < EARLY else [(YF, a, r)])


def make_plan():
    it, un = {}, {}
    groups = range(NG)
    for r in groups:
        q = GROUPS[r][2] / 8 / NB
        f = 4 * q
        for a in (X, G):
            it[XS, a, r] = (0, q, [])
            it[XR, a, r] = (0, q / 2, [(XS, a, r)])
            row = [(XS, a, r), (XR, a, r)]
            if r < EARLY:
                it[YA, a, r] = (1, q, [])
                it[YB, a, r] = (1, 3 * q, row)
                it[YR, a, r] = (1, 2 * q, [(YA, a, r), (YB, a, r)])
            else:
                it[YF, a, r] = (1, 4 * q, row + [(OWN,)])
                it[YR, a, r] = (1, 2 * q, [(YF, a, r)])
        it[GP, r] = (2, 8 * q, full(G, r))
        it[XP, r] = (2, 4 * q, full(X, r))
        it[HP, r] = (2, 4 * q, [(M2, r)])
        it[CS, r] = (0, 4 * q, [(M2, r)])
        it[CR, r] = (0, 2 * q, [(CS, r)])
        dc = [(CS, r), (CR, r)]
        it[CP, r] = (2, 6 * q, [(CS, r)])
        it[CF, r] = (2, 2 * q, [(CR, r)])
        it[Q2, r] = (1, q, [(M3, r)])
        it[QD, r] = (1, q, [(M3, r)])
        it[QS, r] = (1, q, [(QA, r)])
        it[L1, r] = (3, 16 * q, full(X, r))
        it[L2, r] = (3, 16 * q, full(G, r))
        it[L3, r] = (3, 16 * q, dc)
        wu = [(WP, 0, p) for p in range(3)]
        wd = [(WP, 1, p) for p in range(3)]
        un[M1, r] = (0.4 + 4.4 * f, [(L1, r)] + wu)
        un[M2, r] = (0.4 + 6.2 * f, [(L2, r), (M1, r)] + wd)
        un[M3, r] = (0.4 + 4.4 * f, [(L3, r), (WN,)] + ([(QF, r - 2)] if r >= 2 else []))
        un[QA, r] = (0.1 + 0.4 * f, [(Q2, r)])
        un[QF, r] = (0.1 + 0.4 * f, [(QS, r), (QD, r)])
    for w in range(2):
        it[W2, w] = (0, 0.5, [])
        it[W1, w] = (0, 1.0, [])
        it[WR, w] = (0, 0.5, [(W2, w)])
        it[WP, w, 0] = (2, 1, [])
        it[WP, w, 1] = (2, 2, [(W1, w)])
        it[WP, w, 2] = (2, 1, [(WR, w)])
    it[(WN,)] = (2, 4, [])
    it[(OWN,)] = (3, 2, [])
    it[(O2,)] = (0, 0.5, [(M5, 0)])
    it[(O1,)] = (0, 1.0, [(M5, 1)])
    it[(OR,)] = (0, 0.5, [(O2,)])
    for p in range(RING):
        it[L5, p] = (3, 4, [(GP, r) for r in groups] + sum([full(G, r) for r in groups], []))
        it[L4, p] = (3, 4, [(CF if O4[p] == 2 else CP, r) for r in groups] + [(CR if O4[p] == 2 else CS, r) for r in groups])
    it[(LH,)] = (3, 4, [(HP, r) for r in groups] + [(M2, r) for r in groups])
    it[(LX,)] = (3, 8, [(XP, r) for r in groups] + [(M5, 0)])
    for p, (first, n) in enumerate(PARTS):
        un[M4, p] = (4.8 * n, [(L4, first + i) for i in range(n)] + [(LX,)])
        un[M5, p] = (4.8 * n, [(L5, first + i) for i in range(n)] + [(LH,)])
    return it, un


ORDER = (
    "acbdgihjEuyFHGmInJosAptvzBekflqwrxCKDLM",
    "adjmbecfknlosutvzBACGIHJghipqrwxyDKELFM",
    "bagflqpyvudinskxtmchACrejowBEDz",
)


def make_lists(plan):
    it, un = plan
    base = [[n for n in it if it[n][0] == k] for k in range(len(ORDER) - 1)] + [list(un)]
    *lists, units = ([names[string.ascii_letters.index(ch)] for ch in key] for names, key in zip(base, ORDER))
    return lists, units


RATE = (22.5, 22.5, 1.7, 0.4)
DELAY = (3.0, 3.0, 1.5, 1.5)


def make_order(plan, lists, units):
    it, un = plan
    done, free, pos = {}, [0.0] * 4, [0] * 4
    pend, now, order, panels, waits = list(units), 0.0, [], [], []
    late = [n for n in it if it[n][0] >= 2]
    rank = {u: i for i, u in enumerate(units)}
    user = lambda n: (PANEL_OF[n[0]], PART_OF[n[1]] if n[0] in (L4, L5) else n[1])
    panel_rank = lambda n: rank[user(n)] if n[0] in PANEL_OF else rank[{LX: M4, LH: M5}[n[0]], 0] if n[0] in (LX, LH) else -1
    gone = set()
    big = 1e9

    def ready(n):
        return all(done.get(d, big) <= now for d in it[n][2])

    def send(n):
        k = it[n][0]
        start = max(now + 0.3, free[k])
        waits.append((k, start - free[k], n))
        free[k] = start + it[n][1] * RATE[k]
        done[n] = free[k] + DELAY[k]
        order.append(n)

    while True:
        for k in (0, 1):
            while pos[k] < len(lists[k]) and ready(lists[k][pos[k]]):
                send(lists[k][pos[k]])
                pos[k] += 1
        for n in sorted((n for n in late if ready(n)), key=lambda n: (panel_rank(n), n)):
            if n[0] in PANEL_OF:
                if len(panels) >= PAN and user(panels[-PAN]) not in gone:
                    continue
                panels.append(n)
            late.remove(n)
            send(n)
        can = [u for u in pend if all(done.get(d, big) <= now for d in un[u][1])]
        if can:
            pend.remove(can[0])
            order.append(can[0])
            now += un[can[0]][0]
            done[can[0]] = now
            gone.add(can[0])
            continue
        later = [v for v in done.values() if v > now]
        if not later:
            break
        now = min(later)
    assert not pend and not late and all(pos[k] == len(lists[k]) for k in (0, 1)), (pend, late, pos)
    return order, panels, max(done.values()), waits


class Copies:
    def __init__(self, send, recv, local, peers):
        self.send, self.recv, self.local, self.peers = send, recv, local, peers
        self.n_remote = self.n_local = 0
        self.by_name = {}

    def add(self, name, pairs):
        made = []
        for src, dst, to in pairs:
            if to is None:
                c = pltpu.make_async_copy(src, dst, self.local.at[self.n_local])
                self.n_local += 1
            else:
                axis, idx = self.peers[to]
                c = pltpu.make_async_remote_copy(
                    src, dst, self.send.at[self.n_remote], self.recv.at[self.n_remote],
                    device_id={axis: idx}, device_id_type=MESH)
                self.n_remote += 1
            made.append([c, to, False, False])
            c.start()
        self.by_name.setdefault(name, []).extend(made)

    def arrived(self, name):
        for m in self.by_name.get(name, ()):
            if not m[2]:
                m[2] = True
                m[0].wait() if m[1] is None else m[0].wait_recv()

    def left(self, name):
        for m in self.by_name.get(name, ()):
            if m[1] is None:
                if not m[2]:
                    m[2] = True
                    m[0].wait()
            elif not m[3]:
                m[3] = True
                m[0].wait_send()

    def finish(self):
        for name in list(self.by_name):
            self.arrived(name)
            self.left(name)


N_REMOTE = 208
N_LOCAL = 80


def kernel(plan, order, panels, xa, wu, wd, za, dx, dwu, dwd, XF, GF, DF, GPB, DPB, XPB, HPB, su, sd, sw,
           wus, wds, wun, hbuf, pan, ft, dct, rst, rrc, obuf, acc, send, recv, local):
    it, un = plan
    x, y, c = lax.axis_index("cy"), lax.axis_index("cz"), lax.axis_index("cx")
    peers = {
        "R": ("cy", lax.rem(x + 1, RING)), "L": ("cy", lax.rem(x + RING - 1, RING)),
        "U": ("cz", lax.rem(y + 1, RING)), "N": ("cz", lax.rem(y + RING - 1, RING)),
        "P": ("cx", 1 - c),
    }
    barrier = pltpu.get_barrier_semaphore()
    for axis, idx in peers.values():
        pl.semaphore_signal(barrier, inc=1, device_id={axis: idx}, device_id_type=MESH)
    pl.semaphore_wait(barrier, len(peers))

    cp = Copies(send, recv, local, peers)
    blk_rows = xa.shape[1]
    sub = wd.shape[2]
    dh = wu.shape[1]
    mine = pl.ds(pl.multiple_of(c * sub, sub), sub)
    theirs = pl.ds(pl.multiple_of((1 - c) * sub, sub), sub)
    lo, hi = pl.ds(0, sub), pl.ds(sub, sub)
    at = lambda j: lax.rem(x + j, RING)
    cols = lambda j: pl.ds(pl.multiple_of(at(j) * sub, sub), sub)
    slot_of = {n: i % PAN for i, n in enumerate(panels)}
    inp, buf = (xa, za), (XF, GF)

    def group(r):
        b, first, n = GROUPS[r]
        unit_rows = blk_rows // 8
        return b, first * unit_rows, n * unit_rows

    def rel(r, k, part=None):
        _, first, n = group(r)
        start = RING * first + k * n
        return pl.ds(start, n) if part is None else pl.ds(start + part * (n // 2), n // 2)

    def span(r):
        _, first, n = group(r)
        return pl.ds(RING * first, RING * n)

    def copies_of(name):
        kind, a, r = name[0], name[-2:][0], name[-1]
        both = lambda right, left: [right + ("R",), left + ("L",)]
        updn = lambda up, down: [up + ("U",), down + ("N",)]
        if kind == WN:
            return sum([[(wu.at[:, :, cols(j)], wun.at[2 * j:2 * j + 2, :, mine], to) for to in (None, "P")] for j in range(RING)], [])
        if kind == XS or kind == YA:
            b, first, n = group(r)
            src = inp[a].at[b, pl.ds(first, n)]
            if kind == XS:
                return both((src, buf[a].at[3, b, rel(r, 0)]), (src, buf[a].at[1, b, rel(r, 0)]))
            return updn((src, buf[a].at[0, b, rel(r, 3)]), (src, buf[a].at[0, b, rel(r, 1)]))
        if kind == XR:
            b, f, s = group(r)[0], rel(r, 0, 0), rel(r, 0, 1)
            return both((buf[a].at[3, b, f], buf[a].at[2, b, f]), (buf[a].at[1, b, s], buf[a].at[2, b, s]))
        if kind in (YB, YF):
            b, m = group(r)[0], buf[a]
            js = pl.ds(1, RING - 1) if kind == YB else pl.ds(0, RING)
            return updn((m.at[js, b, rel(r, 0)], m.at[js, b, rel(r, 3)]), (m.at[js, b, rel(r, 0)], m.at[js, b, rel(r, 1)]))
        if kind == YR:
            b, m = group(r)[0], buf[a]
            return updn((m.at[0:2, b, rel(r, 3)], m.at[0:2, b, rel(r, 2)]), (m.at[2:4, b, rel(r, 1)], m.at[2:4, b, rel(r, 2)]))
        if kind in (W2, W1, WR):
            half = (lambda h, j: wu.at[h, :, cols(j)]) if r == 0 else (lambda h, j: wd.at[h, at(j)])
            piece = (lambda j: wu.at[:, :, cols(j)]) if r == 0 else (lambda j: wd.at[:, at(j)])
            st, dst = (su, sd)[r], (wus, wds)[r]
            if kind == W2:
                return both((half(0, 2), st.at[0]), (half(1, 2), st.at[1]))
            if kind == W1:
                return both((piece(1), dst.at[6:8, :, mine]), (piece(3), dst.at[2:4, :, mine]))
            return both((st.at[0], dst.at[4, :, mine]), (st.at[1], dst.at[5, :, mine]))
        if kind == WP:
            m = (wus, wds)[a]
            if r == 0:
                src = wu.at[:, :, cols(0)] if a == 0 else wd.at[:, at(0)]
                return [(src, m.at[0:2, :, mine], to) for to in (None, "P")]
            return [(m.at[2 * j:2 * j + 2, :, mine], m.at[2 * j:2 * j + 2, :, mine], "P") for j in ((1, 3) if r == 1 else (2,))]
        if kind == GP:
            return [(GF.at[:, group(r)[0], span(r), theirs], GPB.at[:, group(r)[0], span(r)], "P")]
        if kind == XP:
            return [(XF.at[0, group(r)[0], span(r)], XPB.at[group(r)[0], span(r)], "P")]
        if kind == HP:
            return [(hbuf.at[group(r)[0], span(r)], HPB.at[group(r)[0], span(r)], "P")]
        if kind in (CP, CF):
            b = group(r)[0]
            js = (pl.ds(0, 2), pl.ds(3, 1)) if kind == CP else (pl.ds(2, 1),)
            return [(DF.at[j, b, span(r), theirs], DPB.at[j, b, span(r)], "P") for j in js]
        if kind == CS:
            b, _, n = group(r)
            s = dct.at[r % 2, pl.ds(0, RING * n)]
            return both((s, DF.at[3, b, span(r)]), (s, DF.at[1, b, span(r)])) + [(s, DF.at[0, b, span(r)], None)]
        if kind == CR:
            b, first, n = group(r)
            f, s = (pl.ds(RING * first + h * 2 * n, 2 * n) for h in range(2))
            return both((DF.at[3, b, f], DF.at[2, b, f]), (DF.at[1, b, s], DF.at[2, b, s]))
        if kind in (Q2, QD, QS):
            b, first, n = group(r)
            f = ft.at[r % 2]
            own = lambda k: pl.ds(k * n, n)
            rs = pl.ds(first, n)
            if kind == Q2:
                return updn((f.at[0, own(2)], rst.at[b, 0, rs]), (f.at[1, own(2)], rst.at[b, 1, rs]))
            if kind == QD:
                return updn((f.at[1, own(1)], rrc.at[b, 0, 1, rs]), (f.at[0, own(3)], rrc.at[b, 1, 0, rs]))
            return updn((f.at[0, own(1)], rrc.at[b, 0, 0, rs]), (f.at[1, own(3)], rrc.at[b, 1, 1, rs]))
        if kind in (L1, L2, L3):
            b, _, n = group(r)
            m = {L1: XF, L2: GF, L3: DF}[kind]
            return [(m.at[:, b, span(r)], pan.at[slot_of[name], :, pl.ds(0, RING * n)], None)]
        if kind in (L5, L4):
            m, p, j = (GF, GPB, O5[r]) if kind == L5 else (DF, DPB, O4[r])
            s = pan.at[slot_of[name]]
            return [(m.at[j, :, :, mine], s.at[:, :, lo], None), (p.at[j], s.at[:, :, hi], None)]
        if kind == LH:
            return [(HPB, wds.at[0:4], None)]
        if kind == LX:
            return [(XF.at[0], wus.at[0:4], None), (XPB, wus.at[4:8], None)]
        place = {j: i for i, j in enumerate(O5)}
        if kind == O2:
            return both((obuf.at[place[2], 0], sw.at[0]), (obuf.at[place[2], 1], sw.at[1]))
        if kind == O1:
            return both((obuf.at[place[1]], dwd.at[:, x]), (obuf.at[place[3]], dwd.at[:, x]))
        assert kind == OR
        return both((sw.at[0], dwd.at[0, at(3)]), (sw.at[1], dwd.at[1, at(1)]))

    def total(terms):
        out = None
        for a, b, dims in terms:
            d = lax.dot_general(a, b, dims, preferred_element_type=jnp.float32)
            out = d if out is None else out + d
        return out

    def loop(n, body):
        def step(i, carry):
            body(i)
            return carry
        lax.fori_loop(0, n, step, 0)

    def unit(name):
        kind, r = name[0], name[-1]
        if kind in (M1, M2, M3):
            b, first, n = group(r)
            rows = pl.ds(0, RING * n)
        if kind == M1:
            p = pan.at[slot_of[L1, r]]

            def body(t):
                ns = pl.ds(pl.multiple_of(t * sub, sub), sub)
                s = total([(p[j, rows, h * dh:(h + 1) * dh], wus[2 * j + h, :, ns], NN) for j in range(RING) for h in range(2)])
                hbuf[b, span(r), ns] = s.astype(jnp.bfloat16)
            loop(2, body)
        elif kind == M2:
            p = pan.at[slot_of[L2, r]]
            if r >= 2:
                cp.left((CS, r - 2))
            d = dct.at[r % 2]
            step = min(32, RING * n)

            def body(t):
                ns = pl.ds(pl.multiple_of(t * sub, sub), sub)
                acc[rows, :] = total([(p[j, rows, :], wds[2 * j + t], NT) for j in range(RING)])

                def elem(e):
                    rs = pl.ds(pl.multiple_of(e * step, step), step)
                    hs = pl.ds(pl.multiple_of(RING * first + e * step, step), step)
                    g, s = gelu_parts(hbuf[b, hs, ns].astype(jnp.float32))
                    hbuf[b, hs, ns] = g.astype(jnp.bfloat16)
                    d[rs, ns] = (acc[rs, :] * s).astype(jnp.bfloat16)
                loop(RING * n // step, elem)
            loop(2, body)
        elif kind == M3:
            p = pan.at[slot_of[L3, r]]
            if r >= 2:
                for q in (Q2, QD, QS):
                    cp.left((q, r - 2))
            f = ft.at[r % 2]

            def body(t):
                f[t, rows, :] = total([(p[j, rows, :], wun[2 * j + t], NT) for j in range(RING)])
            loop(2, body)
        elif kind in (M5, M4):
            i0, m = PARTS[r]
            s0, s1 = (slot_of[L5 if kind == M5 else L4, i] for i in (i0, i0 + m - 1))
            j0, j1 = ((O5 if kind == M5 else O4)[i] for i in (i0, i0 + m - 1))
            own, par, p0 = (hbuf, wds, 0) if kind == M5 else (wus, wus, NB)

            def body(i):
                e, t = (0, i) if m == 1 else (i // 2, lax.rem(i, 2))
                p = pan.at[s0 + e * (s1 - s0)]
                ms = pl.ds(pl.multiple_of(t * dh, dh), dh)
                s = total([(own[g, :, ms], p[g, :, lo], TN) for g in range(NB)] + [(par[p0 + g, :, ms], p[g, :, hi], TN) for g in range(NB)])
                if kind == M5:
                    obuf[i0 + e, t] = s.astype(jnp.bfloat16)
                else:
                    dwu[t, :, cols(j0 + e * (j1 - j0))] = s.astype(jnp.bfloat16)
            loop(2 * m, body)
            if kind == M5 and O5[i0] == 0:
                cp.add((OUT, kind), [(obuf.at[i0], dwd.at[:, x], None)])
        else:
            b, first, n = group(r)
            f = ft.at[r % 2]
            rs = pl.ds(first, n)
            own = lambda k: pl.ds(k * n, n)
            if kind == QA:
                f[0, own(1), :] = f[0, own(1), :] + rst[b, 0, rs, :]
                f[1, own(3), :] = f[1, own(3), :] + rst[b, 1, rs, :]
            else:
                for h in range(2):
                    dx[b, rs, h * dh:(h + 1) * dh] = (f[h, own(0), :] + rrc[b, 0, h, rs, :] + rrc[b, 1, h, rs, :]).astype(jnp.bfloat16)

    for name in order:
        for d in (it[name][2] if name in it else un[name][1]):
            cp.arrived(d)
        if name[0] == OWN:
            own = pl.ds(0, blk_rows)
            b0, b1 = pan.at[0, :, own], pan.at[1, :, own]
            cp.add((OUT, OWN), [(xa, b0, None), (za, b1, None)])
            cp.arrived((OUT, OWN))
            pairs = []
            for r in range(NG):
                b, first, n = group(r)
                pairs += [(pan.at[a, b, pl.ds(first, n)], buf[a].at[0, b, rel(r, 0)], None) for a in (X, G)]
            cp.add(name, pairs)
        elif name in it:
            for w in {LX: (0,), LH: (1,)}.get(name[0], ()):
                for p in range(3):
                    cp.left((WP, w, p))
            cp.add(name, copies_of(name))
        else:
            unit(name)
    cp.finish()
    assert cp.n_remote <= N_REMOTE and cp.n_local <= N_LOCAL, (cp.n_remote, cp.n_local)


def solution(mesh):
    assert mesh.shape["cy"] == RING and mesh.shape["cz"] == RING and mesh.shape["cx"] == CORES
    row_spec = P(("dp", "cx", "cz"), "cy")
    up_spec = P("cy", ("cz", "cx"))
    down_spec = P("cz", ("cy", "cx"))
    up_out = P(("dp", "cy"), ("cz", "cx"))
    down_out = P(("dp", "cz"), ("cy", "cx"))
    plan = make_plan()
    order, panels, _, _ = make_order(plan, *make_lists(plan))

    def local_step(x_act, w_up, w_down, z_grad):
        t_loc, d_loc = x_act.shape
        f_loc = w_up.shape[1]
        rows, sub, dh = t_loc // NB, f_loc // RING, d_loc // 2
        grp = RING * rows
        bf, f32 = jnp.bfloat16, jnp.float32
        xa, za = x_act.reshape(NB, rows, d_loc), z_grad.reshape(NB, rows, d_loc)
        wu = w_up.reshape(2, dh, f_loc)
        wd = w_down.reshape(CORES, RING, sub, dh)
        hbm = lambda *s: jax.ShapeDtypeStruct(s, bf)
        outs = (
            pltpu.VMEM((NB, rows, d_loc), bf), pltpu.VMEM((2, dh, f_loc), bf), hbm(CORES, RING, sub, dh),
            hbm(RING, NB, grp, d_loc), hbm(RING, NB, grp, d_loc), hbm(RING, NB, grp, 2 * sub),
            hbm(RING, NB, grp, sub), hbm(RING, NB, grp, sub), hbm(NB, grp, d_loc), hbm(NB, grp, 2 * sub),
            hbm(2, dh, sub), hbm(2, sub, dh), hbm(2, sub, dh),
        )
        scratch = [
            pltpu.VMEM((2 * RING, dh, 2 * sub), bf), pltpu.VMEM((2 * RING, sub, d_loc), bf), pltpu.VMEM((2 * RING, dh, 2 * sub), bf),
            pltpu.VMEM((NB, grp, 2 * sub), bf), pltpu.VMEM((PAN, RING, grp, d_loc), bf),
            pltpu.VMEM((2, 2, grp, dh), f32), pltpu.VMEM((2, grp, 2 * sub), bf),
            pltpu.VMEM((NB, 2, rows, dh), f32), pltpu.VMEM((NB, 2, 2, rows, dh), f32),
            pltpu.VMEM((RING, CORES, sub, dh), bf),
            pltpu.VMEM((grp, sub), f32),
            pltpu.SemaphoreType.DMA((N_REMOTE,)), pltpu.SemaphoreType.DMA((N_REMOTE,)), pltpu.SemaphoreType.DMA((N_LOCAL,)),
        ]
        any_spec = pl.BlockSpec(memory_space=pl.ANY)
        res = pl.pallas_call(
            functools.partial(kernel, plan, order, panels),
            out_shape=outs,
            in_specs=[any_spec] * 4,
            out_specs=[pl.BlockSpec(memory_space=pltpu.VMEM)] * 2 + [any_spec] * (len(outs) - 2),
            scratch_shapes=scratch,
            compiler_params=pltpu.CompilerParams(collective_id=0, has_side_effects=True, vmem_limit_bytes=61800000),
            name="mlp_bwd",
        )(xa, wu, wd, za)
        return (res[0].reshape(t_loc, d_loc), res[1].reshape(w_up.shape), res[2].reshape(w_down.shape))

    return jax.shard_map(local_step, mesh=mesh, in_specs=(row_spec, up_spec, down_spec, row_spec), out_specs=(row_spec, up_out, down_out), check_vma=False)
```

```python
import functools
import math
import string

import jax
import jax.numpy as jnp
from jax import lax
from jax.experimental import pallas as pl
from jax.experimental.pallas import tpu as pltpu
from jax.sharding import PartitionSpec as P

GELU_COEF = 0.044715
SQRT_TWO_PI = math.sqrt(2.0 / math.pi)
NN = (((1,), (0,)), ((), ()))
NT = (((1,), (1,)), ((), ()))
TN = (((0,), (0,)), ((), ()))
MESH = pl.DeviceIdType.MESH
RING = 4
CORES = 2
PAN = 3
GROUPS = ((0, 0, 8), (1, 0, 8), (2, 0, 8), (3, 0, 4), (3, 4, 4))
NB = 4
NG = len(GROUPS)
EARLY = 2
X, G = 0, 1


def gelu_parts(pre_act):
    inner_arg = SQRT_TWO_PI * (pre_act + GELU_COEF * pre_act * pre_act * pre_act)
    tanh_val = jnp.tanh(inner_arg)
    gelu_val = 0.5 * pre_act * (1.0 + tanh_val)
    gelu_slope = 0.5 * (1.0 + tanh_val) + 0.5 * pre_act * (1.0 - tanh_val * tanh_val) * SQRT_TWO_PI * (1.0 + 3.0 * GELU_COEF * pre_act * pre_act)
    return gelu_val, gelu_slope


(XS, XR, W2, W1, WR, CS, CR, O2, O1, OR, YA, YB, YF, YR, Q2, QD, QS, WN, WP, GP, XP, HP, CP, CF,
 OWN, L1, L2, L3, L4, L5, LX, LH, M1, M2, M3, M4, M5, QA, QF, OUT) = range(40)
PANEL_OF = {L1: M1, L2: M2, L3: M3, L4: M4, L5: M5}
O5 = (2, 1, 3, 0)
O4 = (0, 1, 3, 2)
PARTS = ((0, 1), (1, 2), (3, 1))
PART_OF = (0, 1, 1, 2)


def full(a, r):
    return [(XS, a, r), (XR, a, r), (YR, a, r), (OWN,)] + ([(YA, a, r), (YB, a, r)] if r < EARLY else [(YF, a, r)])


def make_plan():
    it, un = {}, {}
    groups = range(NG)
    for r in groups:
        q = GROUPS[r][2] / 8 / NB
        f = 4 * q
        for a in (X, G):
            it[XS, a, r] = (0, q, [])
            it[XR, a, r] = (0, q / 2, [(XS, a, r)])
            row = [(XS, a, r), (XR, a, r)]
            if r < EARLY:
                it[YA, a, r] = (1, q, [])
                it[YB, a, r] = (1, 3 * q, row)
                it[YR, a, r] = (1, 2 * q, [(YA, a, r), (YB, a, r)])
            else:
                it[YF, a, r] = (1, 4 * q, row + [(OWN,)])
                it[YR, a, r] = (1, 2 * q, [(YF, a, r)])
        it[GP, r] = (2, 8 * q, full(G, r))
        it[XP, r] = (2, 4 * q, full(X, r))
        it[HP, r] = (2, 4 * q, [(M2, r)])
        it[CS, r] = (0, 4 * q, [(M2, r)])
        it[CR, r] = (0, 2 * q, [(CS, r)])
        dc = [(CS, r), (CR, r)]
        it[CP, r] = (2, 6 * q, [(CS, r)])
        it[CF, r] = (2, 2 * q, [(CR, r)])
        it[Q2, r] = (1, q, [(M3, r)])
        it[QD, r] = (1, q, [(M3, r)])
        it[QS, r] = (1, q, [(QA, r)])
        it[L1, r] = (3, 16 * q, full(X, r))
        it[L2, r] = (3, 16 * q, full(G, r))
        it[L3, r] = (3, 16 * q, dc)
        wu = [(WP, 0, p) for p in range(3)]
        wd = [(WP, 1, p) for p in range(3)]
        un[M1, r] = (0.4 + 4.4 * f, [(L1, r)] + wu)
        un[M2, r] = (0.4 + 6.2 * f, [(L2, r), (M1, r)] + wd)
        un[M3, r] = (0.4 + 4.4 * f, [(L3, r), (WN,)] + ([(QF, r - 2)] if r >= 2 else []))
        un[QA, r] = (0.1 + 0.4 * f, [(Q2, r)])
        un[QF, r] = (0.1 + 0.4 * f, [(QS, r), (QD, r)])
    for w in range(2):
        it[W2, w] = (0, 0.5, [])
        it[W1, w] = (0, 1.0, [])
        it[WR, w] = (0, 0.5, [(W2, w)])
        it[WP, w, 0] = (2, 1, [])
        it[WP, w, 1] = (2, 2, [(W1, w)])
        it[WP, w, 2] = (2, 1, [(WR, w)])
    it[(WN,)] = (2, 4, [])
    it[(OWN,)] = (3, 2, [])
    it[(O2,)] = (0, 0.5, [(M5, 0)])
    it[(O1,)] = (0, 1.0, [(M5, 1)])
    it[(OR,)] = (0, 0.5, [(O2,)])
    for p in range(RING):
        it[L5, p] = (3, 4, [(GP, r) for r in groups] + sum([full(G, r) for r in groups], []))
        it[L4, p] = (3, 4, [(CF if O4[p] == 2 else CP, r) for r in groups] + [(CR if O4[p] == 2 else CS, r) for r in groups])
    it[(LH,)] = (3, 4, [(HP, r) for r in groups] + [(M2, r) for r in groups])
    it[(LX,)] = (3, 8, [(XP, r) for r in groups] + [(M5, 0)])
    for p, (first, n) in enumerate(PARTS):
        un[M4, p] = (4.8 * n, [(L4, first + i) for i in range(n)] + [(LX,)])
        un[M5, p] = (4.8 * n, [(L5, first + i) for i in range(n)] + [(LH,)])
    return it, un


ORDER = (
    "acbdgihjEuyFHGmInJosAptvzBekflqwrxCKDLM",
    "adjmbecfknlosutvzBACGIHJghipqrwxyDKELFM",
    "bagflqpyvudinskxtmchACrejowBEDz",
)


def make_lists(plan):
    it, un = plan
    base = [[n for n in it if it[n][0] == k] for k in range(len(ORDER) - 1)] + [list(un)]
    *lists, units = ([names[string.ascii_letters.index(ch)] for ch in key] for names, key in zip(base, ORDER))
    return lists, units


RATE = (22.5, 22.5, 1.7, 0.4)
DELAY = (3.0, 3.0, 1.5, 1.5)


def make_order(plan, lists, units):
    it, un = plan
    done, free, pos = {}, [0.0] * 4, [0] * 4
    pend, now, order, panels, waits = list(units), 0.0, [], [], []
    late = [n for n in it if it[n][0] >= 2]
    rank = {u: i for i, u in enumerate(units)}
    user = lambda n: (PANEL_OF[n[0]], PART_OF[n[1]] if n[0] in (L4, L5) else n[1])
    panel_rank = lambda n: rank[user(n)] if n[0] in PANEL_OF else rank[{LX: M4, LH: M5}[n[0]], 0] if n[0] in (LX, LH) else -1
    gone = set()
    big = 1e9

    def ready(n):
        return all(done.get(d, big) <= now for d in it[n][2])

    def send(n):
        k = it[n][0]
        start = max(now + 0.3, free[k])
        waits.append((k, start - free[k], n))
        free[k] = start + it[n][1] * RATE[k]
        done[n] = free[k] + DELAY[k]
        order.append((n, now))

    while True:
        for k in (0, 1):
            while pos[k] < len(lists[k]) and ready(lists[k][pos[k]]):
                send(lists[k][pos[k]])
                pos[k] += 1
        for n in sorted((n for n in late if ready(n)), key=lambda n: (panel_rank(n), n)):
            if n[0] in PANEL_OF:
                if len(panels) >= PAN and user(panels[-PAN]) not in gone:
                    continue
                panels.append(n)
            late.remove(n)
            send(n)
        can = [u for u in pend if all(done.get(d, big) <= now for d in un[u][1])]
        if can:
            pend.remove(can[0])
            order.append((can[0], now))
            now += un[can[0]][0]
            done[can[0]] = now
            gone.add(can[0])
            continue
        later = [v for v in done.values() if v > now]
        if not later:
            break
        now = min(later)
    assert not pend and not late and all(pos[k] == len(lists[k]) for k in (0, 1)), (pend, late, pos)
    return [(n, [m for m in it if t - 30 < done[m] <= t - 2 and it[m][0] < 3]) for n, t in order], panels, max(done.values()), waits


class Copies:
    BACK = {"R": "L", "L": "R", "U": "N", "N": "U", "P": "P"}

    def __init__(self, send, recv, local, peers):
        self.send, self.recv, self.local, self.peers = send, recv, local, peers
        self.by_name, self.clock = {}, 0
        self.used = {"send": 0, "recv": 0, "local": 0}
        self.free = {"send": [], "local": []} | {to: [] for to in peers}
        self.waited = {to: [] for to in peers}

    def take(self, kind, pool):
        if self.free[pool]:
            return self.free[pool].pop()
        self.used[kind] += 1
        return self.used[kind] - 1

    def add(self, name, pairs):
        made = []
        for src, dst, to in pairs:
            self.clock += 1
            if to is None:
                i = self.take("local", "local")
                made.append([pltpu.make_async_copy(src, dst, self.local.at[i]), to, self.clock, i, None])
            else:
                axis, idx = self.peers[to]
                i, j = self.take("send", "send"), self.take("recv", to)
                c = pltpu.make_async_remote_copy(src, dst, self.send.at[i], self.recv.at[j], device_id={axis: idx}, device_id_type=MESH)
                made.append([c, to, self.clock, i, j])
            made[-1][0].start()
        self.by_name.setdefault(name, []).extend(made)

    def arrived(self, name):
        for m in self.by_name.get(name, ()):
            c, to, started, i, j = m
            self.clock += 1
            if to is None and i is not None:
                c.wait()
                self.free["local"].append(i)
                m[3] = None
            elif j is not None:
                c.wait_recv()
                self.waited[to].append((self.clock, j))
                m[4] = None
                back = self.BACK[to]
                self.free[back] += [k for t, k in self.waited[back] if t < started]
                self.waited[back] = [(t, k) for t, k in self.waited[back] if t >= started]

    def left(self, name):
        for m in self.by_name.get(name, ()):
            if m[1] is None:
                self.arrived(name)
            elif m[3] is not None:
                m[0].wait_send()
                self.free["send"].append(m[3])
                m[3] = None

    def finish(self):
        for name in list(self.by_name):
            self.arrived(name)
            self.left(name)


N_SEND, N_RECV, N_LOCAL = 20, 79, 16


def kernel(plan, order, panels, xa, wu, wd, za, dx, dwu, dwd, XF, GF, DF, GPB, DPB, XPB, HPB, su, sd, sw,
           wus, wds, wun, hbuf, pan, ft, dct, rst, rrc, obuf, acc, send, recv, local):
    it, un = plan
    x, y, c = lax.axis_index("cy"), lax.axis_index("cz"), lax.axis_index("cx")
    peers = {
        "R": ("cy", lax.rem(x + 1, RING)), "L": ("cy", lax.rem(x + RING - 1, RING)),
        "U": ("cz", lax.rem(y + 1, RING)), "N": ("cz", lax.rem(y + RING - 1, RING)),
        "P": ("cx", 1 - c),
    }
    barrier = pltpu.get_barrier_semaphore()
    for axis, idx in peers.values():
        pl.semaphore_signal(barrier, inc=1, device_id={axis: idx}, device_id_type=MESH)
    pl.semaphore_wait(barrier, len(peers))

    cp = Copies(send, recv, local, peers)
    blk_rows = xa.shape[1]
    sub = wd.shape[2]
    dh = wu.shape[1]
    mine = pl.ds(pl.multiple_of(c * sub, sub), sub)
    theirs = pl.ds(pl.multiple_of((1 - c) * sub, sub), sub)
    lo, hi = pl.ds(0, sub), pl.ds(sub, sub)
    at = lambda j: lax.rem(x + j, RING)
    cols = lambda j: pl.ds(pl.multiple_of(at(j) * sub, sub), sub)
    slot_of = {n: i % PAN for i, n in enumerate(panels)}
    inp, buf = (xa, za), (XF, GF)

    def group(r):
        b, first, n = GROUPS[r]
        unit_rows = blk_rows // 8
        return b, first * unit_rows, n * unit_rows

    def rel(r, k, part=None):
        _, first, n = group(r)
        start = RING * first + k * n
        return pl.ds(start, n) if part is None else pl.ds(start + part * (n // 2), n // 2)

    def span(r):
        _, first, n = group(r)
        return pl.ds(RING * first, RING * n)

    def copies_of(name):
        kind, a, r = name[0], name[-2:][0], name[-1]
        both = lambda right, left: [right + ("R",), left + ("L",)]
        updn = lambda up, down: [up + ("U",), down + ("N",)]
        if kind == WN:
            return sum([[(wu.at[:, :, cols(j)], wun.at[2 * j:2 * j + 2, :, mine], to) for to in (None, "P")] for j in range(RING)], [])
        if kind == XS or kind == YA:
            b, first, n = group(r)
            src = inp[a].at[b, pl.ds(first, n)]
            if kind == XS:
                return both((src, buf[a].at[3, b, rel(r, 0)]), (src, buf[a].at[1, b, rel(r, 0)]))
            return updn((src, buf[a].at[0, b, rel(r, 3)]), (src, buf[a].at[0, b, rel(r, 1)]))
        if kind == XR:
            b, f, s = group(r)[0], rel(r, 0, 0), rel(r, 0, 1)
            return both((buf[a].at[3, b, f], buf[a].at[2, b, f]), (buf[a].at[1, b, s], buf[a].at[2, b, s]))
        if kind in (YB, YF):
            b, m = group(r)[0], buf[a]
            js = pl.ds(1, RING - 1) if kind == YB else pl.ds(0, RING)
            return updn((m.at[js, b, rel(r, 0)], m.at[js, b, rel(r, 3)]), (m.at[js, b, rel(r, 0)], m.at[js, b, rel(r, 1)]))
        if kind == YR:
            b, m = group(r)[0], buf[a]
            return updn((m.at[0:2, b, rel(r, 3)], m.at[0:2, b, rel(r, 2)]), (m.at[2:4, b, rel(r, 1)], m.at[2:4, b, rel(r, 2)]))
        if kind in (W2, W1, WR):
            half = (lambda h, j: wu.at[h, :, cols(j)]) if r == 0 else (lambda h, j: wd.at[h, at(j)])
            piece = (lambda j: wu.at[:, :, cols(j)]) if r == 0 else (lambda j: wd.at[:, at(j)])
            st, dst = (su, sd)[r], (wus, wds)[r]
            if kind == W2:
                return both((half(0, 2), st.at[0]), (half(1, 2), st.at[1]))
            if kind == W1:
                return both((piece(1), dst.at[6:8, :, mine]), (piece(3), dst.at[2:4, :, mine]))
            return both((st.at[0], dst.at[4, :, mine]), (st.at[1], dst.at[5, :, mine]))
        if kind == WP:
            m = (wus, wds)[a]
            if r == 0:
                src = wu.at[:, :, cols(0)] if a == 0 else wd.at[:, at(0)]
                return [(src, m.at[0:2, :, mine], to) for to in (None, "P")]
            return [(m.at[2 * j:2 * j + 2, :, mine], m.at[2 * j:2 * j + 2, :, mine], "P") for j in ((1, 3) if r == 1 else (2,))]
        if kind == GP:
            return [(GF.at[:, group(r)[0], span(r), theirs], GPB.at[:, group(r)[0], span(r)], "P")]
        if kind == XP:
            return [(XF.at[0, group(r)[0], span(r)], XPB.at[group(r)[0], span(r)], "P")]
        if kind == HP:
            return [(hbuf.at[group(r)[0], span(r)], HPB.at[group(r)[0], span(r)], "P")]
        if kind in (CP, CF):
            b = group(r)[0]
            js = (pl.ds(0, 2), pl.ds(3, 1)) if kind == CP else (pl.ds(2, 1),)
            return [(DF.at[j, b, span(r), theirs], DPB.at[j, b, span(r)], "P") for j in js]
        if kind == CS:
            b, _, n = group(r)
            s = dct.at[r % 2, pl.ds(0, RING * n)]
            return both((s, DF.at[3, b, span(r)]), (s, DF.at[1, b, span(r)])) + [(s, DF.at[0, b, span(r)], None)]
        if kind == CR:
            b, first, n = group(r)
            f, s = (pl.ds(RING * first + h * 2 * n, 2 * n) for h in range(2))
            return both((DF.at[3, b, f], DF.at[2, b, f]), (DF.at[1, b, s], DF.at[2, b, s]))
        if kind in (Q2, QD, QS):
            b, first, n = group(r)
            f = ft.at[r % 2]
            own = lambda k: pl.ds(k * n, n)
            rs = pl.ds(first, n)
            if kind == Q2:
                return updn((f.at[0, own(2)], rst.at[b, 0, rs]), (f.at[1, own(2)], rst.at[b, 1, rs]))
            if kind == QD:
                return updn((f.at[1, own(1)], rrc.at[b, 0, 1, rs]), (f.at[0, own(3)], rrc.at[b, 1, 0, rs]))
            return updn((f.at[0, own(1)], rrc.at[b, 0, 0, rs]), (f.at[1, own(3)], rrc.at[b, 1, 1, rs]))
        if kind in (L1, L2, L3):
            b, _, n = group(r)
            m = {L1: XF, L2: GF, L3: DF}[kind]
            return [(m.at[:, b, span(r)], pan.at[slot_of[name], :, pl.ds(0, RING * n)], None)]
        if kind in (L5, L4):
            m, p, j = (GF, GPB, O5[r]) if kind == L5 else (DF, DPB, O4[r])
            s = pan.at[slot_of[name]]
            return [(m.at[j, :, :, mine], s.at[:, :, lo], None), (p.at[j], s.at[:, :, hi], None)]
        if kind == LH:
            return [(HPB, wds.at[0:4], None)]
        if kind == LX:
            return [(XF.at[0], wus.at[0:4], None), (XPB, wus.at[4:8], None)]
        place = {j: i for i, j in enumerate(O5)}
        if kind == O2:
            return both((obuf.at[place[2], 0], sw.at[0]), (obuf.at[place[2], 1], sw.at[1]))
        if kind == O1:
            return both((obuf.at[place[1]], dwd.at[:, x]), (obuf.at[place[3]], dwd.at[:, x]))
        assert kind == OR
        return both((sw.at[0], dwd.at[0, at(3)]), (sw.at[1], dwd.at[1, at(1)]))

    def total(terms):
        out = None
        for a, b, dims in terms:
            d = lax.dot_general(a, b, dims, preferred_element_type=jnp.float32)
            out = d if out is None else out + d
        return out

    def loop(n, body):
        def step(i, carry):
            body(i)
            return carry
        lax.fori_loop(0, n, step, 0)

    def unit(name):
        kind, r = name[0], name[-1]
        if kind in (M1, M2, M3):
            b, first, n = group(r)
            rows = pl.ds(0, RING * n)
        if kind == M1:
            p = pan.at[slot_of[L1, r]]

            def body(t):
                ns = pl.ds(pl.multiple_of(t * sub, sub), sub)
                s = total([(p[j, rows, h * dh:(h + 1) * dh], wus[2 * j + h, :, ns], NN) for j in range(RING) for h in range(2)])
                hbuf[b, span(r), ns] = s.astype(jnp.bfloat16)
            loop(2, body)
        elif kind == M2:
            p = pan.at[slot_of[L2, r]]
            if r >= 2:
                cp.left((CS, r - 2))
            d = dct.at[r % 2]
            step = min(32, RING * n)

            def body(t):
                ns = pl.ds(pl.multiple_of(t * sub, sub), sub)
                acc[rows, :] = total([(p[j, rows, :], wds[2 * j + t], NT) for j in range(RING)])

                def elem(e):
                    rs = pl.ds(pl.multiple_of(e * step, step), step)
                    hs = pl.ds(pl.multiple_of(RING * first + e * step, step), step)
                    g, s = gelu_parts(hbuf[b, hs, ns].astype(jnp.float32))
                    hbuf[b, hs, ns] = g.astype(jnp.bfloat16)
                    d[rs, ns] = (acc[rs, :] * s).astype(jnp.bfloat16)
                loop(RING * n // step, elem)
            loop(2, body)
        elif kind == M3:
            p = pan.at[slot_of[L3, r]]
            if r >= 2:
                for q in (Q2, QD, QS):
                    cp.left((q, r - 2))
            f = ft.at[r % 2]

            def body(t):
                f[t, rows, :] = total([(p[j, rows, :], wun[2 * j + t], NT) for j in range(RING)])
            loop(2, body)
        elif kind in (M5, M4):
            i0, m = PARTS[r]
            s0, s1 = (slot_of[L5 if kind == M5 else L4, i] for i in (i0, i0 + m - 1))
            j0, j1 = ((O5 if kind == M5 else O4)[i] for i in (i0, i0 + m - 1))
            own, par, p0 = (hbuf, wds, 0) if kind == M5 else (wus, wus, NB)

            def body(i):
                e, t = (0, i) if m == 1 else (i // 2, lax.rem(i, 2))
                p = pan.at[s0 + e * (s1 - s0)]
                ms = pl.ds(pl.multiple_of(t * dh, dh), dh)
                s = total([(own[g, :, ms], p[g, :, lo], TN) for g in range(NB)] + [(par[p0 + g, :, ms], p[g, :, hi], TN) for g in range(NB)])
                if kind == M5:
                    obuf[i0 + e, t] = s.astype(jnp.bfloat16)
                else:
                    dwu[t, :, cols(j0 + e * (j1 - j0))] = s.astype(jnp.bfloat16)
            loop(2 * m, body)
            if kind == M5 and O5[i0] == 0:
                cp.add((OUT, kind), [(obuf.at[i0], dwd.at[:, x], None)])
        else:
            b, first, n = group(r)
            f = ft.at[r % 2]
            rs = pl.ds(first, n)
            own = lambda k: pl.ds(k * n, n)
            if kind == QA:
                f[0, own(1), :] = f[0, own(1), :] + rst[b, 0, rs, :]
                f[1, own(3), :] = f[1, own(3), :] + rst[b, 1, rs, :]
            else:
                for h in range(2):
                    dx[b, rs, h * dh:(h + 1) * dh] = (f[h, own(0), :] + rrc[b, 0, h, rs, :] + rrc[b, 1, h, rs, :]).astype(jnp.bfloat16)

    for name, gone in order:
        for d in gone:
            cp.left(d)
        for d in (it[name][2] if name in it else un[name][1]):
            cp.arrived(d)
        if name[0] == OWN:
            own = pl.ds(0, blk_rows)
            b0, b1 = pan.at[0, :, own], pan.at[1, :, own]
            cp.add((OUT, OWN), [(xa, b0, None), (za, b1, None)])
            cp.arrived((OUT, OWN))
            pairs = []
            for r in range(NG):
                b, first, n = group(r)
                pairs += [(pan.at[a, b, pl.ds(first, n)], buf[a].at[0, b, rel(r, 0)], None) for a in (X, G)]
            cp.add(name, pairs)
        elif name in it:
            for w in {LX: (0,), LH: (1,)}.get(name[0], ()):
                for p in range(3):
                    cp.left((WP, w, p))
            cp.add(name, copies_of(name))
        else:
            unit(name)
    cp.finish()
    assert tuple(cp.used.values()) == (N_SEND, N_RECV, N_LOCAL), cp.used


def solution(mesh):
    assert mesh.shape["cy"] == RING and mesh.shape["cz"] == RING and mesh.shape["cx"] == CORES
    row_spec = P(("dp", "cx", "cz"), "cy")
    up_spec = P("cy", ("cz", "cx"))
    down_spec = P("cz", ("cy", "cx"))
    up_out = P(("dp", "cy"), ("cz", "cx"))
    down_out = P(("dp", "cz"), ("cy", "cx"))
    plan = make_plan()
    order, panels, _, _ = make_order(plan, *make_lists(plan))

    def local_step(x_act, w_up, w_down, z_grad):
        t_loc, d_loc = x_act.shape
        f_loc = w_up.shape[1]
        rows, sub, dh = t_loc // NB, f_loc // RING, d_loc // 2
        grp = RING * rows
        bf, f32 = jnp.bfloat16, jnp.float32
        xa, za = x_act.reshape(NB, rows, d_loc), z_grad.reshape(NB, rows, d_loc)
        wu = w_up.reshape(2, dh, f_loc)
        wd = w_down.reshape(CORES, RING, sub, dh)
        hbm = lambda *s: jax.ShapeDtypeStruct(s, bf)
        outs = (
            pltpu.VMEM((NB, rows, d_loc), bf), pltpu.VMEM((2, dh, f_loc), bf), hbm(CORES, RING, sub, dh),
            hbm(RING, NB, grp, d_loc), hbm(RING, NB, grp, d_loc), hbm(RING, NB, grp, 2 * sub),
            hbm(RING, NB, grp, sub), hbm(RING, NB, grp, sub), hbm(NB, grp, d_loc), hbm(NB, grp, 2 * sub),
            hbm(2, dh, sub), hbm(2, sub, dh), hbm(2, sub, dh),
        )
        scratch = [
            pltpu.VMEM((2 * RING, dh, 2 * sub), bf), pltpu.VMEM((2 * RING, sub, d_loc), bf), pltpu.VMEM((2 * RING, dh, 2 * sub), bf),
            pltpu.VMEM((NB, grp, 2 * sub), bf), pltpu.VMEM((PAN, RING, grp, d_loc), bf),
            pltpu.VMEM((2, 2, grp, dh), f32), pltpu.VMEM((2, grp, 2 * sub), bf),
            pltpu.VMEM((NB, 2, rows, dh), f32), pltpu.VMEM((NB, 2, 2, rows, dh), f32),
            pltpu.VMEM((RING, CORES, sub, dh), bf),
            pltpu.VMEM((grp, sub), f32),
            pltpu.SemaphoreType.DMA((N_SEND,)), pltpu.SemaphoreType.DMA((N_RECV,)), pltpu.SemaphoreType.DMA((N_LOCAL,)),
        ]
        any_spec = pl.BlockSpec(memory_space=pl.ANY)
        res = pl.pallas_call(
            functools.partial(kernel, plan, order, panels),
            out_shape=outs,
            in_specs=[any_spec] * 4,
            out_specs=[pl.BlockSpec(memory_space=pltpu.VMEM)] * 2 + [any_spec] * (len(outs) - 2),
            scratch_shapes=scratch,
            compiler_params=pltpu.CompilerParams(collective_id=0, has_side_effects=True, vmem_limit_bytes=61800000),
            name="mlp_bwd",
        )(xa, wu, wd, za)
        return (res[0].reshape(t_loc, d_loc), res[1].reshape(w_up.shape), res[2].reshape(w_down.shape))

    return jax.shard_map(local_step, mesh=mesh, in_specs=(row_spec, up_spec, down_spec, row_spec), out_specs=(row_spec, up_out, down_out), check_vma=False)
```

```python
import functools
import math
import string

import jax
import jax.numpy as jnp
from jax import lax
from jax.experimental import pallas as pl
from jax.experimental.pallas import tpu as pltpu
from jax.sharding import PartitionSpec as P

GELU_COEF = 0.044715
SQRT_TWO_PI = math.sqrt(2.0 / math.pi)
NN = (((1,), (0,)), ((), ()))
NT = (((1,), (1,)), ((), ()))
TN = (((0,), (0,)), ((), ()))
MESH = pl.DeviceIdType.MESH
RING = 4
CORES = 2
PAN = 3
GROUPS = ((0, 0, 8), (1, 0, 8), (2, 0, 8), (3, 0, 4), (3, 4, 4))
NB = 4
NG = len(GROUPS)
EARLY = 2
X, G = 0, 1


def gelu_parts(pre_act):
    inner_arg = SQRT_TWO_PI * (pre_act + GELU_COEF * pre_act * pre_act * pre_act)
    tanh_val = jnp.tanh(inner_arg)
    gelu_val = 0.5 * pre_act * (1.0 + tanh_val)
    gelu_slope = 0.5 * (1.0 + tanh_val) + 0.5 * pre_act * (1.0 - tanh_val * tanh_val) * SQRT_TWO_PI * (1.0 + 3.0 * GELU_COEF * pre_act * pre_act)
    return gelu_val, gelu_slope


(XS, XR, W2, W1, WR, CS, CR, O2, O1, OR, YA, YB, YF, YR, Q2, QD, QS, WN, WP, GP, XP, HP, CP, CF,
 ST, OWN, L1, L2, L3, L4, L5, LX, LH, M1, M2, M3, M4, M5, QA, QF, OUT) = range(41)
PANEL_OF = {L1: M1, L2: M2, L3: M3, L4: M4, L5: M5}
O5 = (2, 1, 3, 0)
O4 = (0, 1, 3, 2)
PARTS = ((0, 1), (1, 2), (3, 1))
PART_OF = (0, 1, 1, 2)


def full(a, r):
    return [(XS, a, r), (XR, a, r), (YR, a, r), (OWN,)] + ([(YA, a, r), (YB, a, r)] if r < EARLY else [(YF, a, r)])


def staged(r):
    return GROUPS[r][2] == 8


def make_plan():
    it, un = {}, {}
    groups = range(NG)
    for r in groups:
        q = GROUPS[r][2] / 8 / NB
        f = 4 * q
        for a in (X, G):
            it[XS, a, r] = (0, q, [])
            it[XR, a, r] = (0, q / 2, [(XS, a, r)])
            row = [(XS, a, r), (XR, a, r)]
            if r < EARLY:
                it[YA, a, r] = (1, q, [])
                it[YB, a, r] = (1, 3 * q, row)
                it[YR, a, r] = (1, 2 * q, [(YA, a, r), (YB, a, r)])
            else:
                it[YF, a, r] = (1, 4 * q, row + [(OWN,)])
                it[YR, a, r] = (1, 2 * q, [(YF, a, r)])
        it[GP, r] = (2, 8 * q, full(G, r))
        it[XP, r] = (2, 4 * q, full(X, r))
        it[HP, r] = (2, 4 * q, [(M2, r)])
        it[ST, r] = (3, f, [(M2, r)])
        it[CS, r] = (0, f, [(ST, r) if staged(r) else (M2, r)])
        it[CR, r] = (0, 2 * q, [(CS, r)])
        dc = [(ST, r), (CS, r), (CR, r)]
        it[CP, r] = (2, 6 * q, [(ST, r), (CS, r)])
        it[CF, r] = (2, 2 * q, [(CR, r)])
        it[Q2, r] = (1, q, [(M3, r)])
        it[QD, r] = (1, q, [(M3, r)])
        it[QS, r] = (1, q, [(QA, r)])
        it[L1, r] = (3, 16 * q, full(X, r))
        it[L2, r] = (3, 16 * q, full(G, r))
        it[L3, r] = (3, 16 * q, dc)
        wu = [(WP, 0, p) for p in range(3)]
        wd = [(WP, 1, p) for p in range(3)]
        un[M1, r] = (0.4 + 4.4 * f, [(L1, r)] + wu)
        un[M2, r] = (0.4 + 6.2 * f, [(L2, r), (M1, r)] + wd)
        un[M3, r] = (0.4 + 4.4 * f, [(L3, r), (WN,)] + ([(QF, r - 2)] if r >= 2 else []))
        un[QA, r] = (0.1 + 0.4 * f, [(Q2, r)])
        un[QF, r] = (0.1 + 0.4 * f, [(QS, r), (QD, r)])
    for w in range(2):
        it[W2, w] = (0, 0.5, [])
        it[W1, w] = (0, 1.0, [])
        it[WR, w] = (0, 0.5, [(W2, w)])
        it[WP, w, 0] = (2, 1, [])
        it[WP, w, 1] = (2, 2, [(W1, w)])
        it[WP, w, 2] = (2, 1, [(WR, w)])
    it[(WN,)] = (2, 4, [])
    it[(OWN,)] = (3, 2, [])
    it[(O2,)] = (0, 0.5, [(M5, 0)])
    it[(O1,)] = (0, 1.0, [(M5, 1)])
    it[(OR,)] = (0, 0.5, [(O2,)])
    for p in range(RING):
        it[L5, p] = (3, 4, [(GP, r) for r in groups] + sum([full(G, r) for r in groups], []))
        it[L4, p] = (3, 4, [(CF if O4[p] == 2 else CP, r) for r in groups] + [((ST, CS, CS, CR)[p], r) for r in groups])
    it[(LH,)] = (3, 4, [(HP, r) for r in groups] + [(M2, r) for r in groups])
    it[(LX,)] = (3, 8, [(XP, r) for r in groups] + [(M5, 0)])
    for p, (first, n) in enumerate(PARTS):
        un[M4, p] = (4.8 * n, [(L4, first + i) for i in range(n)] + [(LX,)])
        un[M5, p] = (4.8 * n, [(L5, first + i) for i in range(n)] + [(LH,)])
    return it, un


ORDER = (
    "acbdgimInhjEFHGuyJosAptvzBekflqwrxCKDLM",
    "adjbecmknfoslutvzBACGIHJghipqrwxyDKELFM",
    "shympwukqjnlfAogBaivCetxDbrzdcE",
)


def make_lists(plan):
    it, un = plan
    base = [[n for n in it if it[n][0] == k] for k in range(len(ORDER) - 1)] + [list(un)]
    *lists, units = ([names[string.ascii_letters.index(ch)] for ch in key] for names, key in zip(base, ORDER))
    return lists, units


RATE = (22.5, 22.5, 1.7, 0.4)
DELAY = (3.0, 3.0, 1.5, 1.5)


def make_order(plan, lists, units):
    it, un = plan
    done, free, pos = {}, [0.0] * 4, [0] * 4
    pend, now, order, panels, waits = list(units), 0.0, [], [], []
    late = [n for n in it if it[n][0] >= 2]
    rank = {u: i for i, u in enumerate(units)}
    user = lambda n: (PANEL_OF[n[0]], PART_OF[n[1]] if n[0] in (L4, L5) else n[1])
    panel_rank = lambda n: rank[user(n)] if n[0] in PANEL_OF else rank[{LX: M4, LH: M5}[n[0]], 0] if n[0] in (LX, LH) else -1
    gone = set()
    big = 1e9

    def ready(n):
        return all(done.get(d, big) <= now for d in it[n][2])

    def send(n):
        k = it[n][0]
        start = max(now + 0.3, free[k])
        waits.append((k, start - free[k], n))
        free[k] = start + it[n][1] * RATE[k]
        done[n] = free[k] + DELAY[k]
        order.append((n, now))

    while True:
        for k in (0, 1):
            while pos[k] < len(lists[k]) and ready(lists[k][pos[k]]):
                send(lists[k][pos[k]])
                pos[k] += 1
        for n in sorted((n for n in late if ready(n)), key=lambda n: (panel_rank(n), n)):
            if n[0] in PANEL_OF:
                if len(panels) >= PAN and user(panels[-PAN]) not in gone:
                    continue
                panels.append(n)
            late.remove(n)
            send(n)
        can = [u for u in pend if all(done.get(d, big) <= now for d in un[u][1])]
        if can:
            pend.remove(can[0])
            order.append((can[0], now))
            now += un[can[0]][0]
            done[can[0]] = now
            gone.add(can[0])
            continue
        later = [v for v in done.values() if v > now]
        if not later:
            break
        now = min(later)
    assert not pend and not late and all(pos[k] == len(lists[k]) for k in (0, 1)), (pend, late, pos)
    return [(n, [m for m in it if t - 30 < done[m] <= t - 2 and it[m][0] < 3]) for n, t in order], panels, max(done.values()), waits


class Copies:
    BACK = {"R": "L", "L": "R", "U": "N", "N": "U", "P": "P"}

    def __init__(self, send, recv, local, peers):
        self.send, self.recv, self.local, self.peers = send, recv, local, peers
        self.by_name, self.clock = {}, 0
        self.used = {"send": 0, "recv": 0, "local": 0}
        self.free = {"send": [], "local": []} | {to: [] for to in peers}
        self.waited = {to: [] for to in peers}

    def take(self, kind, pool):
        if self.free[pool]:
            return self.free[pool].pop()
        self.used[kind] += 1
        return self.used[kind] - 1

    def add(self, name, pairs):
        made = []
        for src, dst, to in pairs:
            self.clock += 1
            if to is None:
                i = self.take("local", "local")
                made.append([pltpu.make_async_copy(src, dst, self.local.at[i]), to, self.clock, i, None])
            else:
                axis, idx = self.peers[to]
                i, j = self.take("send", "send"), self.take("recv", to)
                c = pltpu.make_async_remote_copy(src, dst, self.send.at[i], self.recv.at[j], device_id={axis: idx}, device_id_type=MESH)
                made.append([c, to, self.clock, i, j])
            made[-1][0].start()
        self.by_name.setdefault(name, []).extend(made)

    def arrived(self, name):
        for m in self.by_name.get(name, ()):
            c, to, started, i, j = m
            self.clock += 1
            if to is None and i is not None:
                c.wait()
                self.free["local"].append(i)
                m[3] = None
            elif j is not None:
                c.wait_recv()
                self.waited[to].append((self.clock, j))
                m[4] = None
                back = self.BACK[to]
                self.free[back] += [k for t, k in self.waited[back] if t < started]
                self.waited[back] = [(t, k) for t, k in self.waited[back] if t >= started]

    def left(self, name):
        for m in self.by_name.get(name, ()):
            if m[1] is None:
                self.arrived(name)
            elif m[3] is not None:
                m[0].wait_send()
                self.free["send"].append(m[3])
                m[3] = None

    def finish(self):
        for name in list(self.by_name):
            self.arrived(name)
            self.left(name)


N_SEND, N_RECV, N_LOCAL = 24, 77, 16


def kernel(plan, order, panels, xa, wu, wd, za, dx, dwu, dwd, XF, GF, DF, GPB, DPB, XPB, HPB, su, sd, sw,
           wus, wds, wun, hbuf, pan, ft, rst, rrc, obuf, acc, send, recv, local):
    it, un = plan
    x, y, c = lax.axis_index("cy"), lax.axis_index("cz"), lax.axis_index("cx")
    peers = {
        "R": ("cy", lax.rem(x + 1, RING)), "L": ("cy", lax.rem(x + RING - 1, RING)),
        "U": ("cz", lax.rem(y + 1, RING)), "N": ("cz", lax.rem(y + RING - 1, RING)),
        "P": ("cx", 1 - c),
    }
    barrier = pltpu.get_barrier_semaphore()
    for axis, idx in peers.values():
        pl.semaphore_signal(barrier, inc=1, device_id={axis: idx}, device_id_type=MESH)
    pl.semaphore_wait(barrier, len(peers))

    cp = Copies(send, recv, local, peers)
    blk_rows = xa.shape[1]
    sub = wd.shape[2]
    dh = wu.shape[1]
    mine = pl.ds(pl.multiple_of(c * sub, sub), sub)
    theirs = pl.ds(pl.multiple_of((1 - c) * sub, sub), sub)
    lo, hi = pl.ds(0, sub), pl.ds(sub, sub)
    at = lambda j: lax.rem(x + j, RING)
    cols = lambda j: pl.ds(pl.multiple_of(at(j) * sub, sub), sub)
    slot_of = {n: i % PAN for i, n in enumerate(panels)}
    inp, buf = (xa, za), (XF, GF)

    def group(r):
        b, first, n = GROUPS[r]
        unit_rows = blk_rows // 8
        return b, first * unit_rows, n * unit_rows

    def rel(r, k, part=None):
        _, first, n = group(r)
        start = RING * first + k * n
        return pl.ds(start, n) if part is None else pl.ds(start + part * (n // 2), n // 2)

    def span(r):
        _, first, n = group(r)
        return pl.ds(RING * first, RING * n)

    def copies_of(name):
        kind, a, r = name[0], name[-2:][0], name[-1]
        both = lambda right, left: [right + ("R",), left + ("L",)]
        updn = lambda up, down: [up + ("U",), down + ("N",)]
        if kind == WN:
            return sum([[(wu.at[:, :, cols(j)], wun.at[2 * j:2 * j + 2, :, mine], to) for to in (None, "P")] for j in range(RING)], [])
        if kind == XS or kind == YA:
            b, first, n = group(r)
            src = inp[a].at[b, pl.ds(first, n)]
            if kind == XS:
                return both((src, buf[a].at[3, b, rel(r, 0)]), (src, buf[a].at[1, b, rel(r, 0)]))
            return updn((src, buf[a].at[0, b, rel(r, 3)]), (src, buf[a].at[0, b, rel(r, 1)]))
        if kind == XR:
            b, f, s = group(r)[0], rel(r, 0, 0), rel(r, 0, 1)
            return both((buf[a].at[3, b, f], buf[a].at[2, b, f]), (buf[a].at[1, b, s], buf[a].at[2, b, s]))
        if kind in (YB, YF):
            b, m = group(r)[0], buf[a]
            js = pl.ds(1, RING - 1) if kind == YB else pl.ds(0, RING)
            return updn((m.at[js, b, rel(r, 0)], m.at[js, b, rel(r, 3)]), (m.at[js, b, rel(r, 0)], m.at[js, b, rel(r, 1)]))
        if kind == YR:
            b, m = group(r)[0], buf[a]
            return updn((m.at[0:2, b, rel(r, 3)], m.at[0:2, b, rel(r, 2)]), (m.at[2:4, b, rel(r, 1)], m.at[2:4, b, rel(r, 2)]))
        if kind in (W2, W1, WR):
            half = (lambda h, j: wu.at[h, :, cols(j)]) if r == 0 else (lambda h, j: wd.at[h, at(j)])
            piece = (lambda j: wu.at[:, :, cols(j)]) if r == 0 else (lambda j: wd.at[:, at(j)])
            st, dst = (su, sd)[r], (wus, wds)[r]
            if kind == W2:
                return both((half(0, 2), st.at[0]), (half(1, 2), st.at[1]))
            if kind == W1:
                return both((piece(1), dst.at[6:8, :, mine]), (piece(3), dst.at[2:4, :, mine]))
            return both((st.at[0], dst.at[4, :, mine]), (st.at[1], dst.at[5, :, mine]))
        if kind == WP:
            m = (wus, wds)[a]
            if r == 0:
                src = wu.at[:, :, cols(0)] if a == 0 else wd.at[:, at(0)]
                return [(src, m.at[0:2, :, mine], to) for to in (None, "P")]
            return [(m.at[2 * j:2 * j + 2, :, mine], m.at[2 * j:2 * j + 2, :, mine], "P") for j in ((1, 3) if r == 1 else (2,))]
        if kind == GP:
            return [(GF.at[:, group(r)[0], span(r), theirs], GPB.at[:, group(r)[0], span(r)], "P")]
        if kind == XP:
            return [(XF.at[0, group(r)[0], span(r)], XPB.at[group(r)[0], span(r)], "P")]
        if kind == HP:
            return [(hbuf.at[group(r)[0], span(r)], HPB.at[group(r)[0], span(r)], "P")]
        if kind in (CP, CF):
            b = group(r)[0]
            js = (pl.ds(0, 2), pl.ds(3, 1)) if kind == CP else (pl.ds(2, 1),)
            return [(DF.at[j, b, 1 - c, span(r)], DPB.at[j, b, span(r)], "P") for j in js]
        if kind == ST:
            b = group(r)[0]
            return [(obuf.at[2, :, span(r)], DF.at[0, b, :, span(r)], None)]
        if kind == CS:
            b = group(r)[0]
            m = DF.at[0, b, :, span(r)] if staged(r) else obuf.at[2, :, span(r)]
            return both((m, DF.at[3, b, :, span(r)]), (m, DF.at[1, b, :, span(r)]))
        if kind == CR:
            b, first, n = group(r)
            f, s = (pl.ds(RING * first + h * 2 * n, 2 * n) for h in range(2))
            return both((DF.at[3, b, :, f], DF.at[2, b, :, f]), (DF.at[1, b, :, s], DF.at[2, b, :, s]))
        if kind in (Q2, QD, QS):
            b, first, n = group(r)
            f = ft.at[r % 2]
            own = lambda k: pl.ds(k * n, n)
            rs = pl.ds(first, n)
            if kind == Q2:
                return updn((f.at[0, own(2)], rst.at[b, 0, rs]), (f.at[1, own(2)], rst.at[b, 1, rs]))
            if kind == QD:
                return updn((f.at[1, own(1)], rrc.at[b, 0, 1, rs]), (f.at[0, own(3)], rrc.at[b, 1, 0, rs]))
            return updn((f.at[0, own(1)], rrc.at[b, 0, 0, rs]), (f.at[1, own(3)], rrc.at[b, 1, 1, rs]))
        if kind in (L1, L2, L3):
            b, _, n = group(r)
            to = pan.at[slot_of[name], :, pl.ds(0, RING * n)]
            if kind == L3:
                return [(DF.at[:, b, h, span(r)], to.at[:, :, h * sub:(h + 1) * sub], None) for h in range(CORES)]
            return [((XF if kind == L1 else GF).at[:, b, span(r)], to, None)]
        if kind in (L5, L4):
            m, p = (GF.at[O5[r], :, :, mine], GPB.at[O5[r]]) if kind == L5 else (DF.at[O4[r], :, c], DPB.at[O4[r]])
            s = pan.at[slot_of[name]]
            return [(m, s.at[:, :, lo], None), (p, s.at[:, :, hi], None)]
        if kind == LH:
            return [(HPB, wds.at[0:4], None)]
        if kind == LX:
            return [(XF.at[0], wus.at[0:4], None), (XPB, wus.at[4:8], None)]
        place = {j: i for i, j in enumerate(O5)}
        if kind == O2:
            return both((obuf.at[place[2], 0], sw.at[0]), (obuf.at[place[2], 1], sw.at[1]))
        if kind == O1:
            return both((obuf.at[place[1]], dwd.at[:, x]), (obuf.at[place[3]], dwd.at[:, x]))
        assert kind == OR
        return both((sw.at[0], dwd.at[0, at(3)]), (sw.at[1], dwd.at[1, at(1)]))

    def total(terms):
        out = None
        for a, b, dims in terms:
            d = lax.dot_general(a, b, dims, preferred_element_type=jnp.float32)
            out = d if out is None else out + d
        return out

    def loop(n, body):
        def step(i, carry):
            body(i)
            return carry
        lax.fori_loop(0, n, step, 0)

    def unit(name):
        kind, r = name[0], name[-1]
        if kind in (M1, M2, M3):
            b, first, n = group(r)
            rows = pl.ds(0, RING * n)
        if kind == M1:
            p = pan.at[slot_of[L1, r]]

            def body(t):
                ns = pl.ds(pl.multiple_of(t * sub, sub), sub)
                s = total([(p[j, rows, h * dh:(h + 1) * dh], wus[2 * j + h, :, ns], NN) for j in range(RING) for h in range(2)])
                hbuf[b, span(r), ns] = s.astype(jnp.bfloat16)
            loop(2, body)
        elif kind == M2:
            p = pan.at[slot_of[L2, r]]
            if r > 0 and staged(r - 1):
                cp.arrived((ST, r - 1))
            step = min(32, RING * n)

            def body(t):
                ns = pl.ds(pl.multiple_of(t * sub, sub), sub)
                acc[rows, :] = total([(p[j, rows, :], wds[2 * j + t], NT) for j in range(RING)])

                def elem(e):
                    rs = pl.ds(pl.multiple_of(e * step, step), step)
                    hs = pl.ds(pl.multiple_of(RING * first + e * step, step), step)
                    g, s = gelu_parts(hbuf[b, hs, ns].astype(jnp.float32))
                    hbuf[b, hs, ns] = g.astype(jnp.bfloat16)
                    obuf[2, t, hs, :] = (acc[rs, :] * s).astype(jnp.bfloat16)
                loop(RING * n // step, elem)
            loop(2, body)
        elif kind == M3:
            p = pan.at[slot_of[L3, r]]
            if r >= 2:
                for q in (Q2, QD, QS):
                    cp.left((q, r - 2))
            f = ft.at[r % 2]

            def body(t):
                f[t, rows, :] = total([(p[j, rows, :], wun[2 * j + t], NT) for j in range(RING)])
            loop(2, body)
        elif kind in (M5, M4):
            i0, m = PARTS[r]
            s0, s1 = (slot_of[L5 if kind == M5 else L4, i] for i in (i0, i0 + m - 1))
            j0, j1 = ((O5 if kind == M5 else O4)[i] for i in (i0, i0 + m - 1))
            own, par, p0 = (hbuf, wds, 0) if kind == M5 else (wus, wus, NB)
            if kind == M5 and i0 + m - 1 == 2:
                for g in range(NG):
                    cp.arrived((ST, g))
                    cp.left((CS, g))

            def body(i):
                e, t = (0, i) if m == 1 else (i // 2, lax.rem(i, 2))
                p = pan.at[s0 + e * (s1 - s0)]
                ms = pl.ds(pl.multiple_of(t * dh, dh), dh)
                s = total([(own[g, :, ms], p[g, :, lo], TN) for g in range(NB)] + [(par[p0 + g, :, ms], p[g, :, hi], TN) for g in range(NB)])
                if kind == M5 and O5[i0] == 0:
                    dwd[t, x] = s.astype(jnp.bfloat16)
                elif kind == M5:
                    obuf[i0 + e, t] = s.astype(jnp.bfloat16)
                else:
                    dwu[t, :, cols(j0 + e * (j1 - j0))] = s.astype(jnp.bfloat16)
            loop(2 * m, body)
        else:
            b, first, n = group(r)
            f = ft.at[r % 2]
            rs = pl.ds(first, n)
            own = lambda k: pl.ds(k * n, n)
            if kind == QA:
                f[0, own(1), :] = f[0, own(1), :] + rst[b, 0, rs, :]
                f[1, own(3), :] = f[1, own(3), :] + rst[b, 1, rs, :]
            else:
                for h in range(2):
                    dx[b, rs, h * dh:(h + 1) * dh] = (f[h, own(0), :] + rrc[b, 0, h, rs, :] + rrc[b, 1, h, rs, :]).astype(jnp.bfloat16)

    for name, gone in order:
        for d in gone:
            cp.left(d)
        for d in (it[name][2] if name in it else un[name][1]):
            cp.arrived(d)
        if name[0] == OWN:
            own = pl.ds(0, blk_rows)
            b0, b1 = pan.at[0, :, own], pan.at[1, :, own]
            cp.add((OUT, OWN), [(xa, b0, None), (za, b1, None)])
            cp.arrived((OUT, OWN))
            pairs = []
            for r in range(NG):
                b, first, n = group(r)
                pairs += [(pan.at[a, b, pl.ds(first, n)], buf[a].at[0, b, rel(r, 0)], None) for a in (X, G)]
            cp.add(name, pairs)
        elif name in it:
            for w in {LX: (0,), LH: (1,)}.get(name[0], ()):
                for p in range(3):
                    cp.left((WP, w, p))
            cp.add(name, copies_of(name))
        else:
            unit(name)
    cp.finish()
    assert tuple(cp.used.values()) == (N_SEND, N_RECV, N_LOCAL), cp.used


def solution(mesh):
    assert mesh.shape["cy"] == RING and mesh.shape["cz"] == RING and mesh.shape["cx"] == CORES
    row_spec = P(("dp", "cx", "cz"), "cy")
    up_spec = P("cy", ("cz", "cx"))
    down_spec = P("cz", ("cy", "cx"))
    up_out = P(("dp", "cy"), ("cz", "cx"))
    down_out = P(("dp", "cz"), ("cy", "cx"))
    plan = make_plan()
    order, panels, _, _ = make_order(plan, *make_lists(plan))

    def local_step(x_act, w_up, w_down, z_grad):
        t_loc, d_loc = x_act.shape
        f_loc = w_up.shape[1]
        rows, sub, dh = t_loc // NB, f_loc // RING, d_loc // 2
        grp = RING * rows
        bf, f32 = jnp.bfloat16, jnp.float32
        xa, za = x_act.reshape(NB, rows, d_loc), z_grad.reshape(NB, rows, d_loc)
        wu = w_up.reshape(2, dh, f_loc)
        wd = w_down.reshape(CORES, RING, sub, dh)
        hbm = lambda *s: jax.ShapeDtypeStruct(s, bf)
        outs = (
            pltpu.VMEM((NB, rows, d_loc), bf), pltpu.VMEM((2, dh, f_loc), bf), pltpu.VMEM((CORES, RING, sub, dh), bf),
            hbm(RING, NB, grp, d_loc), hbm(RING, NB, grp, d_loc), hbm(RING, NB, CORES, grp, sub),
            hbm(RING, NB, grp, sub), hbm(RING, NB, grp, sub), hbm(NB, grp, d_loc), hbm(NB, grp, 2 * sub),
            hbm(2, dh, sub), hbm(2, sub, dh), hbm(2, sub, dh),
        )
        scratch = [
            pltpu.VMEM((2 * RING, dh, 2 * sub), bf), pltpu.VMEM((2 * RING, sub, d_loc), bf), pltpu.VMEM((2 * RING, dh, 2 * sub), bf),
            pltpu.VMEM((NB, grp, 2 * sub), bf), pltpu.VMEM((PAN, RING, grp, d_loc), bf),
            pltpu.VMEM((2, 2, grp, dh), f32),
            pltpu.VMEM((NB, 2, rows, dh), f32), pltpu.VMEM((NB, 2, 2, rows, dh), f32),
            pltpu.VMEM((3, CORES, sub, dh), bf),
            pltpu.VMEM((grp, sub), f32),
            pltpu.SemaphoreType.DMA((N_SEND,)), pltpu.SemaphoreType.DMA((N_RECV,)), pltpu.SemaphoreType.DMA((N_LOCAL,)),
        ]
        any_spec = pl.BlockSpec(memory_space=pl.ANY)
        res = pl.pallas_call(
            functools.partial(kernel, plan, order, panels),
            out_shape=outs,
            in_specs=[any_spec] * 4,
            out_specs=[pl.BlockSpec(memory_space=pltpu.VMEM)] * 3 + [any_spec] * (len(outs) - 3),
            scratch_shapes=scratch,
            compiler_params=pltpu.CompilerParams(collective_id=0, has_side_effects=True, vmem_limit_bytes=57600000),
            name="mlp_bwd",
        )(xa, wu, wd, za)
        return (res[0].reshape(t_loc, d_loc), res[1].reshape(w_up.shape), res[2].reshape(w_down.shape))

    return jax.shard_map(local_step, mesh=mesh, in_specs=(row_spec, up_spec, down_spec, row_spec), out_specs=(row_spec, up_out, down_out), check_vma=False)
```

```python
import functools
import math
import string

import jax
import jax.numpy as jnp
from jax import lax
from jax.experimental import pallas as pl
from jax.experimental.pallas import tpu as pltpu
from jax.sharding import PartitionSpec as P

GELU_COEF = 0.044715
SQRT_TWO_PI = math.sqrt(2.0 / math.pi)
NN = (((1,), (0,)), ((), ()))
NT = (((1,), (1,)), ((), ()))
TN = (((0,), (0,)), ((), ()))
MESH = pl.DeviceIdType.MESH
RING = 4
CORES = 2
PAN = 3
GROUPS = ((0, 0, 8), (1, 0, 8), (2, 0, 8), (3, 0, 4), (3, 4, 4))
NB = 4
NG = len(GROUPS)
EARLY = 2
X, G = 0, 1


def gelu_parts(pre_act):
    inner_arg = SQRT_TWO_PI * (pre_act + GELU_COEF * pre_act * pre_act * pre_act)
    tanh_val = jnp.tanh(inner_arg)
    gelu_val = 0.5 * pre_act * (1.0 + tanh_val)
    gelu_slope = 0.5 * (1.0 + tanh_val) + 0.5 * pre_act * (1.0 - tanh_val * tanh_val) * SQRT_TWO_PI * (1.0 + 3.0 * GELU_COEF * pre_act * pre_act)
    return gelu_val, gelu_slope


(XS, XR, W2, W1, WR, CS, CR, O2, O1, OR, YA, YB, YF, YR, Q2, QD, QS, WN, WP, GP, XP, HP, CP, CF,
 ST, OWN, L1, L2, L3, L4, L5, LX, LH, M1, M2, M3, M4, M5, QA, QF, OUT) = range(41)
PANEL_OF = {L1: M1, L2: M2, L3: M3, L4: M4, L5: M5}
O5 = (2, 1, 3, 0)
O4 = (0, 1, 3, 2)
PARTS = ((0, 1), (1, 2), (3, 1))
PART_OF = [p for p, (_, n) in enumerate(PARTS) for _ in range(n)]


def full(a, r):
    return [(XS, a, r), (XR, a, r), (YR, a, r), (OWN,)] + ([(YA, a, r), (YB, a, r)] if r < EARLY else [(YF, a, r)])


def staged(r):
    return GROUPS[r][2] == 8


def make_plan():
    it, un = {}, {}
    groups = range(NG)
    for r in groups:
        q = GROUPS[r][2] / 8 / NB
        f = 4 * q
        for a in (X, G):
            it[XS, a, r] = (0, q, [])
            it[XR, a, r] = (0, q / 2, [(XS, a, r)])
            row = [(XS, a, r), (XR, a, r)]
            if r < EARLY:
                it[YA, a, r] = (1, q, [])
                it[YB, a, r] = (1, 3 * q, row)
                it[YR, a, r] = (1, 2 * q, [(YA, a, r), (YB, a, r)])
            else:
                it[YF, a, r] = (1, 4 * q, row + [(OWN,)])
                it[YR, a, r] = (1, 2 * q, [(YF, a, r)])
        it[GP, r] = (2, 8 * q, full(G, r))
        it[XP, r] = (2, 4 * q, full(X, r))
        it[HP, r] = (2, 4 * q, [(M2, r)])
        it[ST, r] = (3, f, [(M2, r)])
        it[CS, r] = (0, f, [(ST, r) if staged(r) else (M2, r)])
        it[CR, r] = (0, 2 * q, [(CS, r)])
        dc = [(ST, r), (CS, r), (CR, r)]
        it[CP, r] = (2, 6 * q, [(ST, r), (CS, r)])
        it[CF, r] = (2, 2 * q, [(CR, r)])
        it[Q2, r] = (1, q, [(M3, r)])
        it[QD, r] = (1, q, [(M3, r)])
        it[QS, r] = (1, q, [(QA, r)])
        it[L1, r] = (3, 16 * q, full(X, r))
        it[L2, r] = (3, 16 * q, full(G, r))
        it[L3, r] = (3, 16 * q, dc)
        wu = [(WP, 0, p) for p in range(3)]
        wd = [(WP, 1, p) for p in range(3)]
        un[M1, r] = (0.4 + 4.4 * f, [(L1, r)] + wu)
        un[M2, r] = (0.4 + 6.2 * f, [(L2, r), (M1, r)] + wd)
        un[M3, r] = (0.4 + 4.4 * f, [(L3, r), (WN,)] + ([(QF, r - 2)] if r >= 2 else []))
        un[QA, r] = (0.1 + 0.4 * f, [(Q2, r)])
        un[QF, r] = (0.1 + 0.4 * f, [(QS, r), (QD, r)])
    for w in range(2):
        it[W2, w] = (0, 0.5, [])
        it[W1, w] = (0, 1.0, [])
        it[WR, w] = (0, 0.5, [(W2, w)])
        it[WP, w, 0] = (2, 1, [])
        it[WP, w, 1] = (2, 2, [(W1, w)])
        it[WP, w, 2] = (2, 1, [(WR, w)])
    it[(WN,)] = (2, 4, [])
    it[(OWN,)] = (3, 2, [])
    it[(O2,)] = (0, 0.5, [(M5, 0)])
    it[(O1,)] = (0, 1.0, [(M5, 1)])
    it[(OR,)] = (0, 0.5, [(O2,)])
    for p in range(RING):
        it[L5, p] = (3, 4, [(GP, r) for r in groups] + sum([full(G, r) for r in groups], []))
        it[L4, p] = (3, 4, [(CF if O4[p] == 2 else CP, r) for r in groups] + [((ST, CS, CS, CR)[p], r) for r in groups])
    it[(LH,)] = (3, 4, [(HP, r) for r in groups] + [(M2, r) for r in groups])
    it[(LX,)] = (3, 8, [(XP, r) for r in groups] + [(M5, 0)])
    for p, (first, n) in enumerate(PARTS):
        un[M4, p] = (4.8 * n, [(L4, first + i) for i in range(n)] + [(LX,)])
        un[M5, p] = (4.8 * n, [(L5, first + i) for i in range(n)] + [(LH,)])
    return it, un


ORDER = (
    "acbdimgInhjEHGFyJosuApzteBvkflqwrxCKDML",
    "admjbecsknfolutvzBACGIHJghipqrwxyDKELFM",
    "yompqhsjlwunkfAgBtxCiveabzcrEDd",
)


def make_lists(plan):
    it, un = plan
    base = [[n for n in it if it[n][0] == k] for k in range(len(ORDER) - 1)] + [list(un)]
    *lists, units = ([names[string.ascii_letters.index(ch)] for ch in key] for names, key in zip(base, ORDER))
    return lists, units


LINKS = range(4)
RATE = (22.5,) * 2 + (1.7, 0.4)
DELAY = (3.0,) * 2 + (1.5,) * 2


def make_order(plan, lists, units):
    it, un = plan
    done, free, pos = {}, [0.0 for _ in LINKS], [0 for _ in LINKS]
    pend, now, order, panels, waits = list(units), 0.0, [], [], []
    late = [n for n in it if it[n][0] >= 2]
    rank = {u: i for i, u in enumerate(units)}
    user = lambda n: (PANEL_OF[n[0]], PART_OF[n[1]] if n[0] in (L4, L5) else n[1])
    panel_rank = lambda n: rank[user(n)] if n[0] in PANEL_OF else rank[{LX: M4, LH: M5}[n[0]], 0] if n[0] in (LX, LH) else -1
    gone = set()
    big = 1e9

    def ready(n):
        return all(done.get(d, big) <= now for d in it[n][2])

    def send(n):
        k = it[n][0]
        start = max(now + 0.3, free[k])
        waits.append((k, start - free[k], n))
        free[k] = start + it[n][1] * RATE[k]
        done[n] = free[k] + DELAY[k]
        order.append((n, now))

    while True:
        for k in (0, 1):
            while pos[k] < len(lists[k]) and ready(lists[k][pos[k]]):
                send(lists[k][pos[k]])
                pos[k] += 1
        for n in sorted((n for n in late if ready(n)), key=lambda n: (panel_rank(n), n)):
            if n[0] in PANEL_OF:
                if len(panels) >= PAN and user(panels[-PAN]) not in gone:
                    continue
                panels.append(n)
            late.remove(n)
            send(n)
        can = [u for u in pend if all(done.get(d, big) <= now for d in un[u][1])]
        if can:
            pend.remove(can[0])
            order.append((can[0], now))
            now += un[can[0]][0]
            done[can[0]] = now
            gone.add(can[0])
            continue
        later = [v for v in done.values() if v > now]
        if not later:
            break
        now = min(later)
    assert not pend and not late and all(pos[k] == len(lists[k]) for k in (0, 1)), (pend, late, pos)
    return [(n, [m for m in it if t - 30 < done[m] <= t - 2 and it[m][0] < 3]) for n, t in order], panels, max(done.values()), waits


class Copies:
    BACK = {"R": "L", "L": "R", "U": "N", "N": "U", "P": "P"}

    def __init__(self, send, recv, local, peers):
        self.send, self.recv, self.local, self.peers = send, recv, local, peers
        self.by_name, self.clock = {}, 0
        self.used = {"send": 0, "recv": 0, "local": 0}
        self.free = {"send": [], "local": []} | {to: [] for to in peers}
        self.waited = {to: [] for to in peers}

    def take(self, kind, pool):
        if self.free[pool]:
            return self.free[pool].pop()
        self.used[kind] += 1
        return self.used[kind] - 1

    def add(self, name, pairs):
        made = []
        for src, dst, to in pairs:
            self.clock += 1
            if to is None:
                i = self.take("local", "local")
                made.append([pltpu.make_async_copy(src, dst, self.local.at[i]), to, self.clock, i, None])
            else:
                axis, idx = self.peers[to]
                i, j = self.take("send", "send"), self.take("recv", to)
                c = pltpu.make_async_remote_copy(src, dst, self.send.at[i], self.recv.at[j], device_id={axis: idx}, device_id_type=MESH)
                made.append([c, to, self.clock, i, j])
            made[-1][0].start()
        self.by_name.setdefault(name, []).extend(made)

    def arrived(self, name):
        for m in self.by_name.get(name, ()):
            c, to, started, i, j = m
            self.clock += 1
            if to is None and i is not None:
                c.wait()
                self.free["local"].append(i)
                m[3] = None
            elif j is not None:
                c.wait_recv()
                self.waited[to].append((self.clock, j))
                m[4] = None
                back = self.BACK[to]
                self.free[back] += [k for t, k in self.waited[back] if t < started]
                self.waited[back] = [(t, k) for t, k in self.waited[back] if t >= started]

    def left(self, name):
        for m in self.by_name.get(name, ()):
            if m[1] is None:
                self.arrived(name)
            elif m[3] is not None:
                m[0].wait_send()
                self.free["send"].append(m[3])
                m[3] = None

    def finish(self):
        for name in list(self.by_name):
            self.arrived(name)
            self.left(name)


N_SEND, N_RECV, N_LOCAL = 26, 79, 16


def kernel(plan, order, panels, xa, wu, wd, za, dx, dwu, dwd, XF, GF, DF, GPB, DPB, XPB, HPB, su, sd, sw,
           wus, wds, wun, hbuf, pan, ft, rst, rrc, obuf, acc, send, recv, local):
    it, un = plan
    x, y, c = lax.axis_index("cy"), lax.axis_index("cz"), lax.axis_index("cx")
    peers = {
        "R": ("cy", lax.rem(x + 1, RING)), "L": ("cy", lax.rem(x + RING - 1, RING)),
        "U": ("cz", lax.rem(y + 1, RING)), "N": ("cz", lax.rem(y + RING - 1, RING)),
        "P": ("cx", 1 - c),
    }
    barrier = pltpu.get_barrier_semaphore()
    for axis, idx in peers.values():
        pl.semaphore_signal(barrier, inc=1, device_id={axis: idx}, device_id_type=MESH)
    pl.semaphore_wait(barrier, len(peers))

    cp = Copies(send, recv, local, peers)
    blk_rows = xa.shape[1]
    sub = wd.shape[2]
    dh = wu.shape[1]
    mine = pl.ds(pl.multiple_of(c * sub, sub), sub)
    theirs = pl.ds(pl.multiple_of((1 - c) * sub, sub), sub)
    lo, hi = pl.ds(0, sub), pl.ds(sub, sub)
    at = lambda j: lax.rem(x + j, RING)
    cols = lambda j: pl.ds(pl.multiple_of(at(j) * sub, sub), sub)
    slot_of = {n: i % PAN for i, n in enumerate(panels)}
    inp, buf = (xa, za), (XF, GF)

    def group(r):
        b, first, n = GROUPS[r]
        unit_rows = blk_rows // 8
        return b, first * unit_rows, n * unit_rows

    def rel(r, k, part=None):
        _, first, n = group(r)
        start = RING * first + k * n
        return pl.ds(start, n) if part is None else pl.ds(start + part * (n // 2), n // 2)

    def span(r):
        _, first, n = group(r)
        return pl.ds(RING * first, RING * n)

    def copies_of(name):
        kind, a, r = name[0], name[-2:][0], name[-1]
        both = lambda right, left: [right + ("R",), left + ("L",)]
        updn = lambda up, down: [up + ("U",), down + ("N",)]
        if kind == WN:
            return sum([[(wu.at[:, :, cols(j)], wun.at[2 * j:2 * j + 2, :, mine], to) for to in (None, "P")] for j in range(RING)], [])
        if kind == XS or kind == YA:
            b, first, n = group(r)
            src = inp[a].at[b, pl.ds(first, n)]
            if kind == XS:
                return both((src, buf[a].at[3, b, rel(r, 0)]), (src, buf[a].at[1, b, rel(r, 0)]))
            return updn((src, buf[a].at[0, b, rel(r, 3)]), (src, buf[a].at[0, b, rel(r, 1)]))
        if kind == XR:
            b, f, s = group(r)[0], rel(r, 0, 0), rel(r, 0, 1)
            return both((buf[a].at[3, b, f], buf[a].at[2, b, f]), (buf[a].at[1, b, s], buf[a].at[2, b, s]))
        if kind in (YB, YF):
            b, m = group(r)[0], buf[a]
            js = pl.ds(1, RING - 1) if kind == YB else pl.ds(0, RING)
            return updn((m.at[js, b, rel(r, 0)], m.at[js, b, rel(r, 3)]), (m.at[js, b, rel(r, 0)], m.at[js, b, rel(r, 1)]))
        if kind == YR:
            b, m = group(r)[0], buf[a]
            return updn((m.at[0:2, b, rel(r, 3)], m.at[0:2, b, rel(r, 2)]), (m.at[2:4, b, rel(r, 1)], m.at[2:4, b, rel(r, 2)]))
        if kind in (W2, W1, WR):
            half = (lambda h, j: wu.at[h, :, cols(j)]) if r == 0 else (lambda h, j: wd.at[h, at(j)])
            piece = (lambda j: wu.at[:, :, cols(j)]) if r == 0 else (lambda j: wd.at[:, at(j)])
            st, dst = (su, sd)[r], (wus, wds)[r]
            if kind == W2:
                return both((half(0, 2), st.at[0]), (half(1, 2), st.at[1]))
            if kind == W1:
                return both((piece(1), dst.at[6:8, :, mine]), (piece(3), dst.at[2:4, :, mine]))
            return both((st.at[0], dst.at[4, :, mine]), (st.at[1], dst.at[5, :, mine]))
        if kind == WP:
            m = (wus, wds)[a]
            if r == 0:
                src = wu.at[:, :, cols(0)] if a == 0 else wd.at[:, at(0)]
                return [(src, m.at[0:2, :, mine], to) for to in (None, "P")]
            return [(m.at[2 * j:2 * j + 2, :, mine], m.at[2 * j:2 * j + 2, :, mine], "P") for j in ((1, 3) if r == 1 else (2,))]
        if kind == GP:
            return [(GF.at[:, group(r)[0], span(r), theirs], GPB.at[:, group(r)[0], span(r)], "P")]
        if kind == XP:
            return [(XF.at[0, group(r)[0], span(r)], XPB.at[group(r)[0], span(r)], "P")]
        if kind == HP:
            return [(hbuf.at[group(r)[0], span(r)], HPB.at[group(r)[0], span(r)], "P")]
        if kind in (CP, CF):
            b = group(r)[0]
            js = (pl.ds(0, 2), pl.ds(3, 1)) if kind == CP else (pl.ds(2, 1),)
            return [(DF.at[j, b, 1 - c, span(r)], DPB.at[j, b, span(r)], "P") for j in js]
        if kind == ST:
            b = group(r)[0]
            return [(obuf.at[2, :, span(r)], DF.at[0, b, :, span(r)], None)]
        if kind == CS:
            b = group(r)[0]
            m = DF.at[0, b, :, span(r)] if staged(r) else obuf.at[2, :, span(r)]
            return both((m, DF.at[3, b, :, span(r)]), (m, DF.at[1, b, :, span(r)]))
        if kind == CR:
            b, first, n = group(r)
            f, s = (pl.ds(RING * first + h * 2 * n, 2 * n) for h in range(2))
            return both((DF.at[3, b, :, f], DF.at[2, b, :, f]), (DF.at[1, b, :, s], DF.at[2, b, :, s]))
        if kind in (Q2, QD, QS):
            b, first, n = group(r)
            f = ft.at[r % 2]
            own = lambda k: pl.ds(k * n, n)
            rs = pl.ds(first, n)
            if kind == Q2:
                return updn((f.at[0, own(2)], rst.at[b, 0, rs]), (f.at[1, own(2)], rst.at[b, 1, rs]))
            if kind == QD:
                return updn((f.at[1, own(1)], rrc.at[b, 0, 1, rs]), (f.at[0, own(3)], rrc.at[b, 1, 0, rs]))
            return updn((f.at[0, own(1)], rrc.at[b, 0, 0, rs]), (f.at[1, own(3)], rrc.at[b, 1, 1, rs]))
        if kind in (L1, L2, L3):
            b, _, n = group(r)
            to = pan.at[slot_of[name], :, pl.ds(0, RING * n)]
            if kind == L3:
                return [(DF.at[:, b, h, span(r)], to.at[:, :, h * sub:(h + 1) * sub], None) for h in range(CORES)]
            return [((XF if kind == L1 else GF).at[:, b, span(r)], to, None)]
        if kind in (L5, L4):
            m, p = (GF.at[O5[r], :, :, mine], GPB.at[O5[r]]) if kind == L5 else (DF.at[O4[r], :, c], DPB.at[O4[r]])
            s = pan.at[slot_of[name]]
            return [(m, s.at[:, :, lo], None), (p, s.at[:, :, hi], None)]
        if kind == LH:
            return [(HPB, wds.at[0:4], None)]
        if kind == LX:
            return [(XF.at[0], wus.at[0:4], None), (XPB, wus.at[4:8], None)]
        place = {j: i for i, j in enumerate(O5)}
        if kind == O2:
            return both((obuf.at[place[2], 0], sw.at[0]), (obuf.at[place[2], 1], sw.at[1]))
        if kind == O1:
            return both((obuf.at[place[1]], dwd.at[:, x]), (obuf.at[place[3]], dwd.at[:, x]))
        assert kind == OR
        return both((sw.at[0], dwd.at[0, at(3)]), (sw.at[1], dwd.at[1, at(1)]))

    def total(terms):
        out = None
        for a, b, dims in terms:
            d = lax.dot_general(a, b, dims, preferred_element_type=jnp.float32)
            out = d if out is None else out + d
        return out

    def loop(n, body):
        def step(i, carry):
            body(i)
            return carry
        lax.fori_loop(0, n, step, 0)

    def unit(name):
        kind, r = name[0], name[-1]
        if kind in (M1, M2, M3):
            b, first, n = group(r)
            rows = pl.ds(0, RING * n)
        if kind == M1:
            p = pan.at[slot_of[L1, r]]

            def body(t):
                ns = pl.ds(pl.multiple_of(t * sub, sub), sub)
                s = total([(p[j, rows, h * dh:(h + 1) * dh], wus[2 * j + h, :, ns], NN) for j in range(RING) for h in range(2)])
                hbuf[b, span(r), ns] = s.astype(jnp.bfloat16)
            loop(2, body)
        elif kind == M2:
            p = pan.at[slot_of[L2, r]]
            if r > 0 and staged(r - 1):
                cp.arrived((ST, r - 1))
            step = min(32, RING * n)

            def body(t):
                ns = pl.ds(pl.multiple_of(t * sub, sub), sub)
                acc[rows, :] = total([(p[j, rows, :], wds[2 * j + t], NT) for j in range(RING)])

                def elem(e):
                    rs = pl.ds(pl.multiple_of(e * step, step), step)
                    hs = pl.ds(pl.multiple_of(RING * first + e * step, step), step)
                    g, s = gelu_parts(hbuf[b, hs, ns].astype(jnp.float32))
                    hbuf[b, hs, ns] = g.astype(jnp.bfloat16)
                    obuf[2, t, hs, :] = (acc[rs, :] * s).astype(jnp.bfloat16)
                loop(RING * n // step, elem)
            loop(2, body)
        elif kind == M3:
            p = pan.at[slot_of[L3, r]]
            if r >= 2:
                for q in (Q2, QD, QS):
                    cp.left((q, r - 2))
            f = ft.at[r % 2]

            def body(t):
                f[t, rows, :] = total([(p[j, rows, :], wun[2 * j + t], NT) for j in range(RING)])
            loop(2, body)
        elif kind in (M5, M4):
            i0, m = PARTS[r]
            s0, s1 = (slot_of[L5 if kind == M5 else L4, i] for i in (i0, i0 + m - 1))
            j0, j1 = ((O5 if kind == M5 else O4)[i] for i in (i0, i0 + m - 1))
            own, par, p0 = (hbuf, wds, 0) if kind == M5 else (wus, wus, NB)
            if kind == M5 and i0 + m - 1 == 2:
                for g in range(NG):
                    cp.arrived((ST, g))
                    cp.left((CS, g))

            def body(i):
                e, t = (0, i) if m == 1 else (i // 2, lax.rem(i, 2))
                p = pan.at[s0 + e * (s1 - s0)]
                ms = pl.ds(pl.multiple_of(t * dh, dh), dh)
                s = total([(own[g, :, ms], p[g, :, lo], TN) for g in range(NB)] + [(par[p0 + g, :, ms], p[g, :, hi], TN) for g in range(NB)])
                if kind == M5 and O5[i0] == 0:
                    dwd[t, x] = s.astype(jnp.bfloat16)
                elif kind == M5:
                    obuf[i0 + e, t] = s.astype(jnp.bfloat16)
                else:
                    dwu[t, :, cols(j0 + e * (j1 - j0))] = s.astype(jnp.bfloat16)
            loop(2 * m, body)
        else:
            b, first, n = group(r)
            f = ft.at[r % 2]
            rs = pl.ds(first, n)
            own = lambda k: pl.ds(k * n, n)
            if kind == QA:
                f[0, own(1), :] = f[0, own(1), :] + rst[b, 0, rs, :]
                f[1, own(3), :] = f[1, own(3), :] + rst[b, 1, rs, :]
            else:
                for h in range(2):
                    dx[b, rs, h * dh:(h + 1) * dh] = (f[h, own(0), :] + rrc[b, 0, h, rs, :] + rrc[b, 1, h, rs, :]).astype(jnp.bfloat16)

    for name, gone in order:
        for d in gone:
            cp.left(d)
        for d in (it[name][2] if name in it else un[name][1]):
            cp.arrived(d)
        if name[0] == OWN:
            own = pl.ds(0, blk_rows)
            b0, b1 = pan.at[0, :, own], pan.at[1, :, own]
            cp.add((OUT, OWN), [(xa, b0, None), (za, b1, None)])
            cp.arrived((OUT, OWN))
            pairs = []
            for r in range(NG):
                b, first, n = group(r)
                pairs += [(pan.at[a, b, pl.ds(first, n)], buf[a].at[0, b, rel(r, 0)], None) for a in (X, G)]
            cp.add(name, pairs)
        elif name in it:
            for w in {LX: (0,), LH: (1,)}.get(name[0], ()):
                for p in range(3):
                    cp.left((WP, w, p))
            cp.add(name, copies_of(name))
        else:
            unit(name)
    cp.finish()
    assert tuple(cp.used.values()) == (N_SEND, N_RECV, N_LOCAL), cp.used


def write_out(dx, dwu, dwd, dx_out, dwu_out, dwd_out, sem):
    pairs = [(a.at[i], b.at[i]) for a, b in ((dx, dx_out), (dwu, dwu_out), (dwd, dwd_out)) for i in range(a.shape[0])]
    copies = [pltpu.make_async_copy(a, b, sem.at[i]) for i, (a, b) in enumerate(pairs)]
    for copy in copies:
        copy.start()
    for copy in copies:
        copy.wait()


def solution(mesh):
    assert mesh.shape["cy"] == RING and mesh.shape["cz"] == RING and mesh.shape["cx"] == CORES
    row_spec = P(("dp", "cx", "cz"), "cy")
    up_spec = P("cy", ("cz", "cx"))
    down_spec = P("cz", ("cy", "cx"))
    up_out = P(("dp", "cy"), ("cz", "cx"))
    down_out = P(("dp", "cz"), ("cy", "cx"))
    plan = make_plan()
    order, panels, _, _ = make_order(plan, *make_lists(plan))

    def local_step(x_act, w_up, w_down, z_grad):
        t_loc, d_loc = x_act.shape
        f_loc = w_up.shape[1]
        rows, sub, dh = t_loc // NB, f_loc // RING, d_loc // 2
        grp = RING * rows
        bf, f32 = jnp.bfloat16, jnp.float32
        xa, za = x_act.reshape(NB, rows, d_loc), z_grad.reshape(NB, rows, d_loc)
        wu = w_up.reshape(2, dh, f_loc)
        wd = w_down.reshape(CORES, RING, sub, dh)
        hbm = lambda *s: jax.ShapeDtypeStruct(s, bf)
        outs = (
            pltpu.VMEM((NB, rows, d_loc), bf), pltpu.VMEM((2, dh, f_loc), bf), pltpu.VMEM((CORES, RING, sub, dh), bf),
            hbm(RING, NB, grp, d_loc), hbm(RING, NB, grp, d_loc), hbm(RING, NB, CORES, grp, sub),
            hbm(RING, NB, grp, sub), hbm(RING, NB, grp, sub), hbm(NB, grp, d_loc), hbm(NB, grp, 2 * sub),
            hbm(2, dh, sub), hbm(2, sub, dh), hbm(2, sub, dh),
        )
        scratch = [
            pltpu.VMEM((2 * RING, dh, 2 * sub), bf), pltpu.VMEM((2 * RING, sub, d_loc), bf), pltpu.VMEM((2 * RING, dh, 2 * sub), bf),
            pltpu.VMEM((NB, grp, 2 * sub), bf), pltpu.VMEM((PAN, RING, grp, d_loc), bf),
            pltpu.VMEM((2, 2, grp, dh), f32),
            pltpu.VMEM((NB, 2, rows, dh), f32), pltpu.VMEM((NB, 2, 2, rows, dh), f32),
            pltpu.VMEM((3, CORES, sub, dh), bf),
            pltpu.VMEM((grp, sub), f32),
            pltpu.SemaphoreType.DMA((N_SEND,)), pltpu.SemaphoreType.DMA((N_RECV,)), pltpu.SemaphoreType.DMA((N_LOCAL,)),
        ]
        any_spec = pl.BlockSpec(memory_space=pl.ANY)
        res = pl.pallas_call(
            functools.partial(kernel, plan, order, panels),
            out_shape=outs,
            in_specs=[any_spec] * 4,
            out_specs=[pl.BlockSpec(memory_space=pltpu.VMEM)] * 3 + [any_spec] * (len(outs) - 3),
            scratch_shapes=scratch,
            compiler_params=pltpu.CompilerParams(collective_id=0, has_side_effects=True, vmem_limit_bytes=57600000),
            name="mlp_bwd",
        )(xa, wu, wd, za)
        outs = [pltpu.with_memory_space_constraint(o, pltpu.VMEM) for o in res[:3]]
        outs = pl.pallas_call(
            write_out,
            out_shape=[jax.ShapeDtypeStruct(o.shape, bf) for o in outs],
            in_specs=[pl.BlockSpec(memory_space=pltpu.VMEM) for _ in outs],
            out_specs=[any_spec for _ in outs],
            scratch_shapes=[pltpu.SemaphoreType.DMA((sum(o.shape[0] for o in outs),))],
            compiler_params=pltpu.CompilerParams(vmem_limit_bytes=1 << 20),
            name="write_out",
        )(*outs)
        return tuple(o.reshape(a.shape) for o, a in zip(outs, (x_act, w_up, w_down)))

    return jax.shard_map(local_step, mesh=mesh, in_specs=(row_spec, up_spec, down_spec, row_spec), out_specs=(row_spec, up_out, down_out), check_vma=False)
```

```python
import functools
import math
import string

import jax
import jax.numpy as jnp
from jax import lax
from jax.experimental import pallas as pl
from jax.experimental.pallas import tpu as pltpu
from jax.sharding import PartitionSpec as P

GELU_COEF = 0.044715
SQRT_TWO_PI = math.sqrt(2.0 / math.pi)
NN = (((1,), (0,)), ((), ()))
NT = (((1,), (1,)), ((), ()))
TN = (((0,), (0,)), ((), ()))
MESH = pl.DeviceIdType.MESH
RING = 4
CORES = 2
PAN = 3
GROUPS = ((0, 0, 8), (1, 0, 8), (2, 0, 8), (3, 0, 4), (3, 4, 4))
NB = 4
NG = len(GROUPS)
EARLY = 2
X, G = 0, 1


def gelu_parts(pre_act):
    inner_arg = SQRT_TWO_PI * (pre_act + GELU_COEF * pre_act * pre_act * pre_act)
    tanh_val = jnp.tanh(inner_arg)
    gelu_val = 0.5 * pre_act * (1.0 + tanh_val)
    gelu_slope = 0.5 * (1.0 + tanh_val) + 0.5 * pre_act * (1.0 - tanh_val * tanh_val) * SQRT_TWO_PI * (1.0 + 3.0 * GELU_COEF * pre_act * pre_act)
    return gelu_val, gelu_slope


(XS, XR, W2, W1, WR, CS, CR, O2, O1, OR, YA, YB, YF, YR, Q2, QD, QS, WN, WP, GP, XP, HP, CP, CF,
 ST, OWN, L1, L2, L3, L4, L5, LX, LH, M1, M2, M3, M4, M5, QA, QF, OUT) = range(41)
PANEL_OF = {L1: M1, L2: M2, L3: M3, L4: M4, L5: M5}
O5 = (2, 1, 3, 0)
O4 = (0, 1, 3, 2)
PARTS = ((0, 1), (1, 2), (3, 1))
PART_OF = [p for p, (_, n) in enumerate(PARTS) for _ in range(n)]


def full(a, r):
    return [(XS, a, r), (XR, a, r), (YR, a, r), (OWN,)] + ([(YA, a, r), (YB, a, r)] if r < EARLY else [(YF, a, r)])


def staged(r):
    return GROUPS[r][2] == 8


def make_plan():
    it, un = {}, {}
    groups = range(NG)
    for r in groups:
        q = GROUPS[r][2] / 8 / NB
        f = 4 * q
        for a in (X, G):
            it[XS, a, r] = (0, q, [])
            it[XR, a, r] = (0, q / 2, [(XS, a, r)])
            row = [(XS, a, r), (XR, a, r)]
            if r < EARLY:
                it[YA, a, r] = (1, q, [])
                it[YB, a, r] = (1, 3 * q, row)
                it[YR, a, r] = (1, 2 * q, [(YA, a, r), (YB, a, r)])
            else:
                it[YF, a, r] = (1, 4 * q, row + [(OWN,)])
                it[YR, a, r] = (1, 2 * q, [(YF, a, r)])
        it[GP, r] = (2, 8 * q, full(G, r))
        it[XP, r] = (2, 4 * q, full(X, r))
        it[HP, r] = (2, 4 * q, [(M2, r)])
        it[ST, r] = (3, f, [(M2, r)])
        it[CS, r] = (0, f, [(ST, r) if staged(r) else (M2, r)])
        it[CR, r] = (0, 2 * q, [(CS, r)])
        dc = [(ST, r), (CS, r), (CR, r)]
        it[CP, r] = (2, 6 * q, [(ST, r), (CS, r)])
        it[CF, r] = (2, 2 * q, [(CR, r)])
        it[Q2, r] = (1, q, [(M3, r)])
        it[QD, r] = (1, q, [(M3, r)])
        it[QS, r] = (1, q, [(QA, r)])
        it[L1, r] = (3, 16 * q, full(X, r))
        it[L2, r] = (3, 16 * q, full(G, r))
        it[L3, r] = (3, 16 * q, dc)
        wu = [(WP, 0, p) for p in range(3)]
        wd = [(WP, 1, p) for p in range(3)]
        un[M1, r] = (0.4 + 4.4 * f, [(L1, r)] + wu)
        un[M2, r] = (0.4 + 6.2 * f, [(L2, r), (M1, r)] + wd)
        un[M3, r] = (0.4 + 4.4 * f, [(L3, r), (WN,)] + ([(QF, r - 2)] if r >= 2 else []))
        un[QA, r] = (0.1 + 0.4 * f, [(Q2, r)])
        un[QF, r] = (0.1 + 0.4 * f, [(QS, r), (QD, r)])
    for w in range(2):
        it[W2, w] = (0, 0.5, [])
        it[W1, w] = (0, 1.0, [])
        it[WR, w] = (0, 0.5, [(W2, w)])
        it[WP, w, 0] = (2, 1, [])
        it[WP, w, 1] = (2, 2, [(W1, w)])
        it[WP, w, 2] = (2, 1, [(WR, w)])
    it[(WN,)] = (2, 4, [])
    it[(OWN,)] = (3, 2, [])
    it[(O2,)] = (0, 0.5, [(M5, 0)])
    it[(O1,)] = (0, 1.0, [(M5, 1)])
    it[(OR,)] = (0, 0.5, [(O2,)])
    for p in range(RING):
        it[L5, p] = (3, 4, [(GP, r) for r in groups] + sum([full(G, r) for r in groups], []))
        it[L4, p] = (3, 4, [(CF if O4[p] == 2 else CP, r) for r in groups] + [((ST, CS, CS, CR)[p], r) for r in groups])
    it[(LH,)] = (3, 4, [(HP, r) for r in groups] + [(M2, r) for r in groups])
    it[(LX,)] = (3, 8, [(XP, r) for r in groups] + [(M5, 0)])
    for p, (first, n) in enumerate(PARTS):
        un[M4, p] = (4.8 * n, [(L4, first + i) for i in range(n)] + [(LX,)])
        un[M5, p] = (4.8 * n, [(L5, first + i) for i in range(n)] + [(LH,)])
    return it, un


ORDER = (
    "acbdimgInhjEHGFyJosuApzteBvkflqwrxCKDML",
    "admjbecsknfolutvzBACGIHJghipqrwxyDKELFM",
    "yompqhsjlwunkfAgBtxCiveabzcrEDd",
)


def make_lists(plan):
    it, un = plan
    base = [[n for n in it if it[n][0] == k] for k in range(len(ORDER) - 1)] + [list(un)]
    *lists, units = ([names[string.ascii_letters.index(ch)] for ch in key] for names, key in zip(base, ORDER))
    return lists, units


LINKS = range(4)
RATE = (22.5,) * 2 + (1.7, 0.4)
DELAY = (3.0,) * 2 + (1.5,) * 2


def make_order(plan, lists, units):
    it, un = plan
    done, free, pos = {}, [0.0 for _ in LINKS], [0 for _ in LINKS]
    pend, now, order, panels, waits = list(units), 0.0, [], [], []
    late = [n for n in it if it[n][0] >= 2]
    rank = {u: i for i, u in enumerate(units)}
    user = lambda n: (PANEL_OF[n[0]], PART_OF[n[1]] if n[0] in (L4, L5) else n[1])
    panel_rank = lambda n: rank[user(n)] if n[0] in PANEL_OF else rank[{LX: M4, LH: M5}[n[0]], 0] if n[0] in (LX, LH) else -1
    gone = set()
    big = 1e9

    def ready(n):
        return all(done.get(d, big) <= now for d in it[n][2])

    def send(n):
        k = it[n][0]
        start = max(now + 0.3, free[k])
        waits.append((k, start - free[k], n))
        free[k] = start + it[n][1] * RATE[k]
        done[n] = free[k] + DELAY[k]
        order.append((n, now))

    while True:
        for k in (0, 1):
            while pos[k] < len(lists[k]) and ready(lists[k][pos[k]]):
                send(lists[k][pos[k]])
                pos[k] += 1
        for n in sorted((n for n in late if ready(n)), key=lambda n: (panel_rank(n), n)):
            if n[0] in PANEL_OF:
                if len(panels) >= PAN and user(panels[-PAN]) not in gone:
                    continue
                panels.append(n)
            late.remove(n)
            send(n)
        can = [u for u in pend if all(done.get(d, big) <= now for d in un[u][1])]
        if can:
            pend.remove(can[0])
            order.append((can[0], now))
            now += un[can[0]][0]
            done[can[0]] = now
            gone.add(can[0])
            continue
        later = [v for v in done.values() if v > now]
        if not later:
            break
        now = min(later)
    assert not pend and not late and all(pos[k] == len(lists[k]) for k in (0, 1)), (pend, late, pos)
    return [(n, [m for m in it if t - 30 < done[m] <= t - 2 and it[m][0] < 3]) for n, t in order], panels, max(done.values()), waits


class Copies:
    BACK = {"R": "L", "L": "R", "U": "N", "N": "U", "P": "P"}

    def __init__(self, send, recv, local, peers):
        self.send, self.recv, self.local, self.peers = send, recv, local, peers
        self.by_name, self.clock = {}, 0
        self.used = {"send": 0, "recv": 0, "local": 0}
        self.free = {"send": [], "local": []} | {to: [] for to in peers}
        self.waited = {to: [] for to in peers}

    def take(self, kind, pool):
        if self.free[pool]:
            return self.free[pool].pop()
        self.used[kind] += 1
        return self.used[kind] - 1

    def add(self, name, pairs):
        made = []
        for src, dst, to in pairs:
            self.clock += 1
            if to is None:
                i = self.take("local", "local")
                made.append([pltpu.make_async_copy(src, dst, self.local.at[i]), to, self.clock, i, None])
            else:
                axis, idx = self.peers[to]
                i, j = self.take("send", "send"), self.take("recv", to)
                c = pltpu.make_async_remote_copy(src, dst, self.send.at[i], self.recv.at[j], device_id={axis: idx}, device_id_type=MESH)
                made.append([c, to, self.clock, i, j])
            made[-1][0].start()
        self.by_name.setdefault(name, []).extend(made)

    def arrived(self, name):
        for m in self.by_name.get(name, ()):
            c, to, started, i, j = m
            self.clock += 1
            if to is None and i is not None:
                c.wait()
                self.free["local"].append(i)
                m[3] = None
            elif j is not None:
                c.wait_recv()
                self.waited[to].append((self.clock, j))
                m[4] = None
                back = self.BACK[to]
                self.free[back] += [k for t, k in self.waited[back] if t < started]
                self.waited[back] = [(t, k) for t, k in self.waited[back] if t >= started]

    def left(self, name):
        for m in self.by_name.get(name, ()):
            if m[1] is None:
                self.arrived(name)
            elif m[3] is not None:
                m[0].wait_send()
                self.free["send"].append(m[3])
                m[3] = None

    def finish(self):
        for name in list(self.by_name):
            self.arrived(name)
            self.left(name)


N_SEND, N_RECV, N_LOCAL = 26, 54, 16


def kernel(plan, order, panels, xa, wu, wd, za, dx, dwu, dwd, XF, GF, DF, GPB, DPB, XPB, HPB, su, sd, sw,
           wus, wds, wun, hbuf, pan, ft, rst, rrc, obuf, acc, send, recv, local):
    it, un = plan
    x, y, c = lax.axis_index("cy"), lax.axis_index("cz"), lax.axis_index("cx")
    peers = {
        "R": ("cy", lax.rem(x + 1, RING)), "L": ("cy", lax.rem(x + RING - 1, RING)),
        "U": ("cz", lax.rem(y + 1, RING)), "N": ("cz", lax.rem(y + RING - 1, RING)),
        "P": ("cx", 1 - c),
    }
    barrier = pltpu.get_barrier_semaphore()
    for axis, idx in peers.values():
        pl.semaphore_signal(barrier, inc=1, device_id={axis: idx}, device_id_type=MESH)
    pl.semaphore_wait(barrier, len(peers))

    cp = Copies(send, recv, local, peers)
    blk_rows = xa.shape[1]
    sub = wd.shape[2]
    dh = wu.shape[1]
    mine = pl.ds(pl.multiple_of(c * sub, sub), sub)
    theirs = pl.ds(pl.multiple_of((1 - c) * sub, sub), sub)
    lo, hi = pl.ds(0, sub), pl.ds(sub, sub)
    at = lambda j: lax.rem(x + j, RING)
    cols = lambda j: pl.ds(pl.multiple_of(at(j) * sub, sub), sub)
    slot_of = {n: i % PAN for i, n in enumerate(panels)}
    inp, buf = (xa, za), (XF, GF)

    def group(r):
        b, first, n = GROUPS[r]
        unit_rows = blk_rows // 8
        return b, first * unit_rows, n * unit_rows

    def rel(r, k, part=None):
        _, first, n = group(r)
        start = RING * first + k * n
        return pl.ds(start, n) if part is None else pl.ds(start + part * (n // 2), n // 2)

    def span(r):
        _, first, n = group(r)
        return pl.ds(RING * first, RING * n)

    def copies_of(name):
        kind, a, r = name[0], name[-2:][0], name[-1]
        both = lambda right, left: [right + ("R",), left + ("L",)]
        updn = lambda up, down: [up + ("U",), down + ("N",)]
        if kind == WN:
            return sum([[(wu.at[:, :, cols(j)], wun.at[2 * j:2 * j + 2, :, mine], to) for to in (None, "P")] for j in range(RING)], [])
        if kind == XS or kind == YA:
            b, first, n = group(r)
            src = inp[a].at[b, pl.ds(first, n)]
            if kind == XS:
                return both((src, buf[a].at[3, b, rel(r, 0)]), (src, buf[a].at[1, b, rel(r, 0)]))
            return updn((src, buf[a].at[0, b, rel(r, 3)]), (src, buf[a].at[0, b, rel(r, 1)]))
        if kind == XR:
            b, f, s = group(r)[0], rel(r, 0, 0), rel(r, 0, 1)
            return both((buf[a].at[3, b, f], buf[a].at[2, b, f]), (buf[a].at[1, b, s], buf[a].at[2, b, s]))
        if kind in (YB, YF):
            b, m = group(r)[0], buf[a]
            js = pl.ds(1, RING - 1) if kind == YB else pl.ds(0, RING)
            return updn((m.at[js, b, rel(r, 0)], m.at[js, b, rel(r, 3)]), (m.at[js, b, rel(r, 0)], m.at[js, b, rel(r, 1)]))
        if kind == YR:
            b, m = group(r)[0], buf[a]
            return updn((m.at[0:2, b, rel(r, 3)], m.at[0:2, b, rel(r, 2)]), (m.at[2:4, b, rel(r, 1)], m.at[2:4, b, rel(r, 2)]))
        if kind in (W2, W1, WR):
            half = (lambda h, j: wu.at[h, :, cols(j)]) if r == 0 else (lambda h, j: wd.at[h, at(j)])
            piece = (lambda j: wu.at[:, :, cols(j)]) if r == 0 else (lambda j: wd.at[:, at(j)])
            st, dst = (su, sd)[r], (wus, wds)[r]
            if kind == W2:
                return both((half(0, 2), st.at[0]), (half(1, 2), st.at[1]))
            if kind == W1:
                return both((piece(1), dst.at[6:8, :, mine]), (piece(3), dst.at[2:4, :, mine]))
            return both((st.at[0], dst.at[4, :, mine]), (st.at[1], dst.at[5, :, mine]))
        if kind == WP:
            m = (wus, wds)[a]
            if r == 0:
                src = wu.at[:, :, cols(0)] if a == 0 else wd.at[:, at(0)]
                return [(src, m.at[0:2, :, mine], to) for to in (None, "P")]
            return [(m.at[2 * j:2 * j + 2, :, mine], m.at[2 * j:2 * j + 2, :, mine], "P") for j in ((1, 3) if r == 1 else (2,))]
        if kind == GP:
            return [(GF.at[:, group(r)[0], span(r), theirs], GPB.at[:, group(r)[0], span(r)], "P")]
        if kind == XP:
            return [(XF.at[0, group(r)[0], span(r)], XPB.at[group(r)[0], span(r)], "P")]
        if kind == HP:
            return [(hbuf.at[group(r)[0], span(r)], HPB.at[group(r)[0], span(r)], "P")]
        if kind in (CP, CF):
            b = group(r)[0]
            js = (pl.ds(0, 2), pl.ds(3, 1)) if kind == CP else (pl.ds(2, 1),)
            return [(DF.at[j, b, 1 - c, span(r)], DPB.at[j, b, span(r)], "P") for j in js]
        if kind == ST:
            b = group(r)[0]
            return [(obuf.at[2, :, span(r)], DF.at[0, b, :, span(r)], None)]
        if kind == CS:
            b = group(r)[0]
            m = DF.at[0, b, :, span(r)] if staged(r) else obuf.at[2, :, span(r)]
            return both((m, DF.at[3, b, :, span(r)]), (m, DF.at[1, b, :, span(r)]))
        if kind == CR:
            b, first, n = group(r)
            f, s = (pl.ds(RING * first + h * 2 * n, 2 * n) for h in range(2))
            return both((DF.at[3, b, :, f], DF.at[2, b, :, f]), (DF.at[1, b, :, s], DF.at[2, b, :, s]))
        if kind in (Q2, QD, QS):
            b, first, n = group(r)
            f = ft.at[r % 2]
            own = lambda k: pl.ds(k * n, n)
            rs = pl.ds(first, n)
            if kind == Q2:
                return updn((f.at[0, own(2)], rst.at[b, 0, rs]), (f.at[1, own(2)], rst.at[b, 1, rs]))
            if kind == QD:
                return updn((f.at[1, own(1)], rrc.at[b, 0, 1, rs]), (f.at[0, own(3)], rrc.at[b, 1, 0, rs]))
            return updn((f.at[0, own(1)], rrc.at[b, 0, 0, rs]), (f.at[1, own(3)], rrc.at[b, 1, 1, rs]))
        if kind in (L1, L2, L3):
            b, _, n = group(r)
            to = pan.at[slot_of[name], :, pl.ds(0, RING * n)]
            if kind == L3:
                return [(DF.at[:, b, h, span(r)], to.at[:, :, h * sub:(h + 1) * sub], None) for h in range(CORES)]
            return [((XF if kind == L1 else GF).at[:, b, span(r)], to, None)]
        if kind in (L5, L4):
            m, p = (GF.at[O5[r], :, :, mine], GPB.at[O5[r]]) if kind == L5 else (DF.at[O4[r], :, c], DPB.at[O4[r]])
            s = pan.at[slot_of[name]]
            return [(m, s.at[:, :, lo], None), (p, s.at[:, :, hi], None)]
        if kind == LH:
            return [(HPB, wds.at[0:4], None)]
        if kind == LX:
            return [(XF.at[0], wus.at[0:4], None), (XPB, wus.at[4:8], None)]
        place = {j: i for i, j in enumerate(O5)}
        if kind == O2:
            return both((obuf.at[place[2], 0], sw.at[0]), (obuf.at[place[2], 1], sw.at[1]))
        if kind == O1:
            return both((obuf.at[place[1]], dwd.at[:, x]), (obuf.at[place[3]], dwd.at[:, x]))
        assert kind == OR
        return both((sw.at[0], dwd.at[0, at(3)]), (sw.at[1], dwd.at[1, at(1)]))

    def total(terms):
        out = None
        for a, b, dims in terms:
            d = lax.dot_general(a, b, dims, preferred_element_type=jnp.float32)
            out = d if out is None else out + d
        return out

    def loop(n, body):
        def step(i, carry):
            body(i)
            return carry
        lax.fori_loop(0, n, step, 0)

    def unit(name):
        kind, r = name[0], name[-1]
        if kind in (M1, M2, M3):
            b, first, n = group(r)
            rows = pl.ds(0, RING * n)
        if kind == M1:
            p = pan.at[slot_of[L1, r]]

            def body(t):
                ns = pl.ds(pl.multiple_of(t * sub, sub), sub)
                s = total([(p[j, rows, h * dh:(h + 1) * dh], wus[2 * j + h, :, ns], NN) for j in range(RING) for h in range(2)])
                hbuf[b, span(r), ns] = s.astype(jnp.bfloat16)
            loop(2, body)
        elif kind == M2:
            p = pan.at[slot_of[L2, r]]
            if r > 0 and staged(r - 1):
                cp.arrived((ST, r - 1))
            step = min(32, RING * n)

            def body(t):
                ns = pl.ds(pl.multiple_of(t * sub, sub), sub)
                acc[rows, :] = total([(p[j, rows, :], wds[2 * j + t], NT) for j in range(RING)])

                def elem(e):
                    rs = pl.ds(pl.multiple_of(e * step, step), step)
                    hs = pl.ds(pl.multiple_of(RING * first + e * step, step), step)
                    g, s = gelu_parts(hbuf[b, hs, ns].astype(jnp.float32))
                    hbuf[b, hs, ns] = g.astype(jnp.bfloat16)
                    obuf[2, t, hs, :] = (acc[rs, :] * s).astype(jnp.bfloat16)
                loop(RING * n // step, elem)
            loop(2, body)
        elif kind == M3:
            p = pan.at[slot_of[L3, r]]
            if r >= 2:
                for q in (Q2, QD, QS):
                    cp.left((q, r - 2))
            f = ft.at[r % 2]

            def body(t):
                f[t, rows, :] = total([(p[j, rows, :], wun[2 * j + t], NT) for j in range(RING)])
            loop(2, body)
        elif kind in (M5, M4):
            i0, m = PARTS[r]
            s0, s1 = (slot_of[L5 if kind == M5 else L4, i] for i in (i0, i0 + m - 1))
            j0, j1 = ((O5 if kind == M5 else O4)[i] for i in (i0, i0 + m - 1))
            own, par, p0 = (hbuf, wds, 0) if kind == M5 else (wus, wus, NB)
            if kind == M5 and i0 + m - 1 == 2:
                for g in range(NG):
                    cp.arrived((ST, g))
                    cp.left((CS, g))

            def body(i):
                e, t = (0, i) if m == 1 else (i // 2, lax.rem(i, 2))
                p = pan.at[s0 + e * (s1 - s0)]
                ms = pl.ds(pl.multiple_of(t * dh, dh), dh)
                s = total([(own[g, :, ms], p[g, :, lo], TN) for g in range(NB)] + [(par[p0 + g, :, ms], p[g, :, hi], TN) for g in range(NB)])
                if kind == M5 and O5[i0] == 0:
                    dwd[t, x] = s.astype(jnp.bfloat16)
                elif kind == M5:
                    obuf[i0 + e, t] = s.astype(jnp.bfloat16)
                else:
                    dwu[t, :, cols(j0 + e * (j1 - j0))] = s.astype(jnp.bfloat16)
            loop(2 * m, body)
        else:
            b, first, n = group(r)
            f = ft.at[r % 2]
            rs = pl.ds(first, n)
            own = lambda k: pl.ds(k * n, n)
            if kind == QA:
                f[0, own(1), :] = f[0, own(1), :] + rst[b, 0, rs, :]
                f[1, own(3), :] = f[1, own(3), :] + rst[b, 1, rs, :]
            else:
                for h in range(2):
                    dx[b, rs, h * dh:(h + 1) * dh] = (f[h, own(0), :] + rrc[b, 0, h, rs, :] + rrc[b, 1, h, rs, :]).astype(jnp.bfloat16)

    for name, gone in order:
        for d in gone:
            cp.arrived(d)
            cp.left(d)
        for d in (it[name][2] if name in it else un[name][1]):
            cp.arrived(d)
        if name[0] == OWN:
            own = pl.ds(0, blk_rows)
            b0, b1 = pan.at[0, :, own], pan.at[1, :, own]
            cp.add((OUT, OWN), [(xa, b0, None), (za, b1, None)])
            cp.arrived((OUT, OWN))
            pairs = []
            for r in range(NG):
                b, first, n = group(r)
                pairs += [(pan.at[a, b, pl.ds(first, n)], buf[a].at[0, b, rel(r, 0)], None) for a in (X, G)]
            cp.add(name, pairs)
        elif name in it:
            for w in {LX: (0,), LH: (1,)}.get(name[0], ()):
                for p in range(3):
                    cp.left((WP, w, p))
            cp.add(name, copies_of(name))
        else:
            unit(name)
    cp.finish()
    assert tuple(cp.used.values()) == (N_SEND, N_RECV, N_LOCAL), cp.used


def write_out(dx, dwu, dwd, dx_out, dwu_out, dwd_out, sem):
    pairs = [(a.at[i], b.at[i]) for a, b in ((dx, dx_out), (dwu, dwu_out), (dwd, dwd_out)) for i in range(a.shape[0])]
    copies = [pltpu.make_async_copy(a, b, sem.at[i]) for i, (a, b) in enumerate(pairs)]
    for copy in copies:
        copy.start()
    for copy in copies:
        copy.wait()


def solution(mesh):
    assert mesh.shape["cy"] == RING and mesh.shape["cz"] == RING and mesh.shape["cx"] == CORES
    row_spec = P(("dp", "cx", "cz"), "cy")
    up_spec = P("cy", ("cz", "cx"))
    down_spec = P("cz", ("cy", "cx"))
    up_out = P(("dp", "cy"), ("cz", "cx"))
    down_out = P(("dp", "cz"), ("cy", "cx"))
    plan = make_plan()
    order, panels, _, _ = make_order(plan, *make_lists(plan))

    def local_step(x_act, w_up, w_down, z_grad):
        t_loc, d_loc = x_act.shape
        f_loc = w_up.shape[1]
        rows, sub, dh = t_loc // NB, f_loc // RING, d_loc // 2
        grp = RING * rows
        bf, f32 = jnp.bfloat16, jnp.float32
        xa, za = x_act.reshape(NB, rows, d_loc), z_grad.reshape(NB, rows, d_loc)
        wu = w_up.reshape(2, dh, f_loc)
        wd = w_down.reshape(CORES, RING, sub, dh)
        hbm = lambda *s: jax.ShapeDtypeStruct(s, bf)
        outs = (
            pltpu.VMEM((NB, rows, d_loc), bf), pltpu.VMEM((2, dh, f_loc), bf), pltpu.VMEM((CORES, RING, sub, dh), bf),
            hbm(RING, NB, grp, d_loc), hbm(RING, NB, grp, d_loc), hbm(RING, NB, CORES, grp, sub),
            hbm(RING, NB, grp, sub), hbm(RING, NB, grp, sub), hbm(NB, grp, d_loc), hbm(NB, grp, 2 * sub),
            hbm(2, dh, sub), hbm(2, sub, dh), hbm(2, sub, dh),
        )
        scratch = [
            pltpu.VMEM((2 * RING, dh, 2 * sub), bf), pltpu.VMEM((2 * RING, sub, d_loc), bf), pltpu.VMEM((2 * RING, dh, 2 * sub), bf),
            pltpu.VMEM((NB, grp, 2 * sub), bf), pltpu.VMEM((PAN, RING, grp, d_loc), bf),
            pltpu.VMEM((2, 2, grp, dh), f32),
            pltpu.VMEM((NB, 2, rows, dh), f32), pltpu.VMEM((NB, 2, 2, rows, dh), f32),
            pltpu.VMEM((3, CORES, sub, dh), bf),
            pltpu.VMEM((grp, sub), f32),
            pltpu.SemaphoreType.DMA((N_SEND,)), pltpu.SemaphoreType.DMA((N_RECV,)), pltpu.SemaphoreType.DMA((N_LOCAL,)),
        ]
        any_spec = pl.BlockSpec(memory_space=pl.ANY)
        res = pl.pallas_call(
            functools.partial(kernel, plan, order, panels),
            out_shape=outs,
            in_specs=[any_spec] * 4,
            out_specs=[pl.BlockSpec(memory_space=pltpu.VMEM)] * 3 + [any_spec] * (len(outs) - 3),
            scratch_shapes=scratch,
            compiler_params=pltpu.CompilerParams(collective_id=0, has_side_effects=True, vmem_limit_bytes=57600000),
            name="mlp_bwd",
        )(xa, wu, wd, za)
        outs = [pltpu.with_memory_space_constraint(o, pltpu.VMEM) for o in res[:3]]
        outs = pl.pallas_call(
            write_out,
            out_shape=[jax.ShapeDtypeStruct(o.shape, bf) for o in outs],
            in_specs=[pl.BlockSpec(memory_space=pltpu.VMEM) for _ in outs],
            out_specs=[any_spec for _ in outs],
            scratch_shapes=[pltpu.SemaphoreType.DMA((sum(o.shape[0] for o in outs),))],
            compiler_params=pltpu.CompilerParams(vmem_limit_bytes=1 << 20),
            name="write_out",
        )(*outs)
        return tuple(o.reshape(a.shape) for o, a in zip(outs, (x_act, w_up, w_down)))

    return jax.shard_map(local_step, mesh=mesh, in_specs=(row_spec, up_spec, down_spec, row_spec), out_specs=(row_spec, up_out, down_out), check_vma=False)
```

```python
import functools
import math
import string

import jax
import jax.numpy as jnp
from jax import lax
from jax.experimental import pallas as pl
from jax.experimental.pallas import tpu as pltpu
from jax.sharding import PartitionSpec as P

GELU_COEF = 0.044715
SQRT_TWO_PI = math.sqrt(2.0 / math.pi)
NN = (((1,), (0,)), ((), ()))
NT = (((1,), (1,)), ((), ()))
TN = (((0,), (0,)), ((), ()))
MESH = pl.DeviceIdType.MESH
RING = 4
CORES = 2
PAN = 3
GROUPS = ((0, 0, 8), (1, 0, 8), (2, 0, 8), (3, 0, 4), (3, 4, 4))
NB = 4
NG = len(GROUPS)
EARLY = 2
X, G = 0, 1


def gelu_parts(pre_act):
    inner_arg = SQRT_TWO_PI * (pre_act + GELU_COEF * pre_act * pre_act * pre_act)
    tanh_val = jnp.tanh(inner_arg)
    gelu_val = 0.5 * pre_act * (1.0 + tanh_val)
    gelu_slope = 0.5 * (1.0 + tanh_val) + 0.5 * pre_act * (1.0 - tanh_val * tanh_val) * SQRT_TWO_PI * (1.0 + 3.0 * GELU_COEF * pre_act * pre_act)
    return gelu_val, gelu_slope


(XS, XR, W2, W1, WR, CS, CR, O2, O1, OR, YA, YB, YF, YR, Q2, QD, QS, WN, WP, GP, XP, HP, CP, CF,
 ST, OWN, L1, L2, L3, L4, L5, LX, LH, M1, M2, M3, M4, M5, QA, QF, OUT) = range(41)
PANEL_OF = {L1: M1, L2: M2, L3: M3, L4: M4, L5: M5}
O5 = (2, 1, 3, 0)
O4 = (0, 1, 3, 2)
PARTS = ((0, 1), (1, 2), (3, 1))
PART_OF = [p for p, (_, n) in enumerate(PARTS) for _ in range(n)]


def full(a, r):
    return [(XS, a, r), (XR, a, r), (YR, a, r), (OWN,)] + ([(YA, a, r), (YB, a, r)] if r < EARLY else [(YF, a, r)])


def staged(r):
    return GROUPS[r][2] == 8


def make_plan():
    it, un = {}, {}
    groups = range(NG)
    for r in groups:
        q = GROUPS[r][2] / 8 / NB
        f = 4 * q
        for a in (X, G):
            it[XS, a, r] = (0, q, [])
            it[XR, a, r] = (0, q / 2, [(XS, a, r)])
            row = [(XS, a, r), (XR, a, r)]
            if r < EARLY:
                it[YA, a, r] = (1, q, [])
                it[YB, a, r] = (1, 3 * q, row)
                it[YR, a, r] = (1, 2 * q, [(YA, a, r), (YB, a, r)])
            else:
                it[YF, a, r] = (1, 4 * q, row + [(OWN,)])
                it[YR, a, r] = (1, 2 * q, [(YF, a, r)])
        it[GP, r] = (2, 8 * q, full(G, r))
        it[XP, r] = (2, 4 * q, full(X, r))
        it[HP, r] = (2, 4 * q, [(M2, r)])
        it[ST, r] = (3, f, [(M2, r)])
        it[CS, r] = (0, f, [(ST, r) if staged(r) else (M2, r)])
        it[CR, r] = (0, 2 * q, [(CS, r)])
        dc = [(ST, r), (CS, r), (CR, r)]
        it[CP, r] = (2, 6 * q, [(ST, r), (CS, r)])
        it[CF, r] = (2, 2 * q, [(CR, r)])
        it[Q2, r] = (1, q, [(M3, r)])
        it[QD, r] = (1, q, [(M3, r)])
        it[QS, r] = (1, q, [(QA, r)])
        it[L1, r] = (3, 16 * q, full(X, r))
        it[L2, r] = (3, 16 * q, full(G, r))
        it[L3, r] = (3, 16 * q, dc)
        wu = [(WP, 0, p) for p in range(3)]
        wd = [(WP, 1, p) for p in range(3)]
        un[M1, r] = (0.4 + 4.4 * f, [(L1, r)] + wu)
        un[M2, r] = (0.4 + 6.2 * f, [(L2, r), (M1, r)] + wd)
        un[M3, r] = (0.4 + 4.4 * f, [(L3, r), (WN,)] + ([(QF, r - 2)] if r >= 2 else []))
        un[QA, r] = (0.1 + 0.4 * f, [(Q2, r)])
        un[QF, r] = (0.1 + 0.4 * f, [(QS, r), (QD, r)])
    for w in range(2):
        it[W2, w] = (0, 0.5, [])
        it[W1, w] = (0, 1.0, [])
        it[WR, w] = (0, 0.5, [(W2, w)])
        it[WP, w, 0] = (2, 1, [])
        it[WP, w, 1] = (2, 2, [(W1, w)])
        it[WP, w, 2] = (2, 1, [(WR, w)])
    it[(WN,)] = (2, 4, [])
    it[(OWN,)] = (3, 2, [])
    it[(O2,)] = (0, 0.5, [(M5, 0)])
    it[(O1,)] = (0, 1.0, [(M5, 1)])
    it[(OR,)] = (0, 0.5, [(O2,)])
    for p in range(RING):
        it[L5, p] = (3, 4, [(GP, r) for r in groups] + sum([full(G, r) for r in groups], []))
        it[L4, p] = (3, 4, [(CF if O4[p] == 2 else CP, r) for r in groups] + [((ST, CS, CS, CR)[p], r) for r in groups])
    it[(LH,)] = (3, 4, [(HP, r) for r in groups] + [(M2, r) for r in groups])
    it[(LX,)] = (3, 8, [(XP, r) for r in groups] + [(M5, 0)])
    for p, (first, n) in enumerate(PARTS):
        un[M4, p] = (4.8 * n, [(L4, first + i) for i in range(n)] + [(LX,)])
        un[M5, p] = (4.8 * n, [(L5, first + i) for i in range(n)] + [(LH,)])
    return it, un


ORDER = (
    "acbdimgInhjEHGFyJosuApzteBvkflqwrxCKDML",
    "admjbecsknfolutvzBACGIHJghipqrwxyDKELFM",
    "yompqhsjlwunkfAgBtxCiveabzcrEDd",
)


def make_lists(plan):
    it, un = plan
    base = [[n for n in it if it[n][0] == k] for k in range(len(ORDER) - 1)] + [list(un)]
    *lists, units = ([names[string.ascii_letters.index(ch)] for ch in key] for names, key in zip(base, ORDER))
    return lists, units


LINKS = range(4)
RATE = (22.5,) * 2 + (1.7, 0.4)
DELAY = (3.0,) * 2 + (1.5,) * 2


def make_order(plan, lists, units):
    it, un = plan
    done, free, pos = {}, [0.0 for _ in LINKS], [0 for _ in LINKS]
    pend, now, order, panels, waits = list(units), 0.0, [], [], []
    late = [n for n in it if it[n][0] >= 2]
    rank = {u: i for i, u in enumerate(units)}
    user = lambda n: (PANEL_OF[n[0]], PART_OF[n[1]] if n[0] in (L4, L5) else n[1])
    panel_rank = lambda n: rank[user(n)] if n[0] in PANEL_OF else rank[{LX: M4, LH: M5}[n[0]], 0] if n[0] in (LX, LH) else -1
    gone = set()
    big = 1e9

    def ready(n):
        return all(done.get(d, big) <= now for d in it[n][2])

    def send(n):
        k = it[n][0]
        start = max(now + 0.3, free[k])
        waits.append((k, start - free[k], n))
        free[k] = start + it[n][1] * RATE[k]
        done[n] = free[k] + DELAY[k]
        order.append((n, now))

    while True:
        for k in (0, 1):
            while pos[k] < len(lists[k]) and ready(lists[k][pos[k]]):
                send(lists[k][pos[k]])
                pos[k] += 1
        for n in sorted((n for n in late if ready(n)), key=lambda n: (panel_rank(n), n)):
            if n[0] in PANEL_OF:
                if len(panels) >= PAN and user(panels[-PAN]) not in gone:
                    continue
                panels.append(n)
            late.remove(n)
            send(n)
        can = [u for u in pend if all(done.get(d, big) <= now for d in un[u][1])]
        if can:
            pend.remove(can[0])
            order.append((can[0], now))
            now += un[can[0]][0]
            done[can[0]] = now
            gone.add(can[0])
            continue
        later = [v for v in done.values() if v > now]
        if not later:
            break
        now = min(later)
    assert not pend and not late and all(pos[k] == len(lists[k]) for k in (0, 1)), (pend, late, pos)
    return [(n, [m for m in it if t - 30 < done[m] <= t - 2 and it[m][0] < 3]) for n, t in order], panels, max(done.values()), waits


class Copies:
    BACK = {"R": "L", "L": "R", "U": "N", "N": "U", "P": "P"}

    def __init__(self, send, recv, local, peers):
        self.send, self.recv, self.local, self.peers = send, recv, local, peers
        self.by_name, self.clock = {}, 0
        self.used = {"send": 0, "recv": 0, "local": 0}
        self.free = {"send": [], "local": []} | {to: [] for to in peers}
        self.waited = {to: [] for to in peers}

    def take(self, kind, pool):
        if self.free[pool]:
            return self.free[pool].pop()
        self.used[kind] += 1
        return self.used[kind] - 1

    def add(self, name, pairs):
        made = []
        for src, dst, to in pairs:
            self.clock += 1
            if to is None:
                i = self.take("local", "local")
                made.append([pltpu.make_async_copy(src, dst, self.local.at[i]), to, self.clock, i, None])
            else:
                axis, idx = self.peers[to]
                i, j = self.take("send", "send"), self.take("recv", to)
                c = pltpu.make_async_remote_copy(src, dst, self.send.at[i], self.recv.at[j], device_id={axis: idx}, device_id_type=MESH)
                made.append([c, to, self.clock, i, j])
            made[-1][0].start()
        self.by_name.setdefault(name, []).extend(made)

    def arrived(self, name):
        for m in self.by_name.get(name, ()):
            c, to, started, i, j = m
            self.clock += 1
            if to is None and i is not None:
                c.wait()
                self.free["local"].append(i)
                m[3] = None
            elif j is not None:
                c.wait_recv()
                self.waited[to].append((self.clock, j))
                m[4] = None
                back = self.BACK[to]
                self.free[back] += [k for t, k in self.waited[back] if t < started]
                self.waited[back] = [(t, k) for t, k in self.waited[back] if t >= started]

    def left(self, name):
        for m in self.by_name.get(name, ()):
            if m[1] is None:
                self.arrived(name)
            elif m[3] is not None:
                m[0].wait_send()
                self.free["send"].append(m[3])
                m[3] = None

    def finish(self):
        for name in list(self.by_name):
            self.arrived(name)
            self.left(name)


PIECES = 4
N_SEND, N_RECV, N_LOCAL = 26, 54, 16


def work(plan, order, panels, xa, wu, wd, za, dx, dwu, dwd, XF, GF, DF, GPB, DPB, XPB, HPB, su, sd, sw,
           wus, wds, wun, hbuf, pan, ft, rst, rrc, obuf, acc, send, recv, local):
    it, un = plan
    x, y, c = lax.axis_index("cy"), lax.axis_index("cz"), lax.axis_index("cx")
    peers = {
        "R": ("cy", lax.rem(x + 1, RING)), "L": ("cy", lax.rem(x + RING - 1, RING)),
        "U": ("cz", lax.rem(y + 1, RING)), "N": ("cz", lax.rem(y + RING - 1, RING)),
        "P": ("cx", 1 - c),
    }
    barrier = pltpu.get_barrier_semaphore()
    for axis, idx in peers.values():
        pl.semaphore_signal(barrier, inc=1, device_id={axis: idx}, device_id_type=MESH)
    pl.semaphore_wait(barrier, len(peers))

    cp = Copies(send, recv, local, peers)
    blk_rows = xa.shape[1]
    sub = wd.shape[2]
    dh = wu.shape[1]
    mine = pl.ds(pl.multiple_of(c * sub, sub), sub)
    theirs = pl.ds(pl.multiple_of((1 - c) * sub, sub), sub)
    lo, hi = pl.ds(0, sub), pl.ds(sub, sub)
    at = lambda j: lax.rem(x + j, RING)
    cols = lambda j: pl.ds(pl.multiple_of(at(j) * sub, sub), sub)
    slot_of = {n: i % PAN for i, n in enumerate(panels)}
    inp, buf = (xa, za), (XF, GF)

    def group(r):
        b, first, n = GROUPS[r]
        unit_rows = blk_rows // 8
        return b, first * unit_rows, n * unit_rows

    def rel(r, k, part=None):
        _, first, n = group(r)
        start = RING * first + k * n
        return pl.ds(start, n) if part is None else pl.ds(start + part * (n // 2), n // 2)

    def span(r):
        _, first, n = group(r)
        return pl.ds(RING * first, RING * n)

    def copies_of(name):
        kind, a, r = name[0], name[-2:][0], name[-1]
        both = lambda right, left: [right + ("R",), left + ("L",)]
        updn = lambda up, down: [up + ("U",), down + ("N",)]
        if kind == WN:
            return sum([[(wu.at[:, :, cols(j)], wun.at[2 * j:2 * j + 2, :, mine], to) for to in (None, "P")] for j in range(RING)], [])
        if kind == XS or kind == YA:
            b, first, n = group(r)
            src = inp[a].at[b, pl.ds(first, n)]
            if kind == XS:
                return both((src, buf[a].at[3, b, rel(r, 0)]), (src, buf[a].at[1, b, rel(r, 0)]))
            return updn((src, buf[a].at[0, b, rel(r, 3)]), (src, buf[a].at[0, b, rel(r, 1)]))
        if kind == XR:
            b, f, s = group(r)[0], rel(r, 0, 0), rel(r, 0, 1)
            return both((buf[a].at[3, b, f], buf[a].at[2, b, f]), (buf[a].at[1, b, s], buf[a].at[2, b, s]))
        if kind in (YB, YF):
            b, m = group(r)[0], buf[a]
            js = pl.ds(1, RING - 1) if kind == YB else pl.ds(0, RING)
            return updn((m.at[js, b, rel(r, 0)], m.at[js, b, rel(r, 3)]), (m.at[js, b, rel(r, 0)], m.at[js, b, rel(r, 1)]))
        if kind == YR:
            b, m = group(r)[0], buf[a]
            return updn((m.at[0:2, b, rel(r, 3)], m.at[0:2, b, rel(r, 2)]), (m.at[2:4, b, rel(r, 1)], m.at[2:4, b, rel(r, 2)]))
        if kind in (W2, W1, WR):
            half = (lambda h, j: wu.at[h, :, cols(j)]) if r == 0 else (lambda h, j: wd.at[h, at(j)])
            piece = (lambda j: wu.at[:, :, cols(j)]) if r == 0 else (lambda j: wd.at[:, at(j)])
            st, dst = (su, sd)[r], (wus, wds)[r]
            if kind == W2:
                return both((half(0, 2), st.at[0]), (half(1, 2), st.at[1]))
            if kind == W1:
                return both((piece(1), dst.at[6:8, :, mine]), (piece(3), dst.at[2:4, :, mine]))
            return both((st.at[0], dst.at[4, :, mine]), (st.at[1], dst.at[5, :, mine]))
        if kind == WP:
            m = (wus, wds)[a]
            if r == 0:
                src = wu.at[:, :, cols(0)] if a == 0 else wd.at[:, at(0)]
                return [(src, m.at[0:2, :, mine], to) for to in (None, "P")]
            return [(m.at[2 * j:2 * j + 2, :, mine], m.at[2 * j:2 * j + 2, :, mine], "P") for j in ((1, 3) if r == 1 else (2,))]
        if kind == GP:
            return [(GF.at[:, group(r)[0], span(r), theirs], GPB.at[:, group(r)[0], span(r)], "P")]
        if kind == XP:
            return [(XF.at[0, group(r)[0], span(r)], XPB.at[group(r)[0], span(r)], "P")]
        if kind == HP:
            return [(hbuf.at[group(r)[0], span(r)], HPB.at[group(r)[0], span(r)], "P")]
        if kind in (CP, CF):
            b = group(r)[0]
            js = (pl.ds(0, 2), pl.ds(3, 1)) if kind == CP else (pl.ds(2, 1),)
            return [(DF.at[j, b, 1 - c, span(r)], DPB.at[j, b, span(r)], "P") for j in js]
        if kind == ST:
            b = group(r)[0]
            return [(obuf.at[2, :, span(r)], DF.at[0, b, :, span(r)], None)]
        if kind == CS:
            b = group(r)[0]
            m = DF.at[0, b, :, span(r)] if staged(r) else obuf.at[2, :, span(r)]
            return both((m, DF.at[3, b, :, span(r)]), (m, DF.at[1, b, :, span(r)]))
        if kind == CR:
            b, first, n = group(r)
            f, s = (pl.ds(RING * first + h * 2 * n, 2 * n) for h in range(2))
            return both((DF.at[3, b, :, f], DF.at[2, b, :, f]), (DF.at[1, b, :, s], DF.at[2, b, :, s]))
        if kind in (Q2, QD, QS):
            b, first, n = group(r)
            f = ft.at[r % 2]
            own = lambda k: pl.ds(k * n, n)
            rs = pl.ds(first, n)
            if kind == Q2:
                return updn((f.at[0, own(2)], rst.at[b, 0, rs]), (f.at[1, own(2)], rst.at[b, 1, rs]))
            if kind == QD:
                return updn((f.at[1, own(1)], rrc.at[b, 0, 1, rs]), (f.at[0, own(3)], rrc.at[b, 1, 0, rs]))
            return updn((f.at[0, own(1)], rrc.at[b, 0, 0, rs]), (f.at[1, own(3)], rrc.at[b, 1, 1, rs]))
        if kind in (L1, L2, L3):
            b, _, n = group(r)
            to = pan.at[slot_of[name], :, pl.ds(0, RING * n)]
            if kind == L3:
                return [(DF.at[:, b, h, span(r)], to.at[:, :, h * sub:(h + 1) * sub], None) for h in range(CORES)]
            return [((XF if kind == L1 else GF).at[:, b, span(r)], to, None)]
        if kind in (L5, L4):
            m, p = (GF.at[O5[r], :, :, mine], GPB.at[O5[r]]) if kind == L5 else (DF.at[O4[r], :, c], DPB.at[O4[r]])
            s = pan.at[slot_of[name]]
            return [(m, s.at[:, :, lo], None), (p, s.at[:, :, hi], None)]
        if kind == LH:
            return [(HPB, wds.at[0:4], None)]
        if kind == LX:
            return [(XF.at[0], wus.at[0:4], None), (XPB, wus.at[4:8], None)]
        place = {j: i for i, j in enumerate(O5)}
        if kind == O2:
            return both((obuf.at[place[2], 0], sw.at[0]), (obuf.at[place[2], 1], sw.at[1]))
        if kind == O1:
            return both((obuf.at[place[1]], dwd.at[:, x]), (obuf.at[place[3]], dwd.at[:, x]))
        assert kind == OR
        return both((sw.at[0], dwd.at[0, at(3)]), (sw.at[1], dwd.at[1, at(1)]))

    def total(terms):
        out = None
        for a, b, dims in terms:
            d = lax.dot_general(a, b, dims, preferred_element_type=jnp.float32)
            out = d if out is None else out + d
        return out

    def loop(n, body):
        def step(i, carry):
            body(i)
            return carry
        lax.fori_loop(0, n, step, 0)

    def unit(name):
        kind, r = name[0], name[-1]
        if kind in (M1, M2, M3):
            b, first, n = group(r)
            rows = pl.ds(0, RING * n)
        if kind == M1:
            p = pan.at[slot_of[L1, r]]

            def body(t):
                ns = pl.ds(pl.multiple_of(t * sub, sub), sub)
                s = total([(p[j, rows, h * dh:(h + 1) * dh], wus[2 * j + h, :, ns], NN) for j in range(RING) for h in range(2)])
                hbuf[b, span(r), ns] = s.astype(jnp.bfloat16)
            loop(2, body)
        elif kind == M2:
            p = pan.at[slot_of[L2, r]]
            if r > 0 and staged(r - 1):
                cp.arrived((ST, r - 1))
            step = min(32, RING * n)

            def body(t):
                ns = pl.ds(pl.multiple_of(t * sub, sub), sub)
                acc[rows, :] = total([(p[j, rows, :], wds[2 * j + t], NT) for j in range(RING)])

                def elem(e):
                    rs = pl.ds(pl.multiple_of(e * step, step), step)
                    hs = pl.ds(pl.multiple_of(RING * first + e * step, step), step)
                    g, s = gelu_parts(hbuf[b, hs, ns].astype(jnp.float32))
                    hbuf[b, hs, ns] = g.astype(jnp.bfloat16)
                    obuf[2, t, hs, :] = (acc[rs, :] * s).astype(jnp.bfloat16)
                loop(RING * n // step, elem)
            loop(2, body)
        elif kind == M3:
            p = pan.at[slot_of[L3, r]]
            if r >= 2:
                for q in (Q2, QD, QS):
                    cp.left((q, r - 2))
            f = ft.at[r % 2]

            def body(t):
                f[t, rows, :] = total([(p[j, rows, :], wun[2 * j + t], NT) for j in range(RING)])
            loop(2, body)
        elif kind in (M5, M4):
            i0, m = PARTS[r]
            s0, s1 = (slot_of[L5 if kind == M5 else L4, i] for i in (i0, i0 + m - 1))
            j0, j1 = ((O5 if kind == M5 else O4)[i] for i in (i0, i0 + m - 1))
            own, par, p0 = (hbuf, wds, 0) if kind == M5 else (wus, wus, NB)
            if kind == M5 and i0 + m - 1 == 2:
                for g in range(NG):
                    cp.arrived((ST, g))
                    cp.left((CS, g))

            def body(i):
                e, t = (0, i) if m == 1 else (i // 2, lax.rem(i, 2))
                p = pan.at[s0 + e * (s1 - s0)]
                ms = pl.ds(pl.multiple_of(t * dh, dh), dh)
                s = total([(own[g, :, ms], p[g, :, lo], TN) for g in range(NB)] + [(par[p0 + g, :, ms], p[g, :, hi], TN) for g in range(NB)])
                if kind == M5 and O5[i0] == 0:
                    dwd[t, x] = s.astype(jnp.bfloat16)
                elif kind == M5:
                    obuf[i0 + e, t] = s.astype(jnp.bfloat16)
                else:
                    dwu[t, :, cols(j0 + e * (j1 - j0))] = s.astype(jnp.bfloat16)
            loop(2 * m, body)
        else:
            b, first, n = group(r)
            f = ft.at[r % 2]
            rs = pl.ds(first, n)
            own = lambda k: pl.ds(k * n, n)
            if kind == QA:
                f[0, own(1), :] = f[0, own(1), :] + rst[b, 0, rs, :]
                f[1, own(3), :] = f[1, own(3), :] + rst[b, 1, rs, :]
            else:
                for h in range(2):
                    dx[b, rs, h * dh:(h + 1) * dh] = (f[h, own(0), :] + rrc[b, 0, h, rs, :] + rrc[b, 1, h, rs, :]).astype(jnp.bfloat16)

    for name, gone in order:
        for d in gone:
            cp.arrived(d)
            cp.left(d)
        for d in (it[name][2] if name in it else un[name][1]):
            cp.arrived(d)
        if name[0] == OWN:
            own = pl.ds(0, blk_rows)
            b0, b1 = pan.at[0, :, own], pan.at[1, :, own]
            cp.add((OUT, OWN), [(xa, b0, None), (za, b1, None)])
            cp.arrived((OUT, OWN))
            pairs = []
            for r in range(NG):
                b, first, n = group(r)
                pairs += [(pan.at[a, b, pl.ds(first, n)], buf[a].at[0, b, rel(r, 0)], None) for a in (X, G)]
            cp.add(name, pairs)
        elif name in it:
            for w in {LX: (0,), LH: (1,)}.get(name[0], ()):
                for p in range(3):
                    cp.left((WP, w, p))
            cp.add(name, copies_of(name))
        else:
            unit(name)
    cp.finish()
    assert tuple(cp.used.values()) == (N_SEND, N_RECV, N_LOCAL), cp.used


def kernel(plan, order, panels, *refs):
    pl.run_scoped(functools.partial(work, plan, order, panels, *refs), *(pltpu.SemaphoreType.DMA((n,)) for n in (N_SEND, N_RECV, N_LOCAL)))


def write_out(dx, dwu, dwd, dx_out, dwu_out, dwd_out, sem):
    arrays = ((dx, dx_out), (dwu, dwu_out), (dwd, dwd_out))
    for i, (a, b) in enumerate(arrays):
        n = a.shape[1] // PIECES
        for j in range(a.shape[0]):
            for p in range(PIECES):
                rows = pl.ds(p * n, n)
                pltpu.make_async_copy(a.at[j, rows], b.at[j, rows], sem.at[i]).start()
    for i, (a, b) in enumerate(arrays):
        pltpu.make_async_copy(a, b, sem.at[i]).wait()


def solution(mesh):
    assert mesh.shape["cy"] == RING and mesh.shape["cz"] == RING and mesh.shape["cx"] == CORES
    row_spec = P(("dp", "cx", "cz"), "cy")
    up_spec = P("cy", ("cz", "cx"))
    down_spec = P("cz", ("cy", "cx"))
    up_out = P(("dp", "cy"), ("cz", "cx"))
    down_out = P(("dp", "cz"), ("cy", "cx"))
    plan = make_plan()
    order, panels, _, _ = make_order(plan, *make_lists(plan))

    def local_step(x_act, w_up, w_down, z_grad):
        t_loc, d_loc = x_act.shape
        f_loc = w_up.shape[1]
        rows, sub, dh = t_loc // NB, f_loc // RING, d_loc // 2
        grp = RING * rows
        bf, f32 = jnp.bfloat16, jnp.float32
        xa, za = x_act.reshape(NB, rows, d_loc), z_grad.reshape(NB, rows, d_loc)
        wu = w_up.reshape(2, dh, f_loc)
        wd = w_down.reshape(CORES, RING, sub, dh)
        hbm = lambda *s: jax.ShapeDtypeStruct(s, bf)
        outs = (
            pltpu.VMEM((NB, rows, d_loc), bf), pltpu.VMEM((2, dh, f_loc), bf), pltpu.VMEM((CORES, RING, sub, dh), bf),
            hbm(RING, NB, grp, d_loc), hbm(RING, NB, grp, d_loc), hbm(RING, NB, CORES, grp, sub),
            hbm(RING, NB, grp, sub), hbm(RING, NB, grp, sub), hbm(NB, grp, d_loc), hbm(NB, grp, 2 * sub),
            hbm(2, dh, sub), hbm(2, sub, dh), hbm(2, sub, dh),
        )
        scratch = [
            pltpu.VMEM((2 * RING, dh, 2 * sub), bf), pltpu.VMEM((2 * RING, sub, d_loc), bf), pltpu.VMEM((2 * RING, dh, 2 * sub), bf),
            pltpu.VMEM((NB, grp, 2 * sub), bf), pltpu.VMEM((PAN, RING, grp, d_loc), bf),
            pltpu.VMEM((2, 2, grp, dh), f32),
            pltpu.VMEM((NB, 2, rows, dh), f32), pltpu.VMEM((NB, 2, 2, rows, dh), f32),
            pltpu.VMEM((3, CORES, sub, dh), bf),
            pltpu.VMEM((grp, sub), f32),
        ]
        any_spec = pl.BlockSpec(memory_space=pl.ANY)
        res = pl.pallas_call(
            functools.partial(kernel, plan, order, panels),
            out_shape=outs,
            in_specs=[any_spec] * 4,
            out_specs=[pl.BlockSpec(memory_space=pltpu.VMEM)] * 3 + [any_spec] * (len(outs) - 3),
            scratch_shapes=scratch,
            compiler_params=pltpu.CompilerParams(collective_id=0, has_side_effects=True, vmem_limit_bytes=57600000),
            name="mlp_bwd",
        )(xa, wu, wd, za)
        outs = [pltpu.with_memory_space_constraint(o, pltpu.VMEM) for o in res[:3]]
        outs = pl.pallas_call(
            write_out,
            out_shape=[jax.ShapeDtypeStruct(o.shape, bf) for o in outs],
            in_specs=[pl.BlockSpec(memory_space=pltpu.VMEM) for _ in outs],
            out_specs=[any_spec for _ in outs],
            scratch_shapes=[pltpu.SemaphoreType.DMA((len(outs),))],
            compiler_params=pltpu.CompilerParams(vmem_limit_bytes=1 << 20),
            name="write_out",
        )(*outs)
        return tuple(o.reshape(a.shape) for o, a in zip(outs, (x_act, w_up, w_down)))

    return jax.shard_map(local_step, mesh=mesh, in_specs=(row_spec, up_spec, down_spec, row_spec), out_specs=(row_spec, up_out, down_out), check_vma=False)
```

```python
import functools
import math
import string

import jax
import jax.numpy as jnp
from jax import lax
from jax.experimental import pallas as pl
from jax.experimental.pallas import tpu as pltpu
from jax.sharding import PartitionSpec as P

GELU_COEF = 0.044715
SQRT_TWO_PI = math.sqrt(2.0 / math.pi)
NN = (((1,), (0,)), ((), ()))
NT = (((1,), (1,)), ((), ()))
TN = (((0,), (0,)), ((), ()))
MESH = pl.DeviceIdType.MESH
RING = 4
CORES = 2
PAN = 3
GROUPS = ((0, 0, 8), (1, 0, 8), (2, 0, 8), (3, 0, 4), (3, 4, 4))
NB = 4
NG = len(GROUPS)
EARLY = 2
X, G = 0, 1


def gelu_parts(pre_act):
    inner_arg = SQRT_TWO_PI * (pre_act + GELU_COEF * pre_act * pre_act * pre_act)
    tanh_val = jnp.tanh(inner_arg)
    gelu_val = 0.5 * pre_act * (1.0 + tanh_val)
    gelu_slope = 0.5 * (1.0 + tanh_val) + 0.5 * pre_act * (1.0 - tanh_val * tanh_val) * SQRT_TWO_PI * (1.0 + 3.0 * GELU_COEF * pre_act * pre_act)
    return gelu_val, gelu_slope


(XS, XR, W2, W1, WR, CS, CR, O2, O1, OR, YA, YB, YF, YR, Q2, QD, QS, WN, WP, GP, XP, HP, CP, CF,
 ST, OWN, L1, L2, L3, L4, L5, LX, LH, M1, M2, M3, M4, M5, QA, QF, OUT) = range(41)
PANEL_OF = {L1: M1, L2: M2, L3: M3, L4: M4, L5: M5}
O5 = (2, 1, 3, 0)
O4 = (0, 1, 3, 2)
PARTS = ((0, 1), (1, 2), (3, 1))
PART_OF = [p for p, (_, n) in enumerate(PARTS) for _ in range(n)]


def full(a, r):
    return [(XS, a, r), (XR, a, r), (YR, a, r), (OWN,)] + ([(YA, a, r), (YB, a, r)] if r < EARLY else [(YF, a, r)])


def staged(r):
    return GROUPS[r][2] == 8


def make_plan():
    it, un = {}, {}
    groups = range(NG)
    for r in groups:
        q = GROUPS[r][2] / 8 / NB
        f = 4 * q
        for a in (X, G):
            it[XS, a, r] = (0, q, [])
            it[XR, a, r] = (0, q / 2, [(XS, a, r)])
            row = [(XS, a, r), (XR, a, r)]
            if r < EARLY:
                it[YA, a, r] = (1, q, [])
                it[YB, a, r] = (1, 3 * q, row)
                it[YR, a, r] = (1, 2 * q, [(YA, a, r), (YB, a, r)])
            else:
                it[YF, a, r] = (1, 4 * q, row + [(OWN,)])
                it[YR, a, r] = (1, 2 * q, [(YF, a, r)])
        it[GP, r] = (2, 8 * q, full(G, r))
        it[XP, r] = (2, 4 * q, full(X, r))
        it[HP, r] = (2, 4 * q, [(M2, r)])
        it[ST, r] = (3, f, [(M2, r)])
        it[CS, r] = (0, f, [(ST, r) if staged(r) else (M2, r)])
        it[CR, r] = (0, 2 * q, [(CS, r)])
        dc = [(ST, r), (CS, r), (CR, r)]
        it[CP, r] = (2, 6 * q, [(ST, r), (CS, r)])
        it[CF, r] = (2, 2 * q, [(CR, r)])
        it[Q2, r] = (1, q, [(M3, r)])
        it[QD, r] = (1, q, [(M3, r)])
        it[QS, r] = (1, q, [(QA, r)])
        it[L1, r] = (3, 16 * q, full(X, r))
        it[L2, r] = (3, 16 * q, full(G, r))
        it[L3, r] = (3, 16 * q, dc)
        wu = [(WP, 0, p) for p in range(3)]
        wd = [(WP, 1, p) for p in range(3)]
        un[M1, r] = (0.4 + 4.4 * f, [(L1, r)] + wu)
        un[M2, r] = (0.4 + 6.2 * f, [(L2, r), (M1, r)] + wd)
        un[M3, r] = (0.4 + 4.4 * f, [(L3, r), (WN,)] + ([(QF, r - 2)] if r >= 2 else []))
        un[QA, r] = (0.1 + 0.4 * f, [(Q2, r)])
        un[QF, r] = (0.1 + 0.4 * f, [(QS, r), (QD, r)])
    for w in range(2):
        it[W2, w] = (0, 0.5, [])
        it[W1, w] = (0, 1.0, [])
        it[WR, w] = (0, 0.5, [(W2, w)])
        it[WP, w, 0] = (2, 1, [])
        it[WP, w, 1] = (2, 2, [(W1, w)])
        it[WP, w, 2] = (2, 1, [(WR, w)])
    it[(WN,)] = (2, 4, [])
    it[(OWN,)] = (3, 2, [])
    it[(O2,)] = (0, 0.5, [(M5, 0)])
    it[(O1,)] = (0, 1.0, [(M5, 1)])
    it[(OR,)] = (0, 0.5, [(O2,)])
    for p in range(RING):
        it[L5, p] = (3, 4, [(GP, r) for r in groups] + sum([full(G, r) for r in groups], []))
        it[L4, p] = (3, 4, [(CF if O4[p] == 2 else CP, r) for r in groups] + [((ST, CS, CS, CR)[p], r) for r in groups])
    it[(LH,)] = (3, 4, [(HP, r) for r in groups] + [(M2, r) for r in groups])
    it[(LX,)] = (3, 8, [(XP, r) for r in groups] + [(M5, 0)])
    for p, (first, n) in enumerate(PARTS):
        un[M4, p] = (4.8 * n, [(L4, first + i) for i in range(n)] + [(LX,)])
        un[M5, p] = (4.8 * n, [(L5, first + i) for i in range(n)] + [(LH,)])
    return it, un


ORDER = (
    "abicgdhjmFnIEHGJuosAyptBekvzflqwrxCKDLM",
    "dajmbenscfkolutvzBACGIHJghipqrwxyDELKFM",
    "gkbyAdcesvDuphBmoiwCrltjaxzqfEn",
)


def make_lists(plan):
    it, un = plan
    base = [[n for n in it if it[n][0] == k] for k in range(len(ORDER) - 1)] + [list(un)]
    *lists, units = ([names[string.ascii_letters.index(ch)] for ch in key] for names, key in zip(base, ORDER))
    return lists, units


LINKS = range(4)
RATE = (22.5,) * 2 + (1.7, 0.4)
DELAY = (3.0,) * 2 + (1.5,) * 2


def make_order(plan, lists, units):
    it, un = plan
    done, free, pos = {}, [0.0 for _ in LINKS], [0 for _ in LINKS]
    pend, now, order, panels, waits = list(units), 0.0, [], [], []
    late = [n for n in it if it[n][0] >= 2]
    rank = {u: i for i, u in enumerate(units)}
    user = lambda n: (PANEL_OF[n[0]], PART_OF[n[1]] if n[0] in (L4, L5) else n[1])
    panel_rank = lambda n: rank[user(n)] if n[0] in PANEL_OF else rank[{LX: M4, LH: M5}[n[0]], 0] if n[0] in (LX, LH) else -1
    gone = set()
    big = 1e9

    def ready(n):
        return all(done.get(d, big) <= now for d in it[n][2])

    def send(n):
        k = it[n][0]
        start = max(now + 0.3, free[k])
        waits.append((k, start - free[k], n))
        free[k] = start + it[n][1] * RATE[k]
        done[n] = free[k] + DELAY[k]
        order.append((n, now))

    while True:
        for k in (0, 1):
            while pos[k] < len(lists[k]) and ready(lists[k][pos[k]]):
                send(lists[k][pos[k]])
                pos[k] += 1
        for n in sorted((n for n in late if ready(n)), key=lambda n: (panel_rank(n), n)):
            if n[0] in PANEL_OF:
                if len(panels) >= PAN and user(panels[-PAN]) not in gone:
                    continue
                panels.append(n)
            late.remove(n)
            send(n)
        can = [u for u in pend if all(done.get(d, big) <= now for d in un[u][1])]
        if can:
            pend.remove(can[0])
            order.append((can[0], now))
            now += un[can[0]][0]
            done[can[0]] = now
            gone.add(can[0])
            continue
        later = [v for v in done.values() if v > now]
        if not later:
            break
        now = min(later)
    assert not pend and not late and all(pos[k] == len(lists[k]) for k in (0, 1)), (pend, late, pos)
    return [(n, [m for m in it if t - 30 < done[m] <= t - 2 and it[m][0] < 3]) for n, t in order], panels, max(done.values()), waits


class Copies:
    BACK = {"R": "L", "L": "R", "U": "N", "N": "U", "P": "P"}

    def __init__(self, send, recv, local, peers):
        self.send, self.recv, self.local, self.peers = send, recv, local, peers
        self.by_name, self.clock = {}, 0
        self.used = {"send": 0, "recv": 0, "local": 0}
        self.free = {"send": [], "local": []} | {to: [] for to in peers}
        self.waited = {to: [] for to in peers}

    def take(self, kind, pool):
        if self.free[pool]:
            return self.free[pool].pop()
        self.used[kind] += 1
        return self.used[kind] - 1

    def add(self, name, pairs):
        made = []
        for src, dst, to in pairs:
            self.clock += 1
            if to is None:
                i = self.take("local", "local")
                made.append([pltpu.make_async_copy(src, dst, self.local.at[i]), to, self.clock, i, None])
            else:
                axis, idx = self.peers[to]
                i, j = self.take("send", "send"), self.take("recv", to)
                c = pltpu.make_async_remote_copy(src, dst, self.send.at[i], self.recv.at[j], device_id={axis: idx}, device_id_type=MESH)
                made.append([c, to, self.clock, i, j])
            made[-1][0].start()
        self.by_name.setdefault(name, []).extend(made)

    def arrived(self, name):
        for m in self.by_name.get(name, ()):
            c, to, started, i, j = m
            self.clock += 1
            if to is None and i is not None:
                c.wait()
                self.free["local"].append(i)
                m[3] = None
            elif j is not None:
                c.wait_recv()
                self.waited[to].append((self.clock, j))
                m[4] = None
                back = self.BACK[to]
                self.free[back] += [k for t, k in self.waited[back] if t < started]
                self.waited[back] = [(t, k) for t, k in self.waited[back] if t >= started]

    def left(self, name):
        for m in self.by_name.get(name, ()):
            if m[1] is None:
                self.arrived(name)
            elif m[3] is not None:
                m[0].wait_send()
                self.free["send"].append(m[3])
                m[3] = None

    def finish(self):
        for name in list(self.by_name):
            self.arrived(name)
            self.left(name)


PIECES = 2
N_SEND, N_RECV, N_LOCAL = 24, 48, 16


def work(plan, order, panels, xa, wu, wd, za, dx, dwu, dwd, XF, GF, DF, GPB, DPB, XPB, HPB, su, sd, sw,
           wus, wds, wun, hbuf, pan, ft, rst, rrc, obuf, acc, send, recv, local):
    it, un = plan
    x, y, c = lax.axis_index("cy"), lax.axis_index("cz"), lax.axis_index("cx")
    peers = {
        "R": ("cy", lax.rem(x + 1, RING)), "L": ("cy", lax.rem(x + RING - 1, RING)),
        "U": ("cz", lax.rem(y + 1, RING)), "N": ("cz", lax.rem(y + RING - 1, RING)),
        "P": ("cx", 1 - c),
    }
    barrier = pltpu.get_barrier_semaphore()
    for axis, idx in peers.values():
        pl.semaphore_signal(barrier, inc=1, device_id={axis: idx}, device_id_type=MESH)
    pl.semaphore_wait(barrier, len(peers))

    cp = Copies(send, recv, local, peers)
    blk_rows = xa.shape[1]
    sub = wd.shape[2]
    dh = wu.shape[1]
    mine = pl.ds(pl.multiple_of(c * sub, sub), sub)
    theirs = pl.ds(pl.multiple_of((1 - c) * sub, sub), sub)
    lo, hi = pl.ds(0, sub), pl.ds(sub, sub)
    at = lambda j: lax.rem(x + j, RING)
    cols = lambda j: pl.ds(pl.multiple_of(at(j) * sub, sub), sub)
    slot_of = {n: i % PAN for i, n in enumerate(panels)}
    inp, buf = (xa, za), (XF, GF)

    def group(r):
        b, first, n = GROUPS[r]
        unit_rows = blk_rows // 8
        return b, first * unit_rows, n * unit_rows

    def rel(r, k, part=None):
        _, first, n = group(r)
        start = RING * first + k * n
        return pl.ds(start, n) if part is None else pl.ds(start + part * (n // 2), n // 2)

    def span(r):
        _, first, n = group(r)
        return pl.ds(RING * first, RING * n)

    def copies_of(name):
        kind, a, r = name[0], name[-2:][0], name[-1]
        both = lambda right, left: [right + ("R",), left + ("L",)]
        updn = lambda up, down: [up + ("U",), down + ("N",)]
        if kind == WN:
            return sum([[(wu.at[:, :, cols(j)], wun.at[2 * j:2 * j + 2, :, mine], to) for to in (None, "P")] for j in range(RING)], [])
        if kind == XS or kind == YA:
            b, first, n = group(r)
            src = inp[a].at[b, pl.ds(first, n)]
            if kind == XS:
                return both((src, buf[a].at[3, b, rel(r, 0)]), (src, buf[a].at[1, b, rel(r, 0)]))
            return updn((src, buf[a].at[0, b, rel(r, 3)]), (src, buf[a].at[0, b, rel(r, 1)]))
        if kind == XR:
            b, f, s = group(r)[0], rel(r, 0, 0), rel(r, 0, 1)
            return both((buf[a].at[3, b, f], buf[a].at[2, b, f]), (buf[a].at[1, b, s], buf[a].at[2, b, s]))
        if kind in (YB, YF):
            b, m = group(r)[0], buf[a]
            js = pl.ds(1, RING - 1) if kind == YB else pl.ds(0, RING)
            return updn((m.at[js, b, rel(r, 0)], m.at[js, b, rel(r, 3)]), (m.at[js, b, rel(r, 0)], m.at[js, b, rel(r, 1)]))
        if kind == YR:
            b, m = group(r)[0], buf[a]
            return updn((m.at[0:2, b, rel(r, 3)], m.at[0:2, b, rel(r, 2)]), (m.at[2:4, b, rel(r, 1)], m.at[2:4, b, rel(r, 2)]))
        if kind in (W2, W1, WR):
            half = (lambda h, j: wu.at[h, :, cols(j)]) if r == 0 else (lambda h, j: wd.at[h, at(j)])
            piece = (lambda j: wu.at[:, :, cols(j)]) if r == 0 else (lambda j: wd.at[:, at(j)])
            st, dst = (su, sd)[r], (wus, wds)[r]
            if kind == W2:
                return both((half(0, 2), st.at[0]), (half(1, 2), st.at[1]))
            if kind == W1:
                return both((piece(1), dst.at[6:8, :, mine]), (piece(3), dst.at[2:4, :, mine]))
            return both((st.at[0], dst.at[4, :, mine]), (st.at[1], dst.at[5, :, mine]))
        if kind == WP:
            m = (wus, wds)[a]
            if r == 0:
                src = wu.at[:, :, cols(0)] if a == 0 else wd.at[:, at(0)]
                return [(src, m.at[0:2, :, mine], to) for to in (None, "P")]
            return [(m.at[2 * j:2 * j + 2, :, mine], m.at[2 * j:2 * j + 2, :, mine], "P") for j in ((1, 3) if r == 1 else (2,))]
        if kind == GP:
            return [(GF.at[:, group(r)[0], span(r), theirs], GPB.at[:, group(r)[0], span(r)], "P")]
        if kind == XP:
            return [(XF.at[0, group(r)[0], span(r)], XPB.at[group(r)[0], span(r)], "P")]
        if kind == HP:
            return [(hbuf.at[group(r)[0], span(r)], HPB.at[group(r)[0], span(r)], "P")]
        if kind in (CP, CF):
            b = group(r)[0]
            js = (pl.ds(0, 2), pl.ds(3, 1)) if kind == CP else (pl.ds(2, 1),)
            return [(DF.at[j, b, 1 - c, span(r)], DPB.at[j, b, span(r)], "P") for j in js]
        if kind == ST:
            b = group(r)[0]
            return [(obuf.at[2, :, span(r)], DF.at[0, b, :, span(r)], None)]
        if kind == CS:
            b = group(r)[0]
            m = DF.at[0, b, :, span(r)] if staged(r) else obuf.at[2, :, span(r)]
            return both((m, DF.at[3, b, :, span(r)]), (m, DF.at[1, b, :, span(r)]))
        if kind == CR:
            b, first, n = group(r)
            f, s = (pl.ds(RING * first + h * 2 * n, 2 * n) for h in range(2))
            return both((DF.at[3, b, :, f], DF.at[2, b, :, f]), (DF.at[1, b, :, s], DF.at[2, b, :, s]))
        if kind in (Q2, QD, QS):
            b, first, n = group(r)
            f = ft.at[r % 2]
            own = lambda k: pl.ds(k * n, n)
            rs = pl.ds(first, n)
            if kind == Q2:
                return updn((f.at[0, own(2)], rst.at[b, 0, rs]), (f.at[1, own(2)], rst.at[b, 1, rs]))
            if kind == QD:
                return updn((f.at[1, own(1)], rrc.at[b, 0, 1, rs]), (f.at[0, own(3)], rrc.at[b, 1, 0, rs]))
            return updn((f.at[0, own(1)], rrc.at[b, 0, 0, rs]), (f.at[1, own(3)], rrc.at[b, 1, 1, rs]))
        if kind in (L1, L2, L3):
            b, _, n = group(r)
            to = pan.at[slot_of[name], :, pl.ds(0, RING * n)]
            if kind == L3:
                return [(DF.at[:, b, h, span(r)], to.at[:, :, h * sub:(h + 1) * sub], None) for h in range(CORES)]
            return [((XF if kind == L1 else GF).at[:, b, span(r)], to, None)]
        if kind in (L5, L4):
            m, p = (GF.at[O5[r], :, :, mine], GPB.at[O5[r]]) if kind == L5 else (DF.at[O4[r], :, c], DPB.at[O4[r]])
            s = pan.at[slot_of[name]]
            return [(m, s.at[:, :, lo], None), (p, s.at[:, :, hi], None)]
        if kind == LH:
            return [(HPB, wds.at[0:4], None)]
        if kind == LX:
            return [(XF.at[0], wus.at[0:4], None), (XPB, wus.at[4:8], None)]
        place = {j: i for i, j in enumerate(O5)}
        if kind == O2:
            return both((obuf.at[place[2], 0], sw.at[0]), (obuf.at[place[2], 1], sw.at[1]))
        if kind == O1:
            return both((obuf.at[place[1]], dwd.at[:, x]), (obuf.at[place[3]], dwd.at[:, x]))
        assert kind == OR
        return both((sw.at[0], dwd.at[0, at(3)]), (sw.at[1], dwd.at[1, at(1)]))

    def total(terms):
        out = None
        for a, b, dims in terms:
            d = lax.dot_general(a, b, dims, preferred_element_type=jnp.float32)
            out = d if out is None else out + d
        return out

    def loop(n, body):
        def step(i, carry):
            body(i)
            return carry
        lax.fori_loop(0, n, step, 0)

    def unit(name):
        kind, r = name[0], name[-1]
        if kind in (M1, M2, M3):
            b, first, n = group(r)
            rows = pl.ds(0, RING * n)
        if kind == M1:
            p = pan.at[slot_of[L1, r]]

            def body(t):
                ns = pl.ds(pl.multiple_of(t * sub, sub), sub)
                s = total([(p[j, rows, h * dh:(h + 1) * dh], wus[2 * j + h, :, ns], NN) for j in range(RING) for h in range(2)])
                hbuf[b, span(r), ns] = s.astype(jnp.bfloat16)
            loop(2, body)
        elif kind == M2:
            p = pan.at[slot_of[L2, r]]
            if r > 0 and staged(r - 1):
                cp.arrived((ST, r - 1))
            step = min(32, RING * n)

            def body(t):
                ns = pl.ds(pl.multiple_of(t * sub, sub), sub)
                acc[rows, :] = total([(p[j, rows, :], wds[2 * j + t], NT) for j in range(RING)])

                def elem(e):
                    rs = pl.ds(pl.multiple_of(e * step, step), step)
                    hs = pl.ds(pl.multiple_of(RING * first + e * step, step), step)
                    g, s = gelu_parts(hbuf[b, hs, ns].astype(jnp.float32))
                    hbuf[b, hs, ns] = g.astype(jnp.bfloat16)
                    obuf[2, t, hs, :] = (acc[rs, :] * s).astype(jnp.bfloat16)
                loop(RING * n // step, elem)
            loop(2, body)
        elif kind == M3:
            p = pan.at[slot_of[L3, r]]
            if r >= 2:
                for q in (Q2, QD, QS):
                    cp.left((q, r - 2))
            f = ft.at[r % 2]

            def body(t):
                f[t, rows, :] = total([(p[j, rows, :], wun[2 * j + t], NT) for j in range(RING)])
            loop(2, body)
        elif kind in (M5, M4):
            i0, m = PARTS[r]
            s0, s1 = (slot_of[L5 if kind == M5 else L4, i] for i in (i0, i0 + m - 1))
            j0, j1 = ((O5 if kind == M5 else O4)[i] for i in (i0, i0 + m - 1))
            own, par, p0 = (hbuf, wds, 0) if kind == M5 else (wus, wus, NB)
            if kind == M5 and i0 + m - 1 == 2:
                for g in range(NG):
                    cp.arrived((ST, g))
                    cp.left((CS, g))

            def body(i):
                e, t = (0, i) if m == 1 else (i // 2, lax.rem(i, 2))
                p = pan.at[s0 + e * (s1 - s0)]
                ms = pl.ds(pl.multiple_of(t * dh, dh), dh)
                s = total([(own[g, :, ms], p[g, :, lo], TN) for g in range(NB)] + [(par[p0 + g, :, ms], p[g, :, hi], TN) for g in range(NB)])
                if kind == M5 and O5[i0] == 0:
                    dwd[t, x] = s.astype(jnp.bfloat16)
                elif kind == M5:
                    obuf[i0 + e, t] = s.astype(jnp.bfloat16)
                else:
                    dwu[t, :, cols(j0 + e * (j1 - j0))] = s.astype(jnp.bfloat16)
            loop(2 * m, body)
        else:
            b, first, n = group(r)
            f = ft.at[r % 2]
            rs = pl.ds(first, n)
            own = lambda k: pl.ds(k * n, n)
            if kind == QA:
                f[0, own(1), :] = f[0, own(1), :] + rst[b, 0, rs, :]
                f[1, own(3), :] = f[1, own(3), :] + rst[b, 1, rs, :]
            else:
                for h in range(2):
                    dx[b, rs, h * dh:(h + 1) * dh] = (f[h, own(0), :] + rrc[b, 0, h, rs, :] + rrc[b, 1, h, rs, :]).astype(jnp.bfloat16)

    for name, gone in order:
        for d in gone:
            cp.arrived(d)
            cp.left(d)
        for d in (it[name][2] if name in it else un[name][1]):
            cp.arrived(d)
        if name[0] == OWN:
            own = pl.ds(0, blk_rows)
            b0, b1 = pan.at[0, :, own], pan.at[1, :, own]
            cp.add((OUT, OWN), [(xa, b0, None), (za, b1, None)])
            cp.arrived((OUT, OWN))
            pairs = []
            for r in range(NG):
                b, first, n = group(r)
                pairs += [(pan.at[a, b, pl.ds(first, n)], buf[a].at[0, b, rel(r, 0)], None) for a in (X, G)]
            cp.add(name, pairs)
        elif name in it:
            for w in {LX: (0,), LH: (1,)}.get(name[0], ()):
                for p in range(3):
                    cp.left((WP, w, p))
            cp.add(name, copies_of(name))
        else:
            unit(name)
    cp.finish()
    assert tuple(cp.used.values()) == (N_SEND, N_RECV, N_LOCAL), cp.used


def kernel(plan, order, panels, *refs):
    pl.run_scoped(functools.partial(work, plan, order, panels, *refs), *(pltpu.SemaphoreType.DMA((n,)) for n in (N_SEND, N_RECV, N_LOCAL)))


def write_out(dx, dwu, dwd, dx_out, dwu_out, dwd_out, sem):
    arrays = ((dx, dx_out), (dwu, dwu_out), (dwd, dwd_out))
    for i, (a, b) in enumerate(arrays):
        n = a.shape[1] // PIECES
        for j in range(a.shape[0]):
            for p in range(PIECES):
                rows = pl.ds(p * n, n)
                pltpu.make_async_copy(a.at[j, rows], b.at[j, rows], sem.at[i]).start()
    for i, (a, b) in enumerate(arrays):
        pltpu.make_async_copy(a, b, sem.at[i]).wait()


def solution(mesh):
    assert mesh.shape["cy"] == RING and mesh.shape["cz"] == RING and mesh.shape["cx"] == CORES
    row_spec = P(("dp", "cx", "cz"), "cy")
    up_spec = P("cy", ("cz", "cx"))
    down_spec = P("cz", ("cy", "cx"))
    up_out = P(("dp", "cy"), ("cz", "cx"))
    down_out = P(("dp", "cz"), ("cy", "cx"))
    plan = make_plan()
    order, panels, _, _ = make_order(plan, *make_lists(plan))

    def local_step(x_act, w_up, w_down, z_grad):
        t_loc, d_loc = x_act.shape
        f_loc = w_up.shape[1]
        rows, sub, dh = t_loc // NB, f_loc // RING, d_loc // 2
        grp = RING * rows
        bf, f32 = jnp.bfloat16, jnp.float32
        xa, za = x_act.reshape(NB, rows, d_loc), z_grad.reshape(NB, rows, d_loc)
        wu = w_up.reshape(2, dh, f_loc)
        wd = w_down.reshape(CORES, RING, sub, dh)
        hbm = lambda *s: jax.ShapeDtypeStruct(s, bf)
        outs = (
            pltpu.VMEM((NB, rows, d_loc), bf), pltpu.VMEM((2, dh, f_loc), bf), pltpu.VMEM((CORES, RING, sub, dh), bf),
            hbm(RING, NB, grp, d_loc), hbm(RING, NB, grp, d_loc), hbm(RING, NB, CORES, grp, sub),
            hbm(RING, NB, grp, sub), hbm(RING, NB, grp, sub), hbm(NB, grp, d_loc), hbm(NB, grp, 2 * sub),
            hbm(2, dh, sub), hbm(2, sub, dh), hbm(2, sub, dh),
        )
        scratch = [
            pltpu.VMEM((2 * RING, dh, 2 * sub), bf), pltpu.VMEM((2 * RING, sub, d_loc), bf), pltpu.VMEM((2 * RING, dh, 2 * sub), bf),
            pltpu.VMEM((NB, grp, 2 * sub), bf), pltpu.VMEM((PAN, RING, grp, d_loc), bf),
            pltpu.VMEM((2, 2, grp, dh), f32),
            pltpu.VMEM((NB, 2, rows, dh), f32), pltpu.VMEM((NB, 2, 2, rows, dh), f32),
            pltpu.VMEM((3, CORES, sub, dh), bf),
            pltpu.VMEM((grp, sub), f32),
        ]
        any_spec = pl.BlockSpec(memory_space=pl.ANY)
        res = pl.pallas_call(
            functools.partial(kernel, plan, order, panels),
            out_shape=outs,
            in_specs=[any_spec] * 4,
            out_specs=[pl.BlockSpec(memory_space=pltpu.VMEM)] * 3 + [any_spec] * (len(outs) - 3),
            scratch_shapes=scratch,
            compiler_params=pltpu.CompilerParams(collective_id=0, has_side_effects=True, vmem_limit_bytes=57600000),
            name="mlp_bwd",
        )(xa, wu, wd, za)
        outs = [pltpu.with_memory_space_constraint(o, pltpu.VMEM) for o in res[:3]]
        outs = pl.pallas_call(
            write_out,
            out_shape=[jax.ShapeDtypeStruct(o.shape, bf) for o in outs],
            in_specs=[pl.BlockSpec(memory_space=pltpu.VMEM) for _ in outs],
            out_specs=[any_spec for _ in outs],
            scratch_shapes=[pltpu.SemaphoreType.DMA((len(outs),))],
            compiler_params=pltpu.CompilerParams(vmem_limit_bytes=1 << 20),
            name="write_out",
        )(*outs)
        return tuple(o.reshape(a.shape) for o, a in zip(outs, (x_act, w_up, w_down)))

    return jax.shard_map(local_step, mesh=mesh, in_specs=(row_spec, up_spec, down_spec, row_spec), out_specs=(row_spec, up_out, down_out), check_vma=False)
```

```python
import functools
import math
import string

import jax
import jax.numpy as jnp
from jax import lax
from jax.experimental import pallas as pl
from jax.experimental.pallas import tpu as pltpu
from jax.sharding import PartitionSpec as P

GELU_COEF = 0.044715
SQRT_TWO_PI = math.sqrt(2.0 / math.pi)
NN = (((1,), (0,)), ((), ()))
NT = (((1,), (1,)), ((), ()))
TN = (((0,), (0,)), ((), ()))
MESH = pl.DeviceIdType.MESH
RING = 4
CORES = 2
PAN = 3
GROUPS = ((0, 0, 8), (1, 0, 8), (2, 0, 8), (3, 0, 4), (3, 4, 4))
NB = 4
NG = len(GROUPS)
LAST = NG - 1
EARLY = 2
X, G = 0, 1


def gelu_parts(pre_act):
    inner_arg = SQRT_TWO_PI * (pre_act + GELU_COEF * pre_act * pre_act * pre_act)
    tanh_val = jnp.tanh(inner_arg)
    gelu_val = 0.5 * pre_act * (1.0 + tanh_val)
    gelu_slope = 0.5 * (1.0 + tanh_val) + 0.5 * pre_act * (1.0 - tanh_val * tanh_val) * SQRT_TWO_PI * (1.0 + 3.0 * GELU_COEF * pre_act * pre_act)
    return gelu_val, gelu_slope


(XS, XR, W2, W1, WR, CS, CR, O2, O1, OR, YA, YB, YF, YR, Q2, QD, QS, WN, WP, GP, XP, HP, CP, CF,
 ST, OWN, L1, L2, L3, L4, L5, LX, LH, M1, M2, M3, M4, M5, QA, QF, OUT) = range(41)
PANEL_OF = {L1: M1, L2: M2, L3: M3, L4: M4, L5: M5}
O5 = (2, 1, 3, 0)
O4 = (0, 1, 3, 2)
PARTS = ((0, 1), (1, 2), (3, 1))
PART_OF = [p for p, (_, n) in enumerate(PARTS) for _ in range(n)]


def full(a, r):
    return [(XS, a, r), (XR, a, r), (YR, a, r), (OWN,)] + ([(YA, a, r), (YB, a, r)] if r < EARLY else [(YF, a, r)])


def staged(r):
    return GROUPS[r][2] == 8


def make_plan():
    it, un = {}, {}
    groups = range(NG)
    for r in groups:
        q = GROUPS[r][2] / 8 / NB
        f = 4 * q
        for a in (X, G):
            it[XS, a, r] = (0, q, [])
            it[XR, a, r] = (0, q / 2, [(XS, a, r)])
            row = [(XS, a, r), (XR, a, r)]
            if r < EARLY:
                it[YA, a, r] = (1, q, [])
                it[YB, a, r] = (1, 3 * q, row)
                it[YR, a, r] = (1, 2 * q, [(YA, a, r), (YB, a, r)])
            else:
                it[YF, a, r] = (1, 4 * q, row + [(OWN,)])
                it[YR, a, r] = (1, 2 * q, [(YF, a, r)])
        it[GP, r] = (2, 8 * q, full(G, r))
        it[XP, r] = (2, 4 * q, full(X, r))
        it[HP, r] = (2, 4 * q, [(M2, r)])
        it[ST, r] = (3, f, [(M2, r)])
        it[CS, r] = (0, f, [(ST, r) if staged(r) else (M2, r)])
        it[CR, r] = (0, 2 * q, [(CS, r)])
        dc = [(ST, r), (CS, r), (CR, r)]
        it[CP, r] = (2, 6 * q, [(ST, r), (CS, r)])
        it[CF, r] = (2, 2 * q, [(CR, r)])
        it[Q2, r] = (1, q, [(M3, r)])
        it[QD, r] = (1, q, [(M3, r)])
        it[QS, r] = (1, q, [(QA, r)])
        it[L1, r] = (3, 16 * q, full(X, r))
        it[L2, r] = (3, 16 * q, full(G, r))
        it[L3, r] = (3, 16 * q, dc)
        wu = [(WP, 0, p) for p in range(3)]
        wd = [(WP, 1, p) for p in range(3)]
        un[M1, r] = (0.4 + 4.4 * f, [(L1, r)] + wu)
        un[M2, r] = (0.4 + 6.2 * f, [(L2, r), (M1, r)] + wd)
        un[M3, r] = (0.4 + 4.4 * f, [(L3, r), (WN,)] + ([(QF, r - 2)] if r >= 2 else []))
        un[QA, r] = (0.1 + 0.4 * f, [(Q2, r)])
        un[QF, r] = (0.1 + 0.4 * f, [(QS, r), (QD, r)])
    for w in range(2):
        it[W2, w] = (0, 0.5, [])
        it[W1, w] = (0, 1.0, [])
        it[WR, w] = (0, 0.5, [(W2, w)])
        it[WP, w, 0] = (2, 1, [])
        it[WP, w, 1] = (2, 2, [(W1, w)])
        it[WP, w, 2] = (2, 1, [(WR, w)])
    it[(WN,)] = (2, 4, [])
    it[(OWN,)] = (3, 2, [])
    it[(O2,)] = (0, 0.5, [(M5, 0)])
    it[(O1,)] = (0, 1.0, [(M5, 1)])
    it[(OR,)] = (0, 0.5, [(O2,)])
    for p in range(RING):
        it[L5, p] = (3, 4, [(GP, r) for r in groups] + sum([full(G, r) for r in groups], []))
        it[L4, p] = (3, 4, [(CF if O4[p] == 2 else CP, r) for r in groups] + [((ST, CS, CS, CR)[p], r) for r in groups])
    it[(LH,)] = (3, 4, [(HP, r) for r in groups] + [(M2, r) for r in groups])
    it[(LX,)] = (3, 8, [(XP, r) for r in groups] + [(M5, 0)])
    for p, (first, n) in enumerate(PARTS):
        un[M4, p] = (4.8 * n, [(L4, first + i) for i in range(n)] + [(LX,)])
        un[M5, p] = (4.8 * n, [(L5, first + i) for i in range(n)] + [(LH,)])
    return it, un


ORDER = (
    "acbdimgInhjEHGFyJosuApzteBvkflqwrxCKDML",
    "admjbecsknfolutvzBACGIHJghipqrwxyDKELFM",
    "yompqhsjlwunkfAgBtxCiveabzcrEDd",
)


def make_lists(plan):
    it, un = plan
    base = [[n for n in it if it[n][0] == k] for k in range(len(ORDER) - 1)] + [list(un)]
    *lists, units = ([names[string.ascii_letters.index(ch)] for ch in key] for names, key in zip(base, ORDER))
    return lists, units


LINKS = range(4)
RATE = (22.5,) * 2 + (1.7, 0.4)
DELAY = (3.0,) * 2 + (1.5,) * 2


def make_order(plan, lists, units):
    it, un = plan
    done, free, pos = {}, [0.0 for _ in LINKS], [0 for _ in LINKS]
    pend, now, order, panels, waits = list(units), 0.0, [], [], []
    late = [n for n in it if it[n][0] >= 2]
    rank = {u: i for i, u in enumerate(units)}
    user = lambda n: (PANEL_OF[n[0]], PART_OF[n[1]] if n[0] in (L4, L5) else n[1])
    panel_rank = lambda n: rank[user(n)] if n[0] in PANEL_OF else rank[{LX: M4, LH: M5}[n[0]], 0] if n[0] in (LX, LH) else -1
    gone = set()
    big = 1e9

    def ready(n):
        return all(done.get(d, big) <= now for d in it[n][2])

    def send(n):
        k = it[n][0]
        start = max(now + 0.3, free[k])
        waits.append((k, start - free[k], n))
        free[k] = start + it[n][1] * RATE[k]
        done[n] = free[k] + DELAY[k]
        order.append((n, now))

    while True:
        for k in (0, 1):
            while pos[k] < len(lists[k]) and ready(lists[k][pos[k]]):
                send(lists[k][pos[k]])
                pos[k] += 1
        for n in sorted((n for n in late if ready(n)), key=lambda n: (panel_rank(n), n)):
            if n[0] in PANEL_OF:
                if len(panels) >= PAN and user(panels[-PAN]) not in gone:
                    continue
                panels.append(n)
            late.remove(n)
            send(n)
        can = [u for u in pend if all(done.get(d, big) <= now for d in un[u][1])]
        if can:
            pend.remove(can[0])
            order.append((can[0], now))
            now += un[can[0]][0]
            done[can[0]] = now
            gone.add(can[0])
            continue
        later = [v for v in done.values() if v > now]
        if not later:
            break
        now = min(later)
    assert not pend and not late and all(pos[k] == len(lists[k]) for k in (0, 1)), (pend, late, pos)
    return [(n, [m for m in it if t - 30 < done[m] <= t - 2 and it[m][0] < 3]) for n, t in order], panels, max(done.values()), waits


class Copies:
    BACK = {"R": "L", "L": "R", "U": "N", "N": "U", "P": "P"}

    def __init__(self, send, recv, local, peers):
        self.send, self.recv, self.local, self.peers = send, recv, local, peers
        self.by_name, self.clock = {}, 0
        self.used = {"send": 0, "recv": 0, "local": 0}
        self.free = {"send": [], "local": []} | {to: [] for to in peers}
        self.waited = {to: [] for to in peers}

    def take(self, kind, pool):
        if self.free[pool]:
            return self.free[pool].pop()
        self.used[kind] += 1
        return self.used[kind] - 1

    def add(self, name, pairs):
        made = []
        for src, dst, to in pairs:
            self.clock += 1
            if to is None:
                i = self.take("local", "local")
                made.append([pltpu.make_async_copy(src, dst, self.local.at[i]), to, self.clock, i, None])
            else:
                axis, idx = self.peers[to]
                i, j = self.take("send", "send"), self.take("recv", to)
                c = pltpu.make_async_remote_copy(src, dst, self.send.at[i], self.recv.at[j], device_id={axis: idx}, device_id_type=MESH)
                made.append([c, to, self.clock, i, j])
            made[-1][0].start()
        self.by_name.setdefault(name, []).extend(made)

    def arrived(self, name):
        for m in self.by_name.get(name, ()):
            c, to, started, i, j = m
            self.clock += 1
            if to is None and i is not None:
                c.wait()
                self.free["local"].append(i)
                m[3] = None
            elif j is not None:
                c.wait_recv()
                self.waited[to].append((self.clock, j))
                m[4] = None
                back = self.BACK[to]
                self.free[back] += [k for t, k in self.waited[back] if t < started]
                self.waited[back] = [(t, k) for t, k in self.waited[back] if t >= started]

    def left(self, name):
        for m in self.by_name.get(name, ()):
            if m[1] is None:
                self.arrived(name)
            elif m[3] is not None:
                m[0].wait_send()
                self.free["send"].append(m[3])
                m[3] = None

    def finish(self):
        for name in list(self.by_name):
            self.arrived(name)
            self.left(name)


PIECES = 4
N_SEND, N_RECV, N_LOCAL = 26, 54, 16


def work(plan, order, panels, xa, wu, wd, za, dx, dwu, dwd, XF, GF, DF, GPB, DPB, XPB, HPB, su, sd, sw,
           wus, wds, wun, hbuf, pan, ft, rst, rrc, obuf, acc, send, recv, local):
    it, un = plan
    x, y, c = lax.axis_index("cy"), lax.axis_index("cz"), lax.axis_index("cx")
    peers = {
        "R": ("cy", lax.rem(x + 1, RING)), "L": ("cy", lax.rem(x + RING - 1, RING)),
        "U": ("cz", lax.rem(y + 1, RING)), "N": ("cz", lax.rem(y + RING - 1, RING)),
        "P": ("cx", 1 - c),
    }
    barrier = pltpu.get_barrier_semaphore()
    for axis, idx in peers.values():
        pl.semaphore_signal(barrier, inc=1, device_id={axis: idx}, device_id_type=MESH)
    pl.semaphore_wait(barrier, len(peers))

    cp = Copies(send, recv, local, peers)
    blk_rows = xa.shape[1]
    sub = wd.shape[2]
    dh = wu.shape[1]
    mine = pl.ds(pl.multiple_of(c * sub, sub), sub)
    theirs = pl.ds(pl.multiple_of((1 - c) * sub, sub), sub)
    lo, hi = pl.ds(0, sub), pl.ds(sub, sub)
    at = lambda j: lax.rem(x + j, RING)
    cols = lambda j: pl.ds(pl.multiple_of(at(j) * sub, sub), sub)
    slot_of = {n: i % PAN for i, n in enumerate(panels)}
    inp, buf = (xa, za), (XF, GF)

    def group(r):
        b, first, n = GROUPS[r]
        unit_rows = blk_rows // 8
        return b, first * unit_rows, n * unit_rows

    def rel(r, k, part=None):
        _, first, n = group(r)
        start = RING * first + k * n
        return pl.ds(start, n) if part is None else pl.ds(start + part * (n // 2), n // 2)

    def span(r):
        _, first, n = group(r)
        return pl.ds(RING * first, RING * n)

    def of_part(copies, part, turned=False):
        return [c for i, c in enumerate(copies) if part is None or (i == part) != turned]

    def in_halves(r, kinds, body):
        for t in range(CORES):
            body(t)
            for kind in kinds:
                cp.add((kind, r), copies_of((kind, r), t))

    def copies_of(name, part=None):
        kind, a, r = name[0], name[-2:][0], name[-1]
        both = lambda right, left: [right + ("R",), left + ("L",)]
        updn = lambda up, down: [up + ("U",), down + ("N",)]
        if kind == WN:
            return sum([[(wu.at[:, :, cols(j)], wun.at[2 * j:2 * j + 2, :, mine], to) for to in (None, "P")] for j in range(RING)], [])
        if kind == XS or kind == YA:
            b, first, n = group(r)
            src = inp[a].at[b, pl.ds(first, n)]
            if kind == XS:
                return both((src, buf[a].at[3, b, rel(r, 0)]), (src, buf[a].at[1, b, rel(r, 0)]))
            return updn((src, buf[a].at[0, b, rel(r, 3)]), (src, buf[a].at[0, b, rel(r, 1)]))
        if kind == XR:
            b, f, s = group(r)[0], rel(r, 0, 0), rel(r, 0, 1)
            return both((buf[a].at[3, b, f], buf[a].at[2, b, f]), (buf[a].at[1, b, s], buf[a].at[2, b, s]))
        if kind in (YB, YF):
            b, m = group(r)[0], buf[a]
            js = pl.ds(1, RING - 1) if kind == YB else pl.ds(0, RING)
            return updn((m.at[js, b, rel(r, 0)], m.at[js, b, rel(r, 3)]), (m.at[js, b, rel(r, 0)], m.at[js, b, rel(r, 1)]))
        if kind == YR:
            b, m = group(r)[0], buf[a]
            return updn((m.at[0:2, b, rel(r, 3)], m.at[0:2, b, rel(r, 2)]), (m.at[2:4, b, rel(r, 1)], m.at[2:4, b, rel(r, 2)]))
        if kind in (W2, W1, WR):
            half = (lambda h, j: wu.at[h, :, cols(j)]) if r == 0 else (lambda h, j: wd.at[h, at(j)])
            piece = (lambda j: wu.at[:, :, cols(j)]) if r == 0 else (lambda j: wd.at[:, at(j)])
            st, dst = (su, sd)[r], (wus, wds)[r]
            if kind == W2:
                return both((half(0, 2), st.at[0]), (half(1, 2), st.at[1]))
            if kind == W1:
                return both((piece(1), dst.at[6:8, :, mine]), (piece(3), dst.at[2:4, :, mine]))
            return both((st.at[0], dst.at[4, :, mine]), (st.at[1], dst.at[5, :, mine]))
        if kind == WP:
            m = (wus, wds)[a]
            if r == 0:
                src = wu.at[:, :, cols(0)] if a == 0 else wd.at[:, at(0)]
                return [(src, m.at[0:2, :, mine], to) for to in (None, "P")]
            return [(m.at[2 * j:2 * j + 2, :, mine], m.at[2 * j:2 * j + 2, :, mine], "P") for j in ((1, 3) if r == 1 else (2,))]
        if kind == GP:
            return [(GF.at[:, group(r)[0], span(r), theirs], GPB.at[:, group(r)[0], span(r)], "P")]
        if kind == XP:
            return [(XF.at[0, group(r)[0], span(r)], XPB.at[group(r)[0], span(r)], "P")]
        if kind == HP:
            return [(hbuf.at[group(r)[0], span(r)], HPB.at[group(r)[0], span(r)], "P")]
        if kind in (CP, CF):
            b = group(r)[0]
            js = (pl.ds(0, 2), pl.ds(3, 1)) if kind == CP else (pl.ds(2, 1),)
            return [(DF.at[j, b, 1 - c, span(r)], DPB.at[j, b, span(r)], "P") for j in js]
        if kind == ST:
            b = group(r)[0]
            return [(obuf.at[2, :, span(r)], DF.at[0, b, :, span(r)], None)]
        if kind == CS:
            b = group(r)[0]
            h = pl.ds(0, CORES) if part is None else part
            m = DF.at[0, b, h, span(r)] if staged(r) else obuf.at[2, h, span(r)]
            return both((m, DF.at[3, b, h, span(r)]), (m, DF.at[1, b, h, span(r)]))
        if kind == CR:
            b, first, n = group(r)
            f, s = (pl.ds(RING * first + h * 2 * n, 2 * n) for h in range(2))
            return both((DF.at[3, b, :, f], DF.at[2, b, :, f]), (DF.at[1, b, :, s], DF.at[2, b, :, s]))
        if kind in (Q2, QD, QS):
            b, first, n = group(r)
            f = ft.at[r % 2]
            own = lambda k: pl.ds(k * n, n)
            rs = pl.ds(first, n)
            if kind == Q2:
                return of_part(updn((f.at[0, own(2)], rst.at[b, 0, rs]), (f.at[1, own(2)], rst.at[b, 1, rs])), part)
            if kind == QD:
                return of_part(updn((f.at[1, own(1)], rrc.at[b, 0, 1, rs]), (f.at[0, own(3)], rrc.at[b, 1, 0, rs])), part, True)
            return updn((f.at[0, own(1)], rrc.at[b, 0, 0, rs]), (f.at[1, own(3)], rrc.at[b, 1, 1, rs]))
        if kind in (L1, L2, L3):
            b, _, n = group(r)
            to = pan.at[slot_of[name], :, pl.ds(0, RING * n)]
            if kind == L3:
                return [(DF.at[:, b, h, span(r)], to.at[:, :, h * sub:(h + 1) * sub], None) for h in range(CORES)]
            return [((XF if kind == L1 else GF).at[:, b, span(r)], to, None)]
        if kind in (L5, L4):
            m, p = (GF.at[O5[r], :, :, mine], GPB.at[O5[r]]) if kind == L5 else (DF.at[O4[r], :, c], DPB.at[O4[r]])
            s = pan.at[slot_of[name]]
            return [(m, s.at[:, :, lo], None), (p, s.at[:, :, hi], None)]
        if kind == LH:
            return [(HPB, wds.at[0:4], None)]
        if kind == LX:
            return [(XF.at[0], wus.at[0:4], None), (XPB, wus.at[4:8], None)]
        place = {j: i for i, j in enumerate(O5)}
        if kind == O2:
            return both((obuf.at[place[2], 0], sw.at[0]), (obuf.at[place[2], 1], sw.at[1]))
        if kind == O1:
            return both((obuf.at[place[1]], dwd.at[:, x]), (obuf.at[place[3]], dwd.at[:, x]))
        assert kind == OR
        return both((sw.at[0], dwd.at[0, at(3)]), (sw.at[1], dwd.at[1, at(1)]))

    def total(terms):
        out = None
        for a, b, dims in terms:
            d = lax.dot_general(a, b, dims, preferred_element_type=jnp.float32)
            out = d if out is None else out + d
        return out

    def at_tile(t):
        return pl.ds(t * sub if isinstance(t, int) else pl.multiple_of(t * sub, sub), sub)

    def loop(body, n=CORES):
        def step(i, carry):
            body(i)
            return carry
        lax.fori_loop(0, n, step, 0)

    def unit(name):
        kind, r = name[0], name[-1]
        if kind in (M1, M2, M3):
            b, first, n = group(r)
            rows = pl.ds(0, RING * n)
        if kind == M1:
            p = pan.at[slot_of[L1, r]]

            def body(t):
                ns = pl.ds(pl.multiple_of(t * sub, sub), sub)
                s = total([(p[j, rows, h * dh:(h + 1) * dh], wus[2 * j + h, :, ns], NN) for j in range(RING) for h in range(2)])
                hbuf[b, span(r), ns] = s.astype(jnp.bfloat16)
            loop(body)
        elif kind == M2:
            p = pan.at[slot_of[L2, r]]
            if r > 0 and staged(r - 1):
                cp.arrived((ST, r - 1))
            step = min(32, RING * n)

            def body(t):
                ns = at_tile(t)
                acc[rows, :] = total([(p[j, rows, :], wds[2 * j + t], NT) for j in range(RING)])

                def elem(e):
                    rs = pl.ds(pl.multiple_of(e * step, step), step)
                    hs = pl.ds(pl.multiple_of(RING * first + e * step, step), step)
                    g, s = gelu_parts(hbuf[b, hs, ns].astype(jnp.float32))
                    hbuf[b, hs, ns] = g.astype(jnp.bfloat16)
                    obuf[2, t, hs, :] = (acc[rs, :] * s).astype(jnp.bfloat16)
                loop(elem, RING * n // step)
            if r == LAST:
                in_halves(r, [CS], body)
            else:
                loop(body)
        elif kind == M3:
            p = pan.at[slot_of[L3, r]]
            if r >= 2:
                for q in (Q2, QD, QS):
                    cp.left((q, r - 2))
            f = ft.at[r % 2]

            def body(t):
                f[t, rows, :] = total([(p[j, rows, :], wun[2 * j + t], NT) for j in range(RING)])
            if r == LAST:
                in_halves(r, [Q2, QD], body)
            else:
                loop(body)
        elif kind in (M5, M4):
            i0, m = PARTS[r]
            s0, s1 = (slot_of[L5 if kind == M5 else L4, i] for i in (i0, i0 + m - 1))
            j0, j1 = ((O5 if kind == M5 else O4)[i] for i in (i0, i0 + m - 1))
            own, par, p0 = (hbuf, wds, 0) if kind == M5 else (wus, wus, NB)
            if kind == M5 and i0 + m - 1 == 2:
                for g in range(NG):
                    cp.arrived((ST, g))
                    cp.left((CS, g))

            def body(i):
                e, t = (0, i) if m == 1 else (i // 2, lax.rem(i, 2))
                p = pan.at[s0 + e * (s1 - s0)]
                ms = pl.ds(pl.multiple_of(t * dh, dh), dh)
                s = total([(own[g, :, ms], p[g, :, lo], TN) for g in range(NB)] + [(par[p0 + g, :, ms], p[g, :, hi], TN) for g in range(NB)])
                if kind == M5 and O5[i0] == 0:
                    dwd[t, x] = s.astype(jnp.bfloat16)
                elif kind == M5:
                    obuf[i0 + e, t] = s.astype(jnp.bfloat16)
                else:
                    dwu[t, :, cols(j0 + e * (j1 - j0))] = s.astype(jnp.bfloat16)
            loop(body, CORES * m)
        else:
            b, first, n = group(r)
            f = ft.at[r % 2]
            rs = pl.ds(first, n)
            own = lambda k: pl.ds(k * n, n)
            if kind == QA:
                f[0, own(1), :] = f[0, own(1), :] + rst[b, 0, rs, :]
                f[1, own(3), :] = f[1, own(3), :] + rst[b, 1, rs, :]
            else:
                for h in range(2):
                    dx[b, rs, h * dh:(h + 1) * dh] = (f[h, own(0), :] + rrc[b, 0, h, rs, :] + rrc[b, 1, h, rs, :]).astype(jnp.bfloat16)

    for name, gone in order:
        for d in gone:
            cp.arrived(d)
            cp.left(d)
        for d in (it[name][2] if name in it else un[name][1]):
            cp.arrived(d)
        if name[0] == OWN:
            own = pl.ds(0, blk_rows)
            b0, b1 = pan.at[0, :, own], pan.at[1, :, own]
            cp.add((OUT, OWN), [(xa, b0, None), (za, b1, None)])
            cp.arrived((OUT, OWN))
            pairs = []
            for r in range(NG):
                b, first, n = group(r)
                pairs += [(pan.at[a, b, pl.ds(first, n)], buf[a].at[0, b, rel(r, 0)], None) for a in (X, G)]
            cp.add(name, pairs)
        elif name in it:
            for w in {LX: (0,), LH: (1,)}.get(name[0], ()):
                for p in range(3):
                    cp.left((WP, w, p))
            if name not in cp.by_name:
                cp.add(name, copies_of(name))
        else:
            unit(name)
    cp.finish()
    assert tuple(cp.used.values()) == (N_SEND, N_RECV, N_LOCAL), cp.used


def kernel(plan, order, panels, *refs):
    pl.run_scoped(functools.partial(work, plan, order, panels, *refs), *(pltpu.SemaphoreType.DMA((n,)) for n in (N_SEND, N_RECV, N_LOCAL)))


def write_out(dx, dwu, dwd, dx_out, dwu_out, dwd_out, sem):
    arrays = ((dx, dx_out), (dwu, dwu_out), (dwd, dwd_out))
    for i, (a, b) in enumerate(arrays):
        n = a.shape[1] // PIECES
        for j in range(a.shape[0]):
            for p in range(PIECES):
                rows = pl.ds(p * n, n)
                pltpu.make_async_copy(a.at[j, rows], b.at[j, rows], sem.at[i]).start()
    for i, (a, b) in enumerate(arrays):
        pltpu.make_async_copy(a, b, sem.at[i]).wait()


def solution(mesh):
    assert mesh.shape["cy"] == RING and mesh.shape["cz"] == RING and mesh.shape["cx"] == CORES
    row_spec = P(("dp", "cx", "cz"), "cy")
    up_spec = P("cy", ("cz", "cx"))
    down_spec = P("cz", ("cy", "cx"))
    up_out = P(("dp", "cy"), ("cz", "cx"))
    down_out = P(("dp", "cz"), ("cy", "cx"))
    plan = make_plan()
    order, panels, _, _ = make_order(plan, *make_lists(plan))

    def local_step(x_act, w_up, w_down, z_grad):
        t_loc, d_loc = x_act.shape
        f_loc = w_up.shape[1]
        rows, sub, dh = t_loc // NB, f_loc // RING, d_loc // 2
        grp = RING * rows
        bf, f32 = jnp.bfloat16, jnp.float32
        xa, za = x_act.reshape(NB, rows, d_loc), z_grad.reshape(NB, rows, d_loc)
        wu = w_up.reshape(2, dh, f_loc)
        wd = w_down.reshape(CORES, RING, sub, dh)
        hbm = lambda *s: jax.ShapeDtypeStruct(s, bf)
        outs = (
            pltpu.VMEM((NB, rows, d_loc), bf), pltpu.VMEM((2, dh, f_loc), bf), pltpu.VMEM((CORES, RING, sub, dh), bf),
            hbm(RING, NB, grp, d_loc), hbm(RING, NB, grp, d_loc), hbm(RING, NB, CORES, grp, sub),
            hbm(RING, NB, grp, sub), hbm(RING, NB, grp, sub), hbm(NB, grp, d_loc), hbm(NB, grp, 2 * sub),
            hbm(2, dh, sub), hbm(2, sub, dh), hbm(2, sub, dh),
        )
        scratch = [
            pltpu.VMEM((2 * RING, dh, 2 * sub), bf), pltpu.VMEM((2 * RING, sub, d_loc), bf), pltpu.VMEM((2 * RING, dh, 2 * sub), bf),
            pltpu.VMEM((NB, grp, 2 * sub), bf), pltpu.VMEM((PAN, RING, grp, d_loc), bf),
            pltpu.VMEM((2, 2, grp, dh), f32),
            pltpu.VMEM((NB, 2, rows, dh), f32), pltpu.VMEM((NB, 2, 2, rows, dh), f32),
            pltpu.VMEM((3, CORES, sub, dh), bf),
            pltpu.VMEM((grp, sub), f32),
        ]
        any_spec = pl.BlockSpec(memory_space=pl.ANY)
        res = pl.pallas_call(
            functools.partial(kernel, plan, order, panels),
            out_shape=outs,
            in_specs=[any_spec] * 4,
            out_specs=[pl.BlockSpec(memory_space=pltpu.VMEM)] * 3 + [any_spec] * (len(outs) - 3),
            scratch_shapes=scratch,
            compiler_params=pltpu.CompilerParams(collective_id=0, has_side_effects=True, vmem_limit_bytes=57600000),
            name="mlp_bwd",
        )(xa, wu, wd, za)
        outs = [pltpu.with_memory_space_constraint(o, pltpu.VMEM) for o in res[:3]]
        outs = pl.pallas_call(
            write_out,
            out_shape=[jax.ShapeDtypeStruct(o.shape, bf) for o in outs],
            in_specs=[pl.BlockSpec(memory_space=pltpu.VMEM) for _ in outs],
            out_specs=[any_spec for _ in outs],
            scratch_shapes=[pltpu.SemaphoreType.DMA((len(outs),))],
            compiler_params=pltpu.CompilerParams(vmem_limit_bytes=1 << 20),
            name="write_out",
        )(*outs)
        return tuple(o.reshape(a.shape) for o, a in zip(outs, (x_act, w_up, w_down)))

    return jax.shard_map(local_step, mesh=mesh, in_specs=(row_spec, up_spec, down_spec, row_spec), out_specs=(row_spec, up_out, down_out), check_vma=False)
```

```python
import functools
import math
import string

import jax
import jax.numpy as jnp
from jax import lax
from jax.experimental import pallas as pl
from jax.experimental.pallas import tpu as pltpu
from jax.sharding import PartitionSpec as P

GELU_COEF = 0.044715
SQRT_TWO_PI = math.sqrt(2.0 / math.pi)
NN = (((1,), (0,)), ((), ()))
NT = (((1,), (1,)), ((), ()))
TN = (((0,), (0,)), ((), ()))
MESH = pl.DeviceIdType.MESH
RING = 4
CORES = 2
PAN = 3
GROUPS = ((0, 0, 8), (1, 0, 8), (2, 0, 8), (3, 0, 4), (3, 4, 4))
NB = 4
NG = len(GROUPS)
EARLY = 2
X, G = 0, 1


def gelu_parts(pre_act):
    inner_arg = SQRT_TWO_PI * (pre_act + GELU_COEF * pre_act * pre_act * pre_act)
    tanh_val = jnp.tanh(inner_arg)
    gelu_val = 0.5 * pre_act * (1.0 + tanh_val)
    gelu_slope = 0.5 * (1.0 + tanh_val) + 0.5 * pre_act * (1.0 - tanh_val * tanh_val) * SQRT_TWO_PI * (1.0 + 3.0 * GELU_COEF * pre_act * pre_act)
    return gelu_val, gelu_slope


(XS, XR, W2, W1, WR, CS, CR, O2, O1, OR, YA, YB, YF, YR, Q2, QD, QS, WN, WP, GP, XP, HP, CP, CF,
 ST, OWN, L1, L2, L3, L4, L5, LX, LH, M1, M2, M3, M4, M5, QA, QF, OUT) = range(41)
PANEL_OF = {L1: M1, L2: M2, L3: M3, L4: M4, L5: M5}
O5 = (2, 1, 3, 0)
O4 = (0, 1, 3, 2)
PARTS = ((0, 1), (1, 2), (3, 1))
PART_OF = [p for p, (_, n) in enumerate(PARTS) for _ in range(n)]


def full(a, r):
    return [(XS, a, r), (XR, a, r), (YR, a, r), (OWN,)] + ([(YA, a, r), (YB, a, r)] if r < EARLY else [(YF, a, r)])


def staged(r):
    return GROUPS[r][2] == 8


def make_plan():
    it, un = {}, {}
    groups = range(NG)
    for r in groups:
        q = GROUPS[r][2] / 8 / NB
        f = 4 * q
        for a in (X, G):
            it[XS, a, r] = (0, q, [])
            it[XR, a, r] = (0, q / 2, [(XS, a, r)])
            row = [(XS, a, r), (XR, a, r)]
            if r < EARLY:
                it[YA, a, r] = (1, q, [])
                it[YB, a, r] = (1, 3 * q, row)
                it[YR, a, r] = (1, 2 * q, [(YA, a, r), (YB, a, r)])
            else:
                it[YF, a, r] = (1, 4 * q, row + [(OWN,)])
                it[YR, a, r] = (1, 2 * q, [(YF, a, r)])
        it[GP, r] = (2, 8 * q, full(G, r))
        it[XP, r] = (2, 4 * q, full(X, r))
        it[HP, r] = (2, 4 * q, [(M2, r)])
        it[ST, r] = (3, f, [(M2, r)])
        it[CS, r] = (0, f, [(ST, r) if staged(r) else (M2, r)])
        it[CR, r] = (0, 2 * q, [(CS, r)])
        dc = [(ST, r), (CS, r), (CR, r)]
        it[CP, r] = (2, 6 * q, [(ST, r), (CS, r)])
        it[CF, r] = (2, 2 * q, [(CR, r)])
        it[Q2, r] = (1, q, [(M3, r)])
        it[QD, r] = (1, q, [(M3, r)])
        it[QS, r] = (1, q, [(QA, r)])
        it[L1, r] = (3, 16 * q, full(X, r))
        it[L2, r] = (3, 16 * q, full(G, r))
        it[L3, r] = (3, 16 * q, dc)
        wu = [(WP, 0, p) for p in range(3)]
        wd = [(WP, 1, p) for p in range(3)]
        un[M1, r] = (0.4 + 4.4 * f, [(L1, r)] + wu)
        un[M2, r] = (0.4 + 6.2 * f, [(L2, r), (M1, r)] + wd)
        un[M3, r] = (0.4 + 4.4 * f, [(L3, r), (WN,)] + ([(QF, r - 2)] if r >= 2 else []))
        un[QA, r] = (0.1 + 0.4 * f, [(Q2, r)])
        un[QF, r] = (0.1 + 0.4 * f, [(QS, r), (QD, r)])
    for w in range(2):
        it[W2, w] = (0, 0.5, [])
        it[W1, w] = (0, 1.0, [])
        it[WR, w] = (0, 0.5, [(W2, w)])
        it[WP, w, 0] = (2, 1, [])
        it[WP, w, 1] = (2, 2, [(W1, w)])
        it[WP, w, 2] = (2, 1, [(WR, w)])
    it[(WN,)] = (2, 4, [])
    it[(OWN,)] = (3, 2, [])
    it[(O2,)] = (0, 0.5, [(M5, 0)])
    it[(O1,)] = (0, 1.0, [(M5, 1)])
    it[(OR,)] = (0, 0.5, [(O2,)])
    for p in range(RING):
        it[L5, p] = (3, 4, [(GP, r) for r in groups] + sum([full(G, r) for r in groups], []))
        it[L4, p] = (3, 4, [(CF if O4[p] == 2 else CP, r) for r in groups] + [((ST, CS, CS, CR)[p], r) for r in groups])
    it[(LH,)] = (3, 4, [(HP, r) for r in groups] + [(M2, r) for r in groups])
    it[(LX,)] = (3, 8, [(XP, r) for r in groups] + [(M5, 0)])
    for p, (first, n) in enumerate(PARTS):
        un[M4, p] = (4.8 * n, [(L4, first + i) for i in range(n)] + [(LX,)])
        un[M5, p] = (4.8 * n, [(L5, first + i) for i in range(n)] + [(LH,)])
    return it, un


ORDER = (
    "acbdimgInhjEHGFyJosuApzteBvkflqwrxCKDML",
    "admjbecsknfolutvzBACGIHJghipqrwxyDKELFM",
    "yompqhsjlwunkfAgBtxCiveabzcrEDd",
)


def make_lists(plan):
    it, un = plan
    base = [[n for n in it if it[n][0] == k] for k in range(len(ORDER) - 1)] + [list(un)]
    *lists, units = ([names[string.ascii_letters.index(ch)] for ch in key] for names, key in zip(base, ORDER))
    return lists, units


LINKS = range(4)
RATE = (22.5,) * 2 + (1.7, 0.4)
DELAY = (3.0,) * 2 + (1.5,) * 2


def make_order(plan, lists, units):
    it, un = plan
    done, free, pos = {}, [0.0 for _ in LINKS], [0 for _ in LINKS]
    pend, now, order, panels, waits = list(units), 0.0, [], [], []
    late = [n for n in it if it[n][0] >= 2]
    rank = {u: i for i, u in enumerate(units)}
    user = lambda n: (PANEL_OF[n[0]], PART_OF[n[1]] if n[0] in (L4, L5) else n[1])
    panel_rank = lambda n: rank[user(n)] if n[0] in PANEL_OF else rank[{LX: M4, LH: M5}[n[0]], 0] if n[0] in (LX, LH) else -1
    gone = set()
    big = 1e9

    def ready(n):
        return all(done.get(d, big) <= now for d in it[n][2])

    def send(n):
        k = it[n][0]
        start = max(now + 0.3, free[k])
        waits.append((k, start - free[k], n))
        free[k] = start + it[n][1] * RATE[k]
        done[n] = free[k] + DELAY[k]
        order.append((n, now))

    while True:
        for k in (0, 1):
            while pos[k] < len(lists[k]) and ready(lists[k][pos[k]]):
                send(lists[k][pos[k]])
                pos[k] += 1
        for n in sorted((n for n in late if ready(n)), key=lambda n: (panel_rank(n), n)):
            if n[0] in PANEL_OF:
                if len(panels) >= PAN and user(panels[-PAN]) not in gone:
                    continue
                panels.append(n)
            late.remove(n)
            send(n)
        can = [u for u in pend if all(done.get(d, big) <= now for d in un[u][1])]
        if can:
            pend.remove(can[0])
            order.append((can[0], now))
            now += un[can[0]][0]
            done[can[0]] = now
            gone.add(can[0])
            continue
        later = [v for v in done.values() if v > now]
        if not later:
            break
        now = min(later)
    assert not pend and not late and all(pos[k] == len(lists[k]) for k in (0, 1)), (pend, late, pos)
    return [(n, [m for m in it if t - 30 < done[m] <= t - 2 and it[m][0] < 3]) for n, t in order], panels, max(done.values()), waits


class Copies:
    BACK = {"R": "L", "L": "R", "U": "N", "N": "U", "P": "P"}

    def __init__(self, send, recv, local, peers):
        self.send, self.recv, self.local, self.peers = send, recv, local, peers
        self.by_name, self.clock = {}, 0
        self.used = {"send": 0, "recv": 0, "local": 0}
        self.free = {"send": [], "local": []} | {to: [] for to in peers}
        self.waited = {to: [] for to in peers}

    def take(self, kind, pool):
        if self.free[pool]:
            return self.free[pool].pop()
        self.used[kind] += 1
        return self.used[kind] - 1

    def add(self, name, pairs):
        made = []
        for src, dst, to in pairs:
            self.clock += 1
            if to is None:
                i = self.take("local", "local")
                made.append([pltpu.make_async_copy(src, dst, self.local.at[i]), to, self.clock, i, None])
            else:
                axis, idx = self.peers[to]
                i, j = self.take("send", "send"), self.take("recv", to)
                c = pltpu.make_async_remote_copy(src, dst, self.send.at[i], self.recv.at[j], device_id={axis: idx}, device_id_type=MESH)
                made.append([c, to, self.clock, i, j])
            made[-1][0].start()
        self.by_name.setdefault(name, []).extend(made)

    def arrived(self, name):
        for m in self.by_name.get(name, ()):
            c, to, started, i, j = m
            self.clock += 1
            if to is None and i is not None:
                c.wait()
                self.free["local"].append(i)
                m[3] = None
            elif j is not None:
                c.wait_recv()
                self.waited[to].append((self.clock, j))
                m[4] = None
                back = self.BACK[to]
                self.free[back] += [k for t, k in self.waited[back] if t < started]
                self.waited[back] = [(t, k) for t, k in self.waited[back] if t >= started]

    def left(self, name):
        for m in self.by_name.get(name, ()):
            if m[1] is None:
                self.arrived(name)
            elif m[3] is not None:
                m[0].wait_send()
                self.free["send"].append(m[3])
                m[3] = None

    def finish(self):
        for name in list(self.by_name):
            self.arrived(name)
            self.left(name)


PIECES = 4
N_SEND, N_RECV, N_LOCAL = 26, 54, 16


def work(plan, order, panels, xa, wu, wd, za, dx, dwu, dwd, XF, GF, DF, GPB, DPB, XPB, HPB, su, sd, sw,
           wus, wds, wun, hbuf, pan, ft, rst, rrc, obuf, acc, send, recv, local, ready):
    it, un = plan
    x, y, c = lax.axis_index("cy"), lax.axis_index("cz"), lax.axis_index("cx")
    peers = {
        "R": ("cy", lax.rem(x + 1, RING)), "L": ("cy", lax.rem(x + RING - 1, RING)),
        "U": ("cz", lax.rem(y + 1, RING)), "N": ("cz", lax.rem(y + RING - 1, RING)),
        "P": ("cx", 1 - c),
    }
    barrier = pltpu.get_barrier_semaphore()
    def tell(semaphore, to):
        axis, idx = peers[to]
        pl.semaphore_signal(semaphore, device_id={axis: idx}, device_id_type=MESH)

    ring = [to for to in peers if to != "P"]
    for to in ring:
        tell(barrier, to)
    pl.when(c == 0)(lambda: tell(barrier, "P"))
    pl.semaphore_wait(barrier, len(ring) + c)
    pl.when(c != 0)(lambda: tell(ready, "P"))
    waited = []

    cp = Copies(send, recv, local, peers)
    blk_rows = xa.shape[1]
    sub = wd.shape[2]
    dh = wu.shape[1]
    mine = pl.ds(pl.multiple_of(c * sub, sub), sub)
    theirs = pl.ds(pl.multiple_of((1 - c) * sub, sub), sub)
    lo, hi = pl.ds(0, sub), pl.ds(sub, sub)
    at = lambda j: lax.rem(x + j, RING)
    cols = lambda j: pl.ds(pl.multiple_of(at(j) * sub, sub), sub)
    slot_of = {n: i % PAN for i, n in enumerate(panels)}
    inp, buf = (xa, za), (XF, GF)

    def group(r):
        b, first, n = GROUPS[r]
        unit_rows = blk_rows // 8
        return b, first * unit_rows, n * unit_rows

    def rel(r, k, part=None):
        _, first, n = group(r)
        start = RING * first + k * n
        return pl.ds(start, n) if part is None else pl.ds(start + part * (n // 2), n // 2)

    def span(r):
        _, first, n = group(r)
        return pl.ds(RING * first, RING * n)

    def copies_of(name):
        kind, a, r = name[0], name[-2:][0], name[-1]
        both = lambda right, left: [right + ("R",), left + ("L",)]
        updn = lambda up, down: [up + ("U",), down + ("N",)]
        if kind == WN:
            return sum([[(wu.at[:, :, cols(j)], wun.at[2 * j:2 * j + 2, :, mine], to) for to in (None, "P")] for j in range(RING)], [])
        if kind == XS or kind == YA:
            b, first, n = group(r)
            src = inp[a].at[b, pl.ds(first, n)]
            if kind == XS:
                return both((src, buf[a].at[3, b, rel(r, 0)]), (src, buf[a].at[1, b, rel(r, 0)]))
            return updn((src, buf[a].at[0, b, rel(r, 3)]), (src, buf[a].at[0, b, rel(r, 1)]))
        if kind == XR:
            b, f, s = group(r)[0], rel(r, 0, 0), rel(r, 0, 1)
            return both((buf[a].at[3, b, f], buf[a].at[2, b, f]), (buf[a].at[1, b, s], buf[a].at[2, b, s]))
        if kind in (YB, YF):
            b, m = group(r)[0], buf[a]
            js = pl.ds(1, RING - 1) if kind == YB else pl.ds(0, RING)
            return updn((m.at[js, b, rel(r, 0)], m.at[js, b, rel(r, 3)]), (m.at[js, b, rel(r, 0)], m.at[js, b, rel(r, 1)]))
        if kind == YR:
            b, m = group(r)[0], buf[a]
            return updn((m.at[0:2, b, rel(r, 3)], m.at[0:2, b, rel(r, 2)]), (m.at[2:4, b, rel(r, 1)], m.at[2:4, b, rel(r, 2)]))
        if kind in (W2, W1, WR):
            half = (lambda h, j: wu.at[h, :, cols(j)]) if r == 0 else (lambda h, j: wd.at[h, at(j)])
            piece = (lambda j: wu.at[:, :, cols(j)]) if r == 0 else (lambda j: wd.at[:, at(j)])
            st, dst = (su, sd)[r], (wus, wds)[r]
            if kind == W2:
                return both((half(0, 2), st.at[0]), (half(1, 2), st.at[1]))
            if kind == W1:
                return both((piece(1), dst.at[6:8, :, mine]), (piece(3), dst.at[2:4, :, mine]))
            return both((st.at[0], dst.at[4, :, mine]), (st.at[1], dst.at[5, :, mine]))
        if kind == WP:
            m = (wus, wds)[a]
            if r == 0:
                src = wu.at[:, :, cols(0)] if a == 0 else wd.at[:, at(0)]
                return [(src, m.at[0:2, :, mine], to) for to in (None, "P")]
            return [(m.at[2 * j:2 * j + 2, :, mine], m.at[2 * j:2 * j + 2, :, mine], "P") for j in ((1, 3) if r == 1 else (2,))]
        if kind == GP:
            return [(GF.at[:, group(r)[0], span(r), theirs], GPB.at[:, group(r)[0], span(r)], "P")]
        if kind == XP:
            return [(XF.at[0, group(r)[0], span(r)], XPB.at[group(r)[0], span(r)], "P")]
        if kind == HP:
            return [(hbuf.at[group(r)[0], span(r)], HPB.at[group(r)[0], span(r)], "P")]
        if kind in (CP, CF):
            b = group(r)[0]
            js = (pl.ds(0, 2), pl.ds(3, 1)) if kind == CP else (pl.ds(2, 1),)
            return [(DF.at[j, b, 1 - c, span(r)], DPB.at[j, b, span(r)], "P") for j in js]
        if kind == ST:
            b = group(r)[0]
            return [(obuf.at[2, :, span(r)], DF.at[0, b, :, span(r)], None)]
        if kind == CS:
            b = group(r)[0]
            m = DF.at[0, b, :, span(r)] if staged(r) else obuf.at[2, :, span(r)]
            return both((m, DF.at[3, b, :, span(r)]), (m, DF.at[1, b, :, span(r)]))
        if kind == CR:
            b, first, n = group(r)
            f, s = (pl.ds(RING * first + h * 2 * n, 2 * n) for h in range(2))
            return both((DF.at[3, b, :, f], DF.at[2, b, :, f]), (DF.at[1, b, :, s], DF.at[2, b, :, s]))
        if kind in (Q2, QD, QS):
            b, first, n = group(r)
            f = ft.at[r % 2]
            own = lambda k: pl.ds(k * n, n)
            rs = pl.ds(first, n)
            if kind == Q2:
                return updn((f.at[0, own(2)], rst.at[b, 0, rs]), (f.at[1, own(2)], rst.at[b, 1, rs]))
            if kind == QD:
                return updn((f.at[1, own(1)], rrc.at[b, 0, 1, rs]), (f.at[0, own(3)], rrc.at[b, 1, 0, rs]))
            return updn((f.at[0, own(1)], rrc.at[b, 0, 0, rs]), (f.at[1, own(3)], rrc.at[b, 1, 1, rs]))
        if kind in (L1, L2, L3):
            b, _, n = group(r)
            to = pan.at[slot_of[name], :, pl.ds(0, RING * n)]
            if kind == L3:
                return [(DF.at[:, b, h, span(r)], to.at[:, :, h * sub:(h + 1) * sub], None) for h in range(CORES)]
            return [((XF if kind == L1 else GF).at[:, b, span(r)], to, None)]
        if kind in (L5, L4):
            m, p = (GF.at[O5[r], :, :, mine], GPB.at[O5[r]]) if kind == L5 else (DF.at[O4[r], :, c], DPB.at[O4[r]])
            s = pan.at[slot_of[name]]
            return [(m, s.at[:, :, lo], None), (p, s.at[:, :, hi], None)]
        if kind == LH:
            return [(HPB, wds.at[0:4], None)]
        if kind == LX:
            return [(XF.at[0], wus.at[0:4], None), (XPB, wus.at[4:8], None)]
        place = {j: i for i, j in enumerate(O5)}
        if kind == O2:
            return both((obuf.at[place[2], 0], sw.at[0]), (obuf.at[place[2], 1], sw.at[1]))
        if kind == O1:
            return both((obuf.at[place[1]], dwd.at[:, x]), (obuf.at[place[3]], dwd.at[:, x]))
        assert kind == OR
        return both((sw.at[0], dwd.at[0, at(3)]), (sw.at[1], dwd.at[1, at(1)]))

    def total(terms):
        out = None
        for a, b, dims in terms:
            d = lax.dot_general(a, b, dims, preferred_element_type=jnp.float32)
            out = d if out is None else out + d
        return out

    def loop(n, body):
        def step(i, carry):
            body(i)
            return carry
        lax.fori_loop(0, n, step, 0)

    def unit(name):
        kind, r = name[0], name[-1]
        if kind in (M1, M2, M3):
            b, first, n = group(r)
            rows = pl.ds(0, RING * n)
        if kind == M1:
            p = pan.at[slot_of[L1, r]]

            def body(t):
                ns = pl.ds(pl.multiple_of(t * sub, sub), sub)
                s = total([(p[j, rows, h * dh:(h + 1) * dh], wus[2 * j + h, :, ns], NN) for j in range(RING) for h in range(2)])
                hbuf[b, span(r), ns] = s.astype(jnp.bfloat16)
            loop(2, body)
        elif kind == M2:
            p = pan.at[slot_of[L2, r]]
            if r > 0 and staged(r - 1):
                cp.arrived((ST, r - 1))
            step = min(32, RING * n)

            def body(t):
                ns = pl.ds(pl.multiple_of(t * sub, sub), sub)
                acc[rows, :] = total([(p[j, rows, :], wds[2 * j + t], NT) for j in range(RING)])

                def elem(e):
                    rs = pl.ds(pl.multiple_of(e * step, step), step)
                    hs = pl.ds(pl.multiple_of(RING * first + e * step, step), step)
                    g, s = gelu_parts(hbuf[b, hs, ns].astype(jnp.float32))
                    hbuf[b, hs, ns] = g.astype(jnp.bfloat16)
                    obuf[2, t, hs, :] = (acc[rs, :] * s).astype(jnp.bfloat16)
                loop(RING * n // step, elem)
            loop(2, body)
        elif kind == M3:
            p = pan.at[slot_of[L3, r]]
            if r >= 2:
                for q in (Q2, QD, QS):
                    cp.left((q, r - 2))
            f = ft.at[r % 2]

            def body(t):
                f[t, rows, :] = total([(p[j, rows, :], wun[2 * j + t], NT) for j in range(RING)])
            loop(2, body)
        elif kind in (M5, M4):
            i0, m = PARTS[r]
            s0, s1 = (slot_of[L5 if kind == M5 else L4, i] for i in (i0, i0 + m - 1))
            j0, j1 = ((O5 if kind == M5 else O4)[i] for i in (i0, i0 + m - 1))
            own, par, p0 = (hbuf, wds, 0) if kind == M5 else (wus, wus, NB)
            if kind == M5 and i0 + m - 1 == 2:
                for g in range(NG):
                    cp.arrived((ST, g))
                    cp.left((CS, g))

            def body(i):
                e, t = (0, i) if m == 1 else (i // 2, lax.rem(i, 2))
                p = pan.at[s0 + e * (s1 - s0)]
                ms = pl.ds(pl.multiple_of(t * dh, dh), dh)
                s = total([(own[g, :, ms], p[g, :, lo], TN) for g in range(NB)] + [(par[p0 + g, :, ms], p[g, :, hi], TN) for g in range(NB)])
                if kind == M5 and O5[i0] == 0:
                    dwd[t, x] = s.astype(jnp.bfloat16)
                elif kind == M5:
                    obuf[i0 + e, t] = s.astype(jnp.bfloat16)
                else:
                    dwu[t, :, cols(j0 + e * (j1 - j0))] = s.astype(jnp.bfloat16)
            loop(2 * m, body)
        else:
            b, first, n = group(r)
            f = ft.at[r % 2]
            rs = pl.ds(first, n)
            own = lambda k: pl.ds(k * n, n)
            if kind == QA:
                f[0, own(1), :] = f[0, own(1), :] + rst[b, 0, rs, :]
                f[1, own(3), :] = f[1, own(3), :] + rst[b, 1, rs, :]
            else:
                for h in range(2):
                    dx[b, rs, h * dh:(h + 1) * dh] = (f[h, own(0), :] + rrc[b, 0, h, rs, :] + rrc[b, 1, h, rs, :]).astype(jnp.bfloat16)

    for name, gone in order:
        for d in gone:
            cp.arrived(d)
            cp.left(d)
        for d in (it[name][2] if name in it else un[name][1]):
            cp.arrived(d)
        if name[0] == OWN:
            own = pl.ds(0, blk_rows)
            b0, b1 = pan.at[0, :, own], pan.at[1, :, own]
            cp.add((OUT, OWN), [(xa, b0, None), (za, b1, None)])
            cp.arrived((OUT, OWN))
            pairs = []
            for r in range(NG):
                b, first, n = group(r)
                pairs += [(pan.at[a, b, pl.ds(first, n)], buf[a].at[0, b, rel(r, 0)], None) for a in (X, G)]
            cp.add(name, pairs)
        elif name in it:
            for w in {LX: (0,), LH: (1,)}.get(name[0], ()):
                for p in range(3):
                    cp.left((WP, w, p))
            copies = copies_of(name)
            if not waited and any(to == "P" for _, _, to in copies):
                waited.append(name)
                pl.when(c == 0)(lambda: pl.semaphore_wait(ready))
            cp.add(name, copies)
        else:
            unit(name)
    cp.finish()
    assert tuple(cp.used.values()) == (N_SEND, N_RECV, N_LOCAL), cp.used


def kernel(plan, order, panels, *refs):
    pl.run_scoped(functools.partial(work, plan, order, panels, *refs), *(pltpu.SemaphoreType.DMA((n,)) for n in (N_SEND, N_RECV, N_LOCAL)), pltpu.SemaphoreType.REGULAR)


def write_out(dx, dwu, dwd, dx_out, dwu_out, dwd_out, sem):
    arrays = ((dx, dx_out), (dwu, dwu_out), (dwd, dwd_out))
    for i, (a, b) in enumerate(arrays):
        n = a.shape[1] // PIECES
        for j in range(a.shape[0]):
            for p in range(PIECES):
                rows = pl.ds(p * n, n)
                pltpu.make_async_copy(a.at[j, rows], b.at[j, rows], sem.at[i]).start()
    for i, (a, b) in enumerate(arrays):
        pltpu.make_async_copy(a, b, sem.at[i]).wait()


def solution(mesh):
    assert mesh.shape["cy"] == RING and mesh.shape["cz"] == RING and mesh.shape["cx"] == CORES
    row_spec = P(("dp", "cx", "cz"), "cy")
    up_spec = P("cy", ("cz", "cx"))
    down_spec = P("cz", ("cy", "cx"))
    up_out = P(("dp", "cy"), ("cz", "cx"))
    down_out = P(("dp", "cz"), ("cy", "cx"))
    plan = make_plan()
    order, panels, _, _ = make_order(plan, *make_lists(plan))

    def local_step(x_act, w_up, w_down, z_grad):
        t_loc, d_loc = x_act.shape
        f_loc = w_up.shape[1]
        rows, sub, dh = t_loc // NB, f_loc // RING, d_loc // 2
        grp = RING * rows
        bf, f32 = jnp.bfloat16, jnp.float32
        xa, za = x_act.reshape(NB, rows, d_loc), z_grad.reshape(NB, rows, d_loc)
        wu = w_up.reshape(2, dh, f_loc)
        wd = w_down.reshape(CORES, RING, sub, dh)
        hbm = lambda *s: jax.ShapeDtypeStruct(s, bf)
        outs = (
            pltpu.VMEM((NB, rows, d_loc), bf), pltpu.VMEM((2, dh, f_loc), bf), pltpu.VMEM((CORES, RING, sub, dh), bf),
            hbm(RING, NB, grp, d_loc), hbm(RING, NB, grp, d_loc), hbm(RING, NB, CORES, grp, sub),
            hbm(RING, NB, grp, sub), hbm(RING, NB, grp, sub), hbm(NB, grp, d_loc), hbm(NB, grp, 2 * sub),
            hbm(2, dh, sub), hbm(2, sub, dh), hbm(2, sub, dh),
        )
        scratch = [
            pltpu.VMEM((2 * RING, dh, 2 * sub), bf), pltpu.VMEM((2 * RING, sub, d_loc), bf), pltpu.VMEM((2 * RING, dh, 2 * sub), bf),
            pltpu.VMEM((NB, grp, 2 * sub), bf), pltpu.VMEM((PAN, RING, grp, d_loc), bf),
            pltpu.VMEM((2, 2, grp, dh), f32),
            pltpu.VMEM((NB, 2, rows, dh), f32), pltpu.VMEM((NB, 2, 2, rows, dh), f32),
            pltpu.VMEM((3, CORES, sub, dh), bf),
            pltpu.VMEM((grp, sub), f32),
        ]
        any_spec = pl.BlockSpec(memory_space=pl.ANY)
        res = pl.pallas_call(
            functools.partial(kernel, plan, order, panels),
            out_shape=outs,
            in_specs=[any_spec] * 4,
            out_specs=[pl.BlockSpec(memory_space=pltpu.VMEM)] * 3 + [any_spec] * (len(outs) - 3),
            scratch_shapes=scratch,
            compiler_params=pltpu.CompilerParams(collective_id=0, has_side_effects=True, vmem_limit_bytes=57600000),
            name="mlp_bwd",
        )(xa, wu, wd, za)
        outs = [pltpu.with_memory_space_constraint(o, pltpu.VMEM) for o in res[:3]]
        outs = pl.pallas_call(
            write_out,
            out_shape=[jax.ShapeDtypeStruct(o.shape, bf) for o in outs],
            in_specs=[pl.BlockSpec(memory_space=pltpu.VMEM) for _ in outs],
            out_specs=[any_spec for _ in outs],
            scratch_shapes=[pltpu.SemaphoreType.DMA((len(outs),))],
            compiler_params=pltpu.CompilerParams(vmem_limit_bytes=1 << 20),
            name="write_out",
        )(*outs)
        return tuple(o.reshape(a.shape) for o, a in zip(outs, (x_act, w_up, w_down)))

    return jax.shard_map(local_step, mesh=mesh, in_specs=(row_spec, up_spec, down_spec, row_spec), out_specs=(row_spec, up_out, down_out), check_vma=False)
```

```python
import functools
import math
import string

import jax
import jax.numpy as jnp
from jax import lax
from jax.experimental import pallas as pl
from jax.experimental.pallas import tpu as pltpu
from jax.sharding import PartitionSpec as P

GELU_COEF = 0.044715
SQRT_TWO_PI = math.sqrt(2.0 / math.pi)
NN = (((1,), (0,)), ((), ()))
NT = (((1,), (1,)), ((), ()))
TN = (((0,), (0,)), ((), ()))
MESH = pl.DeviceIdType.MESH
RING = 4
CORES = 2
PAN = 3
GROUPS = ((0, 0, 8), (1, 0, 8), (2, 0, 8), (3, 0, 4), (3, 4, 4))
NB = 4
NG = len(GROUPS)
LAST = NG - 1
EARLY = 2
X, G = 0, 1


def gelu_parts(pre_act):
    inner_arg = SQRT_TWO_PI * (pre_act + GELU_COEF * pre_act * pre_act * pre_act)
    tanh_val = jnp.tanh(inner_arg)
    gelu_val = 0.5 * pre_act * (1.0 + tanh_val)
    gelu_slope = 0.5 * (1.0 + tanh_val) + 0.5 * pre_act * (1.0 - tanh_val * tanh_val) * SQRT_TWO_PI * (1.0 + 3.0 * GELU_COEF * pre_act * pre_act)
    return gelu_val, gelu_slope


(XS, XR, W2, W1, WR, CS, CR, O2, O1, OR, YA, YB, YF, YR, Q2, QD, QS, WN, WP, GP, XP, HP, CP, CF,
 ST, OWN, L1, L2, L3, L4, L5, LX, LH, M1, M2, M3, M4, M5, QA, QF, OUT) = range(41)
PANEL_OF = {L1: M1, L2: M2, L3: M3, L4: M4, L5: M5}
O5 = (2, 1, 3, 0)
O4 = (0, 1, 3, 2)
PARTS = ((0, 1), (1, 2), (3, 1))
PART_OF = [p for p, (_, n) in enumerate(PARTS) for _ in range(n)]


def full(a, r):
    return [(XS, a, r), (XR, a, r), (YR, a, r), (OWN,)] + ([(YA, a, r), (YB, a, r)] if r < EARLY else [(YF, a, r)])


def staged(r):
    return GROUPS[r][2] == 8


def make_plan():
    it, un = {}, {}
    groups = range(NG)
    for r in groups:
        q = GROUPS[r][2] / 8 / NB
        f = 4 * q
        for a in (X, G):
            it[XS, a, r] = (0, q, [])
            it[XR, a, r] = (0, q / 2, [(XS, a, r)])
            row = [(XS, a, r), (XR, a, r)]
            if r < EARLY:
                it[YA, a, r] = (1, q, [])
                it[YB, a, r] = (1, 3 * q, row)
                it[YR, a, r] = (1, 2 * q, [(YA, a, r), (YB, a, r)])
            else:
                it[YF, a, r] = (1, 4 * q, row + [(OWN,)])
                it[YR, a, r] = (1, 2 * q, [(YF, a, r)])
        it[GP, r] = (2, 8 * q, full(G, r))
        it[XP, r] = (2, 4 * q, full(X, r))
        it[HP, r] = (2, 4 * q, [(M2, r)])
        it[ST, r] = (3, f, [(M2, r)])
        it[CS, r] = (0, f, [(ST, r) if staged(r) else (M2, r)])
        it[CR, r] = (0, 2 * q, [(CS, r)])
        dc = [(ST, r), (CS, r), (CR, r)]
        it[CP, r] = (2, 6 * q, [(ST, r), (CS, r)])
        it[CF, r] = (2, 2 * q, [(CR, r)])
        it[Q2, r] = (1, q, [(M3, r)])
        it[QD, r] = (1, q, [(M3, r)])
        it[QS, r] = (1, q, [(QA, r)])
        it[L1, r] = (3, 16 * q, full(X, r))
        it[L2, r] = (3, 16 * q, full(G, r))
        it[L3, r] = (3, 16 * q, dc)
        wu = [(WP, 0, p) for p in range(3)]
        wd = [(WP, 1, p) for p in range(3)]
        un[M1, r] = (0.4 + 4.4 * f, [(L1, r)] + wu)
        un[M2, r] = (0.4 + 6.2 * f, [(L2, r), (M1, r)] + wd)
        un[M3, r] = (0.4 + 4.4 * f, [(L3, r), (WN,)] + ([(QF, r - 2)] if r >= 2 else []))
        un[QA, r] = (0.1 + 0.4 * f, [(Q2, r)])
        un[QF, r] = (0.1 + 0.4 * f, [(QS, r), (QD, r)])
    for w in range(2):
        it[W2, w] = (0, 0.5, [])
        it[W1, w] = (0, 1.0, [])
        it[WR, w] = (0, 0.5, [(W2, w)])
        it[WP, w, 0] = (2, 1, [])
        it[WP, w, 1] = (2, 2, [(W1, w)])
        it[WP, w, 2] = (2, 1, [(WR, w)])
    it[(WN,)] = (2, 4, [])
    it[(OWN,)] = (3, 2, [])
    it[(O2,)] = (0, 0.5, [(M5, 0)])
    it[(O1,)] = (0, 1.0, [(M5, 1)])
    it[(OR,)] = (0, 0.5, [(O2,)])
    for p in range(RING):
        it[L5, p] = (3, 4, [(GP, r) for r in groups] + sum([full(G, r) for r in groups], []))
        it[L4, p] = (3, 4, [(CF if O4[p] == 2 else CP, r) for r in groups] + [((ST, CS, CS, CR)[p], r) for r in groups])
    it[(LH,)] = (3, 4, [(HP, r) for r in groups] + [(M2, r) for r in groups])
    it[(LX,)] = (3, 8, [(XP, r) for r in groups] + [(M5, 0)])
    for p, (first, n) in enumerate(PARTS):
        un[M4, p] = (4.8 * n, [(L4, first + i) for i in range(n)] + [(LX,)])
        un[M5, p] = (4.8 * n, [(L5, first + i) for i in range(n)] + [(LH,)])
    return it, un


ORDER = (
    "abicgdhjmFnIEHGJuosAyptBekvzflqwrxCKDLM",
    "dajmbenscfkolutvzBACGIHJghipqrwxyDELKFM",
    "gkbyAdcesvDuphBmoiwCrltjaxzqfEn",
)


def make_lists(plan):
    it, un = plan
    base = [[n for n in it if it[n][0] == k] for k in range(len(ORDER) - 1)] + [list(un)]
    *lists, units = ([names[string.ascii_letters.index(ch)] for ch in key] for names, key in zip(base, ORDER))
    return lists, units


LINKS = range(4)
RATE = (22.5,) * 2 + (1.7, 0.4)
DELAY = (3.0,) * 2 + (1.5,) * 2


def make_order(plan, lists, units):
    it, un = plan
    done, free, pos = {}, [0.0 for _ in LINKS], [0 for _ in LINKS]
    pend, now, order, panels, waits = list(units), 0.0, [], [], []
    late = [n for n in it if it[n][0] >= 2]
    rank = {u: i for i, u in enumerate(units)}
    user = lambda n: (PANEL_OF[n[0]], PART_OF[n[1]] if n[0] in (L4, L5) else n[1])
    panel_rank = lambda n: rank[user(n)] if n[0] in PANEL_OF else rank[{LX: M4, LH: M5}[n[0]], 0] if n[0] in (LX, LH) else -1
    gone = set()
    big = 1e9

    def ready(n):
        return all(done.get(d, big) <= now for d in it[n][2])

    def send(n):
        k = it[n][0]
        start = max(now + 0.3, free[k])
        waits.append((k, start - free[k], n))
        free[k] = start + it[n][1] * RATE[k]
        done[n] = free[k] + DELAY[k]
        order.append((n, now))

    while True:
        for k in (0, 1):
            while pos[k] < len(lists[k]) and ready(lists[k][pos[k]]):
                send(lists[k][pos[k]])
                pos[k] += 1
        for n in sorted((n for n in late if ready(n)), key=lambda n: (panel_rank(n), n)):
            if n[0] in PANEL_OF:
                if len(panels) >= PAN and user(panels[-PAN]) not in gone:
                    continue
                panels.append(n)
            late.remove(n)
            send(n)
        can = [u for u in pend if all(done.get(d, big) <= now for d in un[u][1])]
        if can:
            pend.remove(can[0])
            order.append((can[0], now))
            now += un[can[0]][0]
            done[can[0]] = now
            gone.add(can[0])
            continue
        later = [v for v in done.values() if v > now]
        if not later:
            break
        now = min(later)
    assert not pend and not late and all(pos[k] == len(lists[k]) for k in (0, 1)), (pend, late, pos)
    return [(n, [m for m in it if t - 30 < done[m] <= t - 2 and it[m][0] < 3]) for n, t in order], panels, max(done.values()), waits


class Copies:
    BACK = {"R": "L", "L": "R", "U": "N", "N": "U", "P": "P"}

    def __init__(self, send, recv, local, peers):
        self.send, self.recv, self.local, self.peers = send, recv, local, peers
        self.by_name, self.clock = {}, 0
        self.used = {"send": 0, "recv": 0, "local": 0}
        self.free = {"send": [], "local": []} | {to: [] for to in peers}
        self.waited = {to: [] for to in peers}

    def take(self, kind, pool):
        if self.free[pool]:
            return self.free[pool].pop()
        self.used[kind] += 1
        return self.used[kind] - 1

    def add(self, name, pairs):
        made = []
        for src, dst, to in pairs:
            self.clock += 1
            if to is None:
                i = self.take("local", "local")
                made.append([pltpu.make_async_copy(src, dst, self.local.at[i]), to, self.clock, i, None])
            else:
                axis, idx = self.peers[to]
                i, j = self.take("send", "send"), self.take("recv", to)
                c = pltpu.make_async_remote_copy(src, dst, self.send.at[i], self.recv.at[j], device_id={axis: idx}, device_id_type=MESH)
                made.append([c, to, self.clock, i, j])
            made[-1][0].start()
        self.by_name.setdefault(name, []).extend(made)

    def arrived(self, name):
        for m in self.by_name.get(name, ()):
            c, to, started, i, j = m
            self.clock += 1
            if to is None and i is not None:
                c.wait()
                self.free["local"].append(i)
                m[3] = None
            elif j is not None:
                c.wait_recv()
                self.waited[to].append((self.clock, j))
                m[4] = None
                back = self.BACK[to]
                self.free[back] += [k for t, k in self.waited[back] if t < started]
                self.waited[back] = [(t, k) for t, k in self.waited[back] if t >= started]

    def left(self, name):
        for m in self.by_name.get(name, ()):
            if m[1] is None:
                self.arrived(name)
            elif m[3] is not None:
                m[0].wait_send()
                self.free["send"].append(m[3])
                m[3] = None

    def finish(self):
        for name in list(self.by_name):
            self.arrived(name)
            self.left(name)


PIECES = 4
N_SEND, N_RECV, N_LOCAL = 24, 48, 16


def work(plan, order, panels, xa, wu, wd, za, dx, dwu, dwd, XF, GF, DF, GPB, DPB, XPB, HPB, su, sd, sw,
           wus, wds, wun, hbuf, pan, ft, rst, rrc, obuf, acc, send, recv, local, ready):
    it, un = plan
    x, y, c = lax.axis_index("cy"), lax.axis_index("cz"), lax.axis_index("cx")
    peers = {
        "R": ("cy", lax.rem(x + 1, RING)), "L": ("cy", lax.rem(x + RING - 1, RING)),
        "U": ("cz", lax.rem(y + 1, RING)), "N": ("cz", lax.rem(y + RING - 1, RING)),
        "P": ("cx", 1 - c),
    }
    barrier = pltpu.get_barrier_semaphore()
    def tell(semaphore, to):
        axis, idx = peers[to]
        pl.semaphore_signal(semaphore, device_id={axis: idx}, device_id_type=MESH)

    ring = [to for to in peers if to != "P"]
    for to in ring:
        tell(barrier, to)
    pl.when(c == 0)(lambda: tell(barrier, "P"))
    pl.semaphore_wait(barrier, len(ring) + c)
    pl.when(c != 0)(lambda: tell(ready, "P"))
    waited = []

    cp = Copies(send, recv, local, peers)
    blk_rows = xa.shape[1]
    sub = wd.shape[2]
    dh = wu.shape[1]
    mine = pl.ds(pl.multiple_of(c * sub, sub), sub)
    theirs = pl.ds(pl.multiple_of((1 - c) * sub, sub), sub)
    lo, hi = pl.ds(0, sub), pl.ds(sub, sub)
    at = lambda j: lax.rem(x + j, RING)
    cols = lambda j: pl.ds(pl.multiple_of(at(j) * sub, sub), sub)
    slot_of = {n: i % PAN for i, n in enumerate(panels)}
    inp, buf = (xa, za), (XF, GF)

    def group(r):
        b, first, n = GROUPS[r]
        unit_rows = blk_rows // 8
        return b, first * unit_rows, n * unit_rows

    def rel(r, k, part=None):
        _, first, n = group(r)
        start = RING * first + k * n
        return pl.ds(start, n) if part is None else pl.ds(start + part * (n // 2), n // 2)

    def span(r):
        _, first, n = group(r)
        return pl.ds(RING * first, RING * n)

    def of_part(copies, part, turned=False):
        return [c for i, c in enumerate(copies) if part is None or (i == part) != turned]

    def in_halves(r, kinds, body):
        for t in range(CORES):
            body(t)
            for kind in kinds:
                cp.add((kind, r), copies_of((kind, r), t))

    def copies_of(name, part=None):
        kind, a, r = name[0], name[-2:][0], name[-1]
        both = lambda right, left: [right + ("R",), left + ("L",)]
        updn = lambda up, down: [up + ("U",), down + ("N",)]
        if kind == WN:
            return sum([[(wu.at[:, :, cols(j)], wun.at[2 * j:2 * j + 2, :, mine], to) for to in (None, "P")] for j in range(RING)], [])
        if kind == XS or kind == YA:
            b, first, n = group(r)
            src = inp[a].at[b, pl.ds(first, n)]
            if kind == XS:
                return both((src, buf[a].at[3, b, rel(r, 0)]), (src, buf[a].at[1, b, rel(r, 0)]))
            return updn((src, buf[a].at[0, b, rel(r, 3)]), (src, buf[a].at[0, b, rel(r, 1)]))
        if kind == XR:
            b, f, s = group(r)[0], rel(r, 0, 0), rel(r, 0, 1)
            return both((buf[a].at[3, b, f], buf[a].at[2, b, f]), (buf[a].at[1, b, s], buf[a].at[2, b, s]))
        if kind in (YB, YF):
            b, m = group(r)[0], buf[a]
            js = pl.ds(1, RING - 1) if kind == YB else pl.ds(0, RING)
            return updn((m.at[js, b, rel(r, 0)], m.at[js, b, rel(r, 3)]), (m.at[js, b, rel(r, 0)], m.at[js, b, rel(r, 1)]))
        if kind == YR:
            b, m = group(r)[0], buf[a]
            return updn((m.at[0:2, b, rel(r, 3)], m.at[0:2, b, rel(r, 2)]), (m.at[2:4, b, rel(r, 1)], m.at[2:4, b, rel(r, 2)]))
        if kind in (W2, W1, WR):
            half = (lambda h, j: wu.at[h, :, cols(j)]) if r == 0 else (lambda h, j: wd.at[h, at(j)])
            piece = (lambda j: wu.at[:, :, cols(j)]) if r == 0 else (lambda j: wd.at[:, at(j)])
            st, dst = (su, sd)[r], (wus, wds)[r]
            if kind == W2:
                return both((half(0, 2), st.at[0]), (half(1, 2), st.at[1]))
            if kind == W1:
                return both((piece(1), dst.at[6:8, :, mine]), (piece(3), dst.at[2:4, :, mine]))
            return both((st.at[0], dst.at[4, :, mine]), (st.at[1], dst.at[5, :, mine]))
        if kind == WP:
            m = (wus, wds)[a]
            if r == 0:
                src = wu.at[:, :, cols(0)] if a == 0 else wd.at[:, at(0)]
                return [(src, m.at[0:2, :, mine], to) for to in (None, "P")]
            return [(m.at[2 * j:2 * j + 2, :, mine], m.at[2 * j:2 * j + 2, :, mine], "P") for j in ((1, 3) if r == 1 else (2,))]
        if kind == GP:
            return [(GF.at[:, group(r)[0], span(r), theirs], GPB.at[:, group(r)[0], span(r)], "P")]
        if kind == XP:
            return [(XF.at[0, group(r)[0], span(r)], XPB.at[group(r)[0], span(r)], "P")]
        if kind == HP:
            return [(hbuf.at[group(r)[0], span(r)], HPB.at[group(r)[0], span(r)], "P")]
        if kind in (CP, CF):
            b = group(r)[0]
            js = (pl.ds(0, 2), pl.ds(3, 1)) if kind == CP else (pl.ds(2, 1),)
            return [(DF.at[j, b, 1 - c, span(r)], DPB.at[j, b, span(r)], "P") for j in js]
        if kind == ST:
            b = group(r)[0]
            return [(obuf.at[2, :, span(r)], DF.at[0, b, :, span(r)], None)]
        if kind == CS:
            b = group(r)[0]
            h = pl.ds(0, CORES) if part is None else part
            m = DF.at[0, b, h, span(r)] if staged(r) else obuf.at[2, h, span(r)]
            return both((m, DF.at[3, b, h, span(r)]), (m, DF.at[1, b, h, span(r)]))
        if kind == CR:
            b, first, n = group(r)
            f, s = (pl.ds(RING * first + h * 2 * n, 2 * n) for h in range(2))
            return both((DF.at[3, b, :, f], DF.at[2, b, :, f]), (DF.at[1, b, :, s], DF.at[2, b, :, s]))
        if kind in (Q2, QD, QS):
            b, first, n = group(r)
            f = ft.at[r % 2]
            own = lambda k: pl.ds(k * n, n)
            rs = pl.ds(first, n)
            if kind == Q2:
                return of_part(updn((f.at[0, own(2)], rst.at[b, 0, rs]), (f.at[1, own(2)], rst.at[b, 1, rs])), part)
            if kind == QD:
                return of_part(updn((f.at[1, own(1)], rrc.at[b, 0, 1, rs]), (f.at[0, own(3)], rrc.at[b, 1, 0, rs])), part, True)
            return updn((f.at[0, own(1)], rrc.at[b, 0, 0, rs]), (f.at[1, own(3)], rrc.at[b, 1, 1, rs]))
        if kind in (L1, L2, L3):
            b, _, n = group(r)
            to = pan.at[slot_of[name], :, pl.ds(0, RING * n)]
            if kind == L3:
                return [(DF.at[:, b, h, span(r)], to.at[:, :, h * sub:(h + 1) * sub], None) for h in range(CORES)]
            return [((XF if kind == L1 else GF).at[:, b, span(r)], to, None)]
        if kind in (L5, L4):
            m, p = (GF.at[O5[r], :, :, mine], GPB.at[O5[r]]) if kind == L5 else (DF.at[O4[r], :, c], DPB.at[O4[r]])
            s = pan.at[slot_of[name]]
            return [(m, s.at[:, :, lo], None), (p, s.at[:, :, hi], None)]
        if kind == LH:
            return [(HPB, wds.at[0:4], None)]
        if kind == LX:
            return [(XF.at[0], wus.at[0:4], None), (XPB, wus.at[4:8], None)]
        place = {j: i for i, j in enumerate(O5)}
        if kind == O2:
            return both((obuf.at[place[2], 0], sw.at[0]), (obuf.at[place[2], 1], sw.at[1]))
        if kind == O1:
            return both((obuf.at[place[1]], dwd.at[:, x]), (obuf.at[place[3]], dwd.at[:, x]))
        assert kind == OR
        return both((sw.at[0], dwd.at[0, at(3)]), (sw.at[1], dwd.at[1, at(1)]))

    def total(terms):
        out = None
        for a, b, dims in terms:
            d = lax.dot_general(a, b, dims, preferred_element_type=jnp.float32)
            out = d if out is None else out + d
        return out

    def at_tile(t):
        return pl.ds(t * sub if isinstance(t, int) else pl.multiple_of(t * sub, sub), sub)

    def loop(body, n=CORES):
        def step(i, carry):
            body(i)
            return carry
        lax.fori_loop(0, n, step, 0)

    def unit(name):
        kind, r = name[0], name[-1]
        if kind in (M1, M2, M3):
            b, first, n = group(r)
            rows = pl.ds(0, RING * n)
        if kind == M1:
            p = pan.at[slot_of[L1, r]]

            def body(t):
                ns = pl.ds(pl.multiple_of(t * sub, sub), sub)
                s = total([(p[j, rows, h * dh:(h + 1) * dh], wus[2 * j + h, :, ns], NN) for j in range(RING) for h in range(2)])
                hbuf[b, span(r), ns] = s.astype(jnp.bfloat16)
            loop(body)
        elif kind == M2:
            p = pan.at[slot_of[L2, r]]
            if r > 0 and staged(r - 1):
                cp.arrived((ST, r - 1))
            step = min(32, RING * n)

            def body(t):
                ns = at_tile(t)
                acc[rows, :] = total([(p[j, rows, :], wds[2 * j + t], NT) for j in range(RING)])

                def elem(e):
                    rs = pl.ds(pl.multiple_of(e * step, step), step)
                    hs = pl.ds(pl.multiple_of(RING * first + e * step, step), step)
                    g, s = gelu_parts(hbuf[b, hs, ns].astype(jnp.float32))
                    hbuf[b, hs, ns] = g.astype(jnp.bfloat16)
                    obuf[2, t, hs, :] = (acc[rs, :] * s).astype(jnp.bfloat16)
                loop(elem, RING * n // step)
            if r == LAST:
                in_halves(r, [CS], body)
            else:
                loop(body)
        elif kind == M3:
            p = pan.at[slot_of[L3, r]]
            if r >= 2:
                for q in (Q2, QD, QS):
                    cp.left((q, r - 2))
            f = ft.at[r % 2]

            def body(t):
                f[t, rows, :] = total([(p[j, rows, :], wun[2 * j + t], NT) for j in range(RING)])
            if r == LAST:
                in_halves(r, [Q2, QD], body)
            else:
                loop(body)
        elif kind in (M5, M4):
            i0, m = PARTS[r]
            s0, s1 = (slot_of[L5 if kind == M5 else L4, i] for i in (i0, i0 + m - 1))
            j0, j1 = ((O5 if kind == M5 else O4)[i] for i in (i0, i0 + m - 1))
            own, par, p0 = (hbuf, wds, 0) if kind == M5 else (wus, wus, NB)
            if kind == M5 and i0 + m - 1 == 2:
                for g in range(NG):
                    cp.arrived((ST, g))
                    cp.left((CS, g))

            def body(i):
                e, t = (0, i) if m == 1 else (i // 2, lax.rem(i, 2))
                p = pan.at[s0 + e * (s1 - s0)]
                ms = pl.ds(pl.multiple_of(t * dh, dh), dh)
                s = total([(own[g, :, ms], p[g, :, lo], TN) for g in range(NB)] + [(par[p0 + g, :, ms], p[g, :, hi], TN) for g in range(NB)])
                if kind == M5 and O5[i0] == 0:
                    dwd[t, x] = s.astype(jnp.bfloat16)
                elif kind == M5:
                    obuf[i0 + e, t] = s.astype(jnp.bfloat16)
                else:
                    dwu[t, :, cols(j0 + e * (j1 - j0))] = s.astype(jnp.bfloat16)
            loop(body, CORES * m)
        else:
            b, first, n = group(r)
            f = ft.at[r % 2]
            rs = pl.ds(first, n)
            own = lambda k: pl.ds(k * n, n)
            if kind == QA:
                f[0, own(1), :] = f[0, own(1), :] + rst[b, 0, rs, :]
                f[1, own(3), :] = f[1, own(3), :] + rst[b, 1, rs, :]
            else:
                for h in range(2):
                    dx[b, rs, h * dh:(h + 1) * dh] = (f[h, own(0), :] + rrc[b, 0, h, rs, :] + rrc[b, 1, h, rs, :]).astype(jnp.bfloat16)

    for name, gone in order:
        for d in gone:
            cp.arrived(d)
            cp.left(d)
        for d in (it[name][2] if name in it else un[name][1]):
            cp.arrived(d)
        if name[0] == OWN:
            own = pl.ds(0, blk_rows)
            b0, b1 = pan.at[0, :, own], pan.at[1, :, own]
            cp.add((OUT, OWN), [(xa, b0, None), (za, b1, None)])
            cp.arrived((OUT, OWN))
            pairs = []
            for r in range(NG):
                b, first, n = group(r)
                pairs += [(pan.at[a, b, pl.ds(first, n)], buf[a].at[0, b, rel(r, 0)], None) for a in (X, G)]
            cp.add(name, pairs)
        elif name in it:
            for w in {LX: (0,), LH: (1,)}.get(name[0], ()):
                for p in range(3):
                    cp.left((WP, w, p))
            if name in cp.by_name:
                continue
            copies = copies_of(name)
            if not waited and any(to == "P" for _, _, to in copies):
                waited.append(name)
                pl.when(c == 0)(lambda: pl.semaphore_wait(ready))
            cp.add(name, copies)
        else:
            unit(name)
    cp.finish()
    assert tuple(cp.used.values()) == (N_SEND, N_RECV, N_LOCAL), cp.used


def kernel(plan, order, panels, *refs):
    pl.run_scoped(functools.partial(work, plan, order, panels, *refs), *(pltpu.SemaphoreType.DMA((n,)) for n in (N_SEND, N_RECV, N_LOCAL)), pltpu.SemaphoreType.REGULAR)


def write_out(dx, dwu, dwd, dx_out, dwu_out, dwd_out, sem):
    arrays = ((dx, dx_out), (dwu, dwu_out), (dwd, dwd_out))
    for i, (a, b) in enumerate(arrays):
        n = a.shape[1] // PIECES
        for j in range(a.shape[0]):
            for p in range(PIECES):
                rows = pl.ds(p * n, n)
                pltpu.make_async_copy(a.at[j, rows], b.at[j, rows], sem.at[i]).start()
    for i, (a, b) in enumerate(arrays):
        pltpu.make_async_copy(a, b, sem.at[i]).wait()


def solution(mesh):
    assert mesh.shape["cy"] == RING and mesh.shape["cz"] == RING and mesh.shape["cx"] == CORES
    row_spec = P(("dp", "cx", "cz"), "cy")
    up_spec = P("cy", ("cz", "cx"))
    down_spec = P("cz", ("cy", "cx"))
    up_out = P(("dp", "cy"), ("cz", "cx"))
    down_out = P(("dp", "cz"), ("cy", "cx"))
    plan = make_plan()
    order, panels, _, _ = make_order(plan, *make_lists(plan))

    def local_step(x_act, w_up, w_down, z_grad):
        t_loc, d_loc = x_act.shape
        f_loc = w_up.shape[1]
        rows, sub, dh = t_loc // NB, f_loc // RING, d_loc // 2
        grp = RING * rows
        bf, f32 = jnp.bfloat16, jnp.float32
        xa, za = x_act.reshape(NB, rows, d_loc), z_grad.reshape(NB, rows, d_loc)
        wu = w_up.reshape(2, dh, f_loc)
        wd = w_down.reshape(CORES, RING, sub, dh)
        hbm = lambda *s: jax.ShapeDtypeStruct(s, bf)
        outs = (
            pltpu.VMEM((NB, rows, d_loc), bf), pltpu.VMEM((2, dh, f_loc), bf), pltpu.VMEM((CORES, RING, sub, dh), bf),
            hbm(RING, NB, grp, d_loc), hbm(RING, NB, grp, d_loc), hbm(RING, NB, CORES, grp, sub),
            hbm(RING, NB, grp, sub), hbm(RING, NB, grp, sub), hbm(NB, grp, d_loc), hbm(NB, grp, 2 * sub),
            hbm(2, dh, sub), hbm(2, sub, dh), hbm(2, sub, dh),
        )
        scratch = [
            pltpu.VMEM((2 * RING, dh, 2 * sub), bf), pltpu.VMEM((2 * RING, sub, d_loc), bf), pltpu.VMEM((2 * RING, dh, 2 * sub), bf),
            pltpu.VMEM((NB, grp, 2 * sub), bf), pltpu.VMEM((PAN, RING, grp, d_loc), bf),
            pltpu.VMEM((2, 2, grp, dh), f32),
            pltpu.VMEM((NB, 2, rows, dh), f32), pltpu.VMEM((NB, 2, 2, rows, dh), f32),
            pltpu.VMEM((3, CORES, sub, dh), bf),
            pltpu.VMEM((grp, sub), f32),
        ]
        any_spec = pl.BlockSpec(memory_space=pl.ANY)
        res = pl.pallas_call(
            functools.partial(kernel, plan, order, panels),
            out_shape=outs,
            in_specs=[any_spec] * 4,
            out_specs=[pl.BlockSpec(memory_space=pltpu.VMEM)] * 3 + [any_spec] * (len(outs) - 3),
            scratch_shapes=scratch,
            compiler_params=pltpu.CompilerParams(collective_id=0, has_side_effects=True, vmem_limit_bytes=57600000),
            name="mlp_bwd",
        )(xa, wu, wd, za)
        outs = [pltpu.with_memory_space_constraint(o, pltpu.VMEM) for o in res[:3]]
        outs = pl.pallas_call(
            write_out,
            out_shape=[jax.ShapeDtypeStruct(o.shape, bf) for o in outs],
            in_specs=[pl.BlockSpec(memory_space=pltpu.VMEM) for _ in outs],
            out_specs=[any_spec for _ in outs],
            scratch_shapes=[pltpu.SemaphoreType.DMA((len(outs),))],
            compiler_params=pltpu.CompilerParams(vmem_limit_bytes=1 << 20),
            name="write_out",
        )(*outs)
        return tuple(o.reshape(a.shape) for o, a in zip(outs, (x_act, w_up, w_down)))

    return jax.shard_map(local_step, mesh=mesh, in_specs=(row_spec, up_spec, down_spec, row_spec), out_specs=(row_spec, up_out, down_out), check_vma=False)
```

```python
import functools
import math
import string
import itertools

import jax
import jax.numpy as jnp
from jax import lax
from jax.experimental import pallas as pl
from jax.experimental.pallas import tpu as pltpu
from jax.sharding import PartitionSpec as P

GELU_COEF = 0.044715
SQRT_TWO_PI = math.sqrt(2.0 / math.pi)
NN = (((1,), (0,)), ((), ()))
NT = (((1,), (1,)), ((), ()))
TN = (((0,), (0,)), ((), ()))
MESH = pl.DeviceIdType.MESH
RING = 4
CORES = 2
PAN = 3
GROUPS = ((0, 0, 8), (1, 0, 8), (2, 0, 8), (3, 0, 4), (3, 4, 4))
NB = 4
NG = len(GROUPS)
EARLY = 2
X, G = 0, 1


def gelu_parts(pre_act):
    inner_arg = SQRT_TWO_PI * (pre_act + GELU_COEF * pre_act * pre_act * pre_act)
    tanh_val = jnp.tanh(inner_arg)
    gelu_val = 0.5 * pre_act * (1.0 + tanh_val)
    gelu_slope = 0.5 * (1.0 + tanh_val) + 0.5 * pre_act * (1.0 - tanh_val * tanh_val) * SQRT_TWO_PI * (1.0 + 3.0 * GELU_COEF * pre_act * pre_act)
    return gelu_val, gelu_slope


(XS, XR, W2, W1, WR, CS, CR, O2, O1, OR, YA, YB, YF, YR, Q2, QD, QS, WN, WP, GP, XP, HP, CP, CF,
 ST, OWN, L1, L2, L3, L4, L5, LX, LH, M1, M2, M3, M4, M5, QA, QF, OUT) = range(41)
PANEL_OF = {L1: M1, L2: M2, L3: M3, L4: M4, L5: M5}
O5 = (2, 1, 3, 0)
O4 = (0, 1, 3, 2)
PARTS = ((0, 1), (1, 2), (3, 1))
PART_OF = [p for p, (_, n) in enumerate(PARTS) for _ in range(n)]


def full(a, r):
    return [(XS, a, r), (XR, a, r), (YR, a, r), (OWN,)] + ([(YA, a, r), (YB, a, r)] if r < EARLY else [(YF, a, r)])


def staged(r):
    return GROUPS[r][2] == 8


def make_plan():
    it, un = {}, {}
    groups = range(NG)
    for r in groups:
        q = GROUPS[r][2] / 8 / NB
        f = 4 * q
        for a in (X, G):
            it[XS, a, r] = (0, q, [])
            it[XR, a, r] = (0, q / 2, [(XS, a, r)])
            row = [(XS, a, r), (XR, a, r)]
            if r < EARLY:
                it[YA, a, r] = (1, q, [])
                it[YB, a, r] = (1, 3 * q, row)
                it[YR, a, r] = (1, 2 * q, [(YA, a, r), (YB, a, r)])
            else:
                it[YF, a, r] = (1, 4 * q, row + [(OWN,)])
                it[YR, a, r] = (1, 2 * q, [(YF, a, r)])
        it[GP, r] = (2, 8 * q, full(G, r))
        it[XP, r] = (2, 4 * q, full(X, r))
        it[HP, r] = (2, 4 * q, [(M2, r)])
        it[ST, r] = (3, f, [(M2, r)])
        it[CS, r] = (0, f, [(ST, r) if staged(r) else (M2, r)])
        it[CR, r] = (0, 2 * q, [(CS, r)])
        dc = [(ST, r), (CS, r), (CR, r)]
        it[CP, r] = (2, 6 * q, [(ST, r), (CS, r)])
        it[CF, r] = (2, 2 * q, [(CR, r)])
        it[Q2, r] = (1, q, [(M3, r)])
        it[QD, r] = (1, q, [(M3, r)])
        it[QS, r] = (1, q, [(QA, r)])
        it[L1, r] = (3, 16 * q, full(X, r))
        it[L2, r] = (3, 16 * q, full(G, r))
        it[L3, r] = (3, 16 * q, dc)
        wu = [(WP, 0, p) for p in range(3)]
        wd = [(WP, 1, p) for p in range(3)]
        un[M1, r] = (0.4 + 4.4 * f, [(L1, r)] + wu)
        un[M2, r] = (0.4 + 6.2 * f, [(L2, r), (M1, r)] + wd)
        un[M3, r] = (0.4 + 4.4 * f, [(L3, r), (WN,)] + ([(QF, r - 2)] if r >= 2 else []))
        un[QA, r] = (0.1 + 0.4 * f, [(Q2, r)])
        un[QF, r] = (0.1 + 0.4 * f, [(QS, r), (QD, r)])
    for w in range(2):
        it[W2, w] = (0, 0.5, [])
        it[W1, w] = (0, 1.0, [])
        it[WR, w] = (0, 0.5, [(W2, w)])
        it[WP, w, 0] = (2, 1, [])
        it[WP, w, 1] = (2, 2, [(W1, w)])
        it[WP, w, 2] = (2, 1, [(WR, w)])
    it[(WN,)] = (2, 4, [])
    it[(OWN,)] = (3, 2, [])
    it[(O2,)] = (0, 0.5, [(M5, 0)])
    it[(O1,)] = (0, 1.0, [(M5, 1)])
    it[(OR,)] = (0, 0.5, [(O2,)])
    for p in range(RING):
        it[L5, p] = (3, 4, [(GP, r) for r in groups] + sum([full(G, r) for r in groups], []))
        it[L4, p] = (3, 4, [(CF if O4[p] == 2 else CP, r) for r in groups] + [((ST, CS, CS, CR)[p], r) for r in groups])
    it[(LH,)] = (3, 4, [(HP, r) for r in groups] + [(M2, r) for r in groups])
    it[(LX,)] = (3, 8, [(XP, r) for r in groups] + [(M5, 0)])
    for p, (first, n) in enumerate(PARTS):
        un[M4, p] = (4.8 * n, [(L4, first + i) for i in range(n)] + [(LX,)])
        un[M5, p] = (4.8 * n, [(L5, first + i) for i in range(n)] + [(LH,)])
    return it, un


ORDER = (
    "acbdimgInhjEHGFyJosuApzteBvkflqwrxCKDML",
    "admjbecsknfolutvzBACGIHJghipqrwxyDKELFM",
    "yompqhsjlwunkfAgBtxCiveabzcrEDd",
)


def make_lists(plan):
    it, un = plan
    base = [[n for n in it if it[n][0] == k] for k in range(len(ORDER) - 1)] + [list(un)]
    *lists, units = ([names[string.ascii_letters.index(ch)] for ch in key] for names, key in zip(base, ORDER))
    return lists, units


LINKS = range(4)
RATE = (22.5,) * 2 + (1.7, 0.4)
DELAY = (3.0,) * 2 + (1.5,) * 2


def make_order(plan, lists, units):
    it, un = plan
    done, free, pos = {}, [0.0 for _ in LINKS], [0 for _ in LINKS]
    pend, now, order, panels, waits = list(units), 0.0, [], [], []
    late = [n for n in it if it[n][0] >= 2]
    rank = {u: i for i, u in enumerate(units)}
    user = lambda n: (PANEL_OF[n[0]], PART_OF[n[1]] if n[0] in (L4, L5) else n[1])
    panel_rank = lambda n: rank[user(n)] if n[0] in PANEL_OF else rank[{LX: M4, LH: M5}[n[0]], 0] if n[0] in (LX, LH) else -1
    gone = set()
    big = 1e9

    def ready(n):
        return all(done.get(d, big) <= now for d in it[n][2])

    def send(n):
        k = it[n][0]
        start = max(now + 0.3, free[k])
        waits.append((k, start - free[k], n))
        free[k] = start + it[n][1] * RATE[k]
        done[n] = free[k] + DELAY[k]
        order.append((n, now))

    while True:
        for k in (0, 1):
            while pos[k] < len(lists[k]) and ready(lists[k][pos[k]]):
                send(lists[k][pos[k]])
                pos[k] += 1
        for n in sorted((n for n in late if ready(n)), key=lambda n: (panel_rank(n), n)):
            if n[0] in PANEL_OF:
                if len(panels) >= PAN and user(panels[-PAN]) not in gone:
                    continue
                panels.append(n)
            late.remove(n)
            send(n)
        can = [u for u in pend if all(done.get(d, big) <= now for d in un[u][1])]
        if can:
            pend.remove(can[0])
            order.append((can[0], now))
            now += un[can[0]][0]
            done[can[0]] = now
            gone.add(can[0])
            continue
        later = [v for v in done.values() if v > now]
        if not later:
            break
        now = min(later)
    assert not pend and not late and all(pos[k] == len(lists[k]) for k in (0, 1)), (pend, late, pos)
    return [(n, [m for m in it if t - 30 < done[m] <= t - 2 and it[m][0] < 3]) for n, t in order], panels, max(done.values()), waits


class Copies:
    BACK = {"R": "L", "L": "R", "U": "N", "N": "U", "P": "P"}

    def __init__(self, send, recv, local, peers):
        self.send, self.recv, self.local, self.peers = send, recv, local, peers
        self.by_name, self.clock = {}, 0
        self.used = {"send": 0, "recv": 0, "local": 0}
        self.free = {"send": [], "local": []} | {to: [] for to in peers}
        self.waited = {to: [] for to in peers}

    def take(self, kind, pool):
        if self.free[pool]:
            return self.free[pool].pop()
        self.used[kind] += 1
        return self.used[kind] - 1

    def add(self, name, pairs):
        made = []
        for src, dst, to in pairs:
            self.clock += 1
            if to is None:
                i = self.take("local", "local")
                made.append([pltpu.make_async_copy(src, dst, self.local.at[i]), to, self.clock, i, None])
            else:
                axis, idx = self.peers[to]
                i, j = self.take("send", "send"), self.take("recv", to)
                c = pltpu.make_async_remote_copy(src, dst, self.send.at[i], self.recv.at[j], device_id={axis: idx}, device_id_type=MESH)
                made.append([c, to, self.clock, i, j])
            made[-1][0].start()
        self.by_name.setdefault(name, []).extend(made)

    def arrived(self, name):
        for m in self.by_name.get(name, ()):
            c, to, started, i, j = m
            self.clock += 1
            if to is None and i is not None:
                c.wait()
                self.free["local"].append(i)
                m[3] = None
            elif j is not None:
                c.wait_recv()
                self.waited[to].append((self.clock, j))
                m[4] = None
                back = self.BACK[to]
                self.free[back] += [k for t, k in self.waited[back] if t < started]
                self.waited[back] = [(t, k) for t, k in self.waited[back] if t >= started]

    def left(self, name):
        for m in self.by_name.get(name, ()):
            if m[1] is None:
                self.arrived(name)
            elif m[3] is not None:
                m[0].wait_send()
                self.free["send"].append(m[3])
                m[3] = None

    def finish(self):
        for name in list(self.by_name):
            self.arrived(name)
            self.left(name)


PIECES = 8
N_SEND, N_RECV, N_LOCAL = 26, 54, 16


def work(plan, order, panels, xa, wu, wd, za, dx, dwu, dwd, XF, GF, DF, GPB, DPB, XPB, HPB, su, sd, sw,
           wus, wds, wun, hbuf, pan, ft, rst, rrc, obuf, acc, send, recv, local):
    it, un = plan
    x, y, c = lax.axis_index("cy"), lax.axis_index("cz"), lax.axis_index("cx")
    peers = {
        "R": ("cy", lax.rem(x + 1, RING)), "L": ("cy", lax.rem(x + RING - 1, RING)),
        "U": ("cz", lax.rem(y + 1, RING)), "N": ("cz", lax.rem(y + RING - 1, RING)),
        "P": ("cx", 1 - c),
    }
    barrier = pltpu.get_barrier_semaphore()
    for axis, idx in peers.values():
        pl.semaphore_signal(barrier, inc=1, device_id={axis: idx}, device_id_type=MESH)
    pl.semaphore_wait(barrier, len(peers))

    cp = Copies(send, recv, local, peers)
    blk_rows = xa.shape[1]
    sub = wd.shape[2]
    dh = wu.shape[1]
    mine = pl.ds(pl.multiple_of(c * sub, sub), sub)
    theirs = pl.ds(pl.multiple_of((1 - c) * sub, sub), sub)
    lo, hi = pl.ds(0, sub), pl.ds(sub, sub)
    at = lambda j: lax.rem(x + j, RING)
    cols = lambda j: pl.ds(pl.multiple_of(at(j) * sub, sub), sub)
    slot_of = {n: i % PAN for i, n in enumerate(panels)}
    inp, buf = (xa, za), (XF, GF)

    def group(r):
        b, first, n = GROUPS[r]
        unit_rows = blk_rows // 8
        return b, first * unit_rows, n * unit_rows

    def rel(r, k, part=None):
        _, first, n = group(r)
        start = RING * first + k * n
        return pl.ds(start, n) if part is None else pl.ds(start + part * (n // 2), n // 2)

    def span(r):
        _, first, n = group(r)
        return pl.ds(RING * first, RING * n)

    def copies_of(name):
        kind, a, r = name[0], name[-2:][0], name[-1]
        both = lambda right, left: [right + ("R",), left + ("L",)]
        updn = lambda up, down: [up + ("U",), down + ("N",)]
        if kind == WN:
            return sum([[(wu.at[:, :, cols(j)], wun.at[2 * j:2 * j + 2, :, mine], to) for to in (None, "P")] for j in range(RING)], [])
        if kind == XS or kind == YA:
            b, first, n = group(r)
            src = inp[a].at[b, pl.ds(first, n)]
            if kind == XS:
                return both((src, buf[a].at[3, b, rel(r, 0)]), (src, buf[a].at[1, b, rel(r, 0)]))
            return updn((src, buf[a].at[0, b, rel(r, 3)]), (src, buf[a].at[0, b, rel(r, 1)]))
        if kind == XR:
            b, f, s = group(r)[0], rel(r, 0, 0), rel(r, 0, 1)
            return both((buf[a].at[3, b, f], buf[a].at[2, b, f]), (buf[a].at[1, b, s], buf[a].at[2, b, s]))
        if kind in (YB, YF):
            b, m = group(r)[0], buf[a]
            js = pl.ds(1, RING - 1) if kind == YB else pl.ds(0, RING)
            return updn((m.at[js, b, rel(r, 0)], m.at[js, b, rel(r, 3)]), (m.at[js, b, rel(r, 0)], m.at[js, b, rel(r, 1)]))
        if kind == YR:
            b, m = group(r)[0], buf[a]
            return updn((m.at[0:2, b, rel(r, 3)], m.at[0:2, b, rel(r, 2)]), (m.at[2:4, b, rel(r, 1)], m.at[2:4, b, rel(r, 2)]))
        if kind in (W2, W1, WR):
            half = (lambda h, j: wu.at[h, :, cols(j)]) if r == 0 else (lambda h, j: wd.at[h, at(j)])
            piece = (lambda j: wu.at[:, :, cols(j)]) if r == 0 else (lambda j: wd.at[:, at(j)])
            st, dst = (su, sd)[r], (wus, wds)[r]
            if kind == W2:
                return both((half(0, 2), st.at[0]), (half(1, 2), st.at[1]))
            if kind == W1:
                return both((piece(1), dst.at[6:8, :, mine]), (piece(3), dst.at[2:4, :, mine]))
            return both((st.at[0], dst.at[4, :, mine]), (st.at[1], dst.at[5, :, mine]))
        if kind == WP:
            m = (wus, wds)[a]
            if r == 0:
                src = wu.at[:, :, cols(0)] if a == 0 else wd.at[:, at(0)]
                return [(src, m.at[0:2, :, mine], to) for to in (None, "P")]
            return [(m.at[2 * j:2 * j + 2, :, mine], m.at[2 * j:2 * j + 2, :, mine], "P") for j in ((1, 3) if r == 1 else (2,))]
        if kind == GP:
            return [(GF.at[:, group(r)[0], span(r), theirs], GPB.at[:, group(r)[0], span(r)], "P")]
        if kind == XP:
            return [(XF.at[0, group(r)[0], span(r)], XPB.at[group(r)[0], span(r)], "P")]
        if kind == HP:
            return [(hbuf.at[group(r)[0], span(r)], HPB.at[group(r)[0], span(r)], "P")]
        if kind in (CP, CF):
            b = group(r)[0]
            js = (pl.ds(0, 2), pl.ds(3, 1)) if kind == CP else (pl.ds(2, 1),)
            return [(DF.at[j, b, 1 - c, span(r)], DPB.at[j, b, span(r)], "P") for j in js]
        if kind == ST:
            b = group(r)[0]
            return [(obuf.at[2, :, span(r)], DF.at[0, b, :, span(r)], None)]
        if kind == CS:
            b = group(r)[0]
            m = DF.at[0, b, :, span(r)] if staged(r) else obuf.at[2, :, span(r)]
            return both((m, DF.at[3, b, :, span(r)]), (m, DF.at[1, b, :, span(r)]))
        if kind == CR:
            b, first, n = group(r)
            f, s = (pl.ds(RING * first + h * 2 * n, 2 * n) for h in range(2))
            return both((DF.at[3, b, :, f], DF.at[2, b, :, f]), (DF.at[1, b, :, s], DF.at[2, b, :, s]))
        if kind in (Q2, QD, QS):
            b, first, n = group(r)
            f = ft.at[r % 2]
            own = lambda k: pl.ds(k * n, n)
            rs = pl.ds(first, n)
            if kind == Q2:
                return updn((f.at[0, own(2)], rst.at[b, 0, rs]), (f.at[1, own(2)], rst.at[b, 1, rs]))
            if kind == QD:
                return updn((f.at[1, own(1)], rrc.at[b, 0, 1, rs]), (f.at[0, own(3)], rrc.at[b, 1, 0, rs]))
            return updn((f.at[0, own(1)], rrc.at[b, 0, 0, rs]), (f.at[1, own(3)], rrc.at[b, 1, 1, rs]))
        if kind in (L1, L2, L3):
            b, _, n = group(r)
            to = pan.at[slot_of[name], :, pl.ds(0, RING * n)]
            if kind == L3:
                return [(DF.at[:, b, h, span(r)], to.at[:, :, h * sub:(h + 1) * sub], None) for h in range(CORES)]
            return [((XF if kind == L1 else GF).at[:, b, span(r)], to, None)]
        if kind in (L5, L4):
            m, p = (GF.at[O5[r], :, :, mine], GPB.at[O5[r]]) if kind == L5 else (DF.at[O4[r], :, c], DPB.at[O4[r]])
            s = pan.at[slot_of[name]]
            return [(m, s.at[:, :, lo], None), (p, s.at[:, :, hi], None)]
        if kind == LH:
            return [(HPB, wds.at[0:4], None)]
        if kind == LX:
            return [(XF.at[0], wus.at[0:4], None), (XPB, wus.at[4:8], None)]
        place = {j: i for i, j in enumerate(O5)}
        if kind == O2:
            return both((obuf.at[place[2], 0], sw.at[0]), (obuf.at[place[2], 1], sw.at[1]))
        if kind == O1:
            return both((obuf.at[place[1]], dwd.at[:, x]), (obuf.at[place[3]], dwd.at[:, x]))
        assert kind == OR
        return both((sw.at[0], dwd.at[0, at(3)]), (sw.at[1], dwd.at[1, at(1)]))

    def total(terms):
        out = None
        for a, b, dims in terms:
            d = lax.dot_general(a, b, dims, preferred_element_type=jnp.float32)
            out = d if out is None else out + d
        return out

    def loop(n, body):
        def step(i, carry):
            body(i)
            return carry
        lax.fori_loop(0, n, step, 0)

    def unit(name):
        kind, r = name[0], name[-1]
        if kind in (M1, M2, M3):
            b, first, n = group(r)
            rows = pl.ds(0, RING * n)
        if kind == M1:
            p = pan.at[slot_of[L1, r]]

            def body(t):
                ns = pl.ds(pl.multiple_of(t * sub, sub), sub)
                s = total([(p[j, rows, h * dh:(h + 1) * dh], wus[2 * j + h, :, ns], NN) for j in range(RING) for h in range(2)])
                hbuf[b, span(r), ns] = s.astype(jnp.bfloat16)
            loop(2, body)
        elif kind == M2:
            p = pan.at[slot_of[L2, r]]
            if r > 0 and staged(r - 1):
                cp.arrived((ST, r - 1))
            step = min(32, RING * n)

            def body(t):
                ns = pl.ds(pl.multiple_of(t * sub, sub), sub)
                acc[rows, :] = total([(p[j, rows, :], wds[2 * j + t], NT) for j in range(RING)])

                def elem(e):
                    rs = pl.ds(pl.multiple_of(e * step, step), step)
                    hs = pl.ds(pl.multiple_of(RING * first + e * step, step), step)
                    g, s = gelu_parts(hbuf[b, hs, ns].astype(jnp.float32))
                    hbuf[b, hs, ns] = g.astype(jnp.bfloat16)
                    obuf[2, t, hs, :] = (acc[rs, :] * s).astype(jnp.bfloat16)
                loop(RING * n // step, elem)
            loop(2, body)
        elif kind == M3:
            p = pan.at[slot_of[L3, r]]
            if r >= 2:
                for q in (Q2, QD, QS):
                    cp.left((q, r - 2))
            f = ft.at[r % 2]

            def body(t):
                f[t, rows, :] = total([(p[j, rows, :], wun[2 * j + t], NT) for j in range(RING)])
            loop(2, body)
        elif kind in (M5, M4):
            i0, m = PARTS[r]
            s0, s1 = (slot_of[L5 if kind == M5 else L4, i] for i in (i0, i0 + m - 1))
            j0, j1 = ((O5 if kind == M5 else O4)[i] for i in (i0, i0 + m - 1))
            own, par, p0 = (hbuf, wds, 0) if kind == M5 else (wus, wus, NB)
            if kind == M5 and i0 + m - 1 == 2:
                for g in range(NG):
                    cp.arrived((ST, g))
                    cp.left((CS, g))

            def body(i):
                e, t = (0, i) if m == 1 else (i // 2, lax.rem(i, 2))
                p = pan.at[s0 + e * (s1 - s0)]
                ms = pl.ds(pl.multiple_of(t * dh, dh), dh)
                s = total([(own[g, :, ms], p[g, :, lo], TN) for g in range(NB)] + [(par[p0 + g, :, ms], p[g, :, hi], TN) for g in range(NB)])
                if kind == M5 and O5[i0] == 0:
                    dwd[t, x] = s.astype(jnp.bfloat16)
                elif kind == M5:
                    obuf[i0 + e, t] = s.astype(jnp.bfloat16)
                else:
                    dwu[t, :, cols(j0 + e * (j1 - j0))] = s.astype(jnp.bfloat16)
            loop(2 * m, body)
        else:
            b, first, n = group(r)
            f = ft.at[r % 2]
            rs = pl.ds(first, n)
            own = lambda k: pl.ds(k * n, n)
            if kind == QA:
                f[0, own(1), :] = f[0, own(1), :] + rst[b, 0, rs, :]
                f[1, own(3), :] = f[1, own(3), :] + rst[b, 1, rs, :]
            else:
                for h in range(2):
                    dx[b, rs, h * dh:(h + 1) * dh] = (f[h, own(0), :] + rrc[b, 0, h, rs, :] + rrc[b, 1, h, rs, :]).astype(jnp.bfloat16)

    for name, gone in order:
        for d in gone:
            cp.arrived(d)
            cp.left(d)
        for d in (it[name][2] if name in it else un[name][1]):
            cp.arrived(d)
        if name[0] == OWN:
            own = pl.ds(0, blk_rows)
            b0, b1 = pan.at[0, :, own], pan.at[1, :, own]
            cp.add((OUT, OWN), [(xa, b0, None), (za, b1, None)])
            cp.arrived((OUT, OWN))
            pairs = []
            for r in range(NG):
                b, first, n = group(r)
                pairs += [(pan.at[a, b, pl.ds(first, n)], buf[a].at[0, b, rel(r, 0)], None) for a in (X, G)]
            cp.add(name, pairs)
        elif name in it:
            for w in {LX: (0,), LH: (1,)}.get(name[0], ()):
                for p in range(3):
                    cp.left((WP, w, p))
            cp.add(name, copies_of(name))
        else:
            unit(name)
    cp.finish()
    assert tuple(cp.used.values()) == (N_SEND, N_RECV, N_LOCAL), cp.used


def kernel(plan, order, panels, *refs):
    pl.run_scoped(functools.partial(work, plan, order, panels, *refs), *(pltpu.SemaphoreType.DMA((n,)) for n in (N_SEND, N_RECV, N_LOCAL)))


def write_out(dx, dwu, dwd, dx_out, dwu_out, dwd_out, sem):
    arrays = ((dwd, dwd_out), (dwu, dwu_out), (dx, dx_out))
    for i, (a, b) in enumerate(arrays):
        lead = a.shape[:-2]
        pieces = PIECES if a is dwu else PIECES // 4
        n = a.shape[-2] // pieces
        for place in itertools.product(*map(range, lead)):
            for p in range(pieces):
                part = place + (pl.ds(p * n, n),)
                pltpu.make_async_copy(a.at[part], b.at[part], sem.at[i]).start()
    for i, (a, b) in enumerate(arrays):
        pltpu.make_async_copy(a, b, sem.at[i]).wait()


def solution(mesh):
    assert mesh.shape["cy"] == RING and mesh.shape["cz"] == RING and mesh.shape["cx"] == CORES
    row_spec = P(("dp", "cx", "cz"), "cy")
    up_spec = P("cy", ("cz", "cx"))
    down_spec = P("cz", ("cy", "cx"))
    up_out = P(("dp", "cy"), ("cz", "cx"))
    down_out = P(("dp", "cz"), ("cy", "cx"))
    plan = make_plan()
    order, panels, _, _ = make_order(plan, *make_lists(plan))

    def local_step(x_act, w_up, w_down, z_grad):
        t_loc, d_loc = x_act.shape
        f_loc = w_up.shape[1]
        rows, sub, dh = t_loc // NB, f_loc // RING, d_loc // 2
        grp = RING * rows
        bf, f32 = jnp.bfloat16, jnp.float32
        xa, za = x_act.reshape(NB, rows, d_loc), z_grad.reshape(NB, rows, d_loc)
        wu = w_up.reshape(2, dh, f_loc)
        wd = w_down.reshape(CORES, RING, sub, dh)
        hbm = lambda *s: jax.ShapeDtypeStruct(s, bf)
        outs = (
            pltpu.VMEM((NB, rows, d_loc), bf), pltpu.VMEM((2, dh, f_loc), bf), pltpu.VMEM((CORES, RING, sub, dh), bf),
            hbm(RING, NB, grp, d_loc), hbm(RING, NB, grp, d_loc), hbm(RING, NB, CORES, grp, sub),
            hbm(RING, NB, grp, sub), hbm(RING, NB, grp, sub), hbm(NB, grp, d_loc), hbm(NB, grp, 2 * sub),
            hbm(2, dh, sub), hbm(2, sub, dh), hbm(2, sub, dh),
        )
        scratch = [
            pltpu.VMEM((2 * RING, dh, 2 * sub), bf), pltpu.VMEM((2 * RING, sub, d_loc), bf), pltpu.VMEM((2 * RING, dh, 2 * sub), bf),
            pltpu.VMEM((NB, grp, 2 * sub), bf), pltpu.VMEM((PAN, RING, grp, d_loc), bf),
            pltpu.VMEM((2, 2, grp, dh), f32),
            pltpu.VMEM((NB, 2, rows, dh), f32), pltpu.VMEM((NB, 2, 2, rows, dh), f32),
            pltpu.VMEM((3, CORES, sub, dh), bf),
            pltpu.VMEM((grp, sub), f32),
        ]
        any_spec = pl.BlockSpec(memory_space=pl.ANY)
        res = pl.pallas_call(
            functools.partial(kernel, plan, order, panels),
            out_shape=outs,
            in_specs=[any_spec] * 4,
            out_specs=[pl.BlockSpec(memory_space=pltpu.VMEM)] * 3 + [any_spec] * (len(outs) - 3),
            scratch_shapes=scratch,
            compiler_params=pltpu.CompilerParams(collective_id=0, has_side_effects=True, vmem_limit_bytes=57600000),
            name="mlp_bwd",
        )(xa, wu, wd, za)
        outs = [pltpu.with_memory_space_constraint(o, pltpu.VMEM) for o in res[:3]]
        outs = pl.pallas_call(
            write_out,
            out_shape=[jax.ShapeDtypeStruct(o.shape, bf) for o in outs],
            in_specs=[pl.BlockSpec(memory_space=pltpu.VMEM) for _ in outs],
            out_specs=[any_spec for _ in outs],
            scratch_shapes=[pltpu.SemaphoreType.DMA((len(outs),))],
            compiler_params=pltpu.CompilerParams(vmem_limit_bytes=1 << 20),
            name="write_out",
        )(*outs)
        return tuple(o.reshape(a.shape) for o, a in zip(outs, (x_act, w_up, w_down)))

    return jax.shard_map(local_step, mesh=mesh, in_specs=(row_spec, up_spec, down_spec, row_spec), out_specs=(row_spec, up_out, down_out), check_vma=False)
```
